8 devices in a mesh: data: 1 (over z), graph: 8 (over y, x, core).
Axes of the slice: x: 2, y: 2, z: 1, core: 2. Of those that a mesh axis runs over, the one named last changes fastest.
Arguments:
- x_feat: bfloat16 [16384, 50], P(('data', 'graph'))
- dst_local: int32 [65536], P(('data', 'graph'))
- src_slot: int32 [65536], P(('data', 'graph'))
- edge_w: float32 [65536], P(('data', 'graph'))
- send_idx: int32 [4096], P(('data', 'graph'))
- hub_ids: int32 [64], P('data')
- w_first: bfloat16 [50, 512], replicated
- b_first: float32 [512], replicated
- w_second: bfloat16 [512, 121], replicated
- grad_out: float32 [16384, 121], P(('data', 'graph'))
Outputs:
- output 1: float32 [16384, 50], P(('data', 'graph'))
- output 2: float32 [50, 512], P('data')
- output 3: float32 [512, 121], P('data')
- output 4: float32 [512], P('data')
- output 5: float32 [121], P('data')
All inputs are finite; a program needn't handle non-finite values.
Results may differ from the reference program's by a relative error of at most 0.0015773.
Values are sent between devices in bfloat16 or wider.
A program may use at most 1 GiB of HBM per device.

```python
import jax
import jax.numpy as jnp
from jax import lax

GROUP_SIZE = 8
NODES_DEV = 2048
FEAT_IN = 50
FEAT_HID = 512
FEAT_OUT = 121
EDGE_DEG = 4
SEND_ROWS = 64
NUM_HUBS = 64
HUB_DST_PCT = 15
HUB_SRC_PCT = 15
HALO_SRC_PCT = 35

VERTICES = GROUP_SIZE * NODES_DEV
EDGE_CAP = NODES_DEV * EDGE_DEG
HALO_ROWS = GROUP_SIZE * SEND_ROWS


def draw_graph(graph_key):
    key_list = jax.random.split(graph_key, 16)
    edge_shape = (GROUP_SIZE, EDGE_CAP)
    hub_ids = jax.random.permutation(key_list[0], VERTICES)[:NUM_HUBS].astype(jnp.int32)
    shrink = jax.random.randint(key_list[1], (GROUP_SIZE,), 1, 5)
    full_dev = jax.random.randint(key_list[2], (), 0, GROUP_SIZE)
    counts = jnp.where(jnp.arange(GROUP_SIZE) == full_dev, EDGE_CAP, EDGE_CAP // shrink)
    edge_live = jnp.arange(EDGE_CAP)[None, :] < counts[:, None]
    dst_pick = jax.random.randint(key_list[3], edge_shape, 0, 100)
    dst_span = jax.random.randint(key_list[4], edge_shape, 1, NODES_DEV + 1)
    dst_node = jax.random.randint(key_list[5], edge_shape, 0, NODES_DEV) % dst_span
    dst_hub = jax.random.randint(key_list[6], edge_shape, 0, NUM_HUBS)
    dst_local = jnp.where(dst_pick < HUB_DST_PCT, NODES_DEV + dst_hub, dst_node)
    src_pick = jax.random.randint(key_list[7], edge_shape, 0, 100)
    src_span = jax.random.randint(key_list[8], edge_shape, 1, NODES_DEV + 1)
    src_node = jax.random.randint(key_list[9], edge_shape, 0, NODES_DEV) % src_span
    peer_step = jax.random.randint(key_list[10], edge_shape, 1, GROUP_SIZE)
    peer_dev = (jnp.arange(GROUP_SIZE)[:, None] + peer_step) % GROUP_SIZE
    row_span = jax.random.randint(key_list[11], edge_shape, 1, SEND_ROWS + 1)
    halo_row = jax.random.randint(key_list[12], edge_shape, 0, SEND_ROWS) % row_span
    src_hub = jax.random.randint(key_list[13], edge_shape, 0, NUM_HUBS)
    src_slot = jnp.where(
        src_pick < HUB_SRC_PCT,
        NODES_DEV + HALO_ROWS + src_hub,
        jnp.where(src_pick < HUB_SRC_PCT + HALO_SRC_PCT, NODES_DEV + peer_dev * SEND_ROWS + halo_row, src_node),
    )
    send_idx = jax.random.randint(key_list[14], (GROUP_SIZE * GROUP_SIZE * SEND_ROWS,), 0, NODES_DEV)
    dst_local = jnp.where(edge_live, dst_local, 0).reshape(-1).astype(jnp.int32)
    src_slot = jnp.where(edge_live, src_slot, 0).reshape(-1).astype(jnp.int32)
    return dst_local, src_slot, edge_live.reshape(-1), send_idx.astype(jnp.int32), hub_ids


def setup_inputs(seed: int = 0, part: int = 0) -> dict:
    part_key = jax.random.fold_in(jax.random.key(seed), part)
    dst_local, src_slot, edge_live, send_idx, hub_ids = draw_graph(part_key)
    value_keys = jax.random.split(jax.random.fold_in(part_key, 3), 3)
    weight_keys = jax.random.split(jax.random.key(seed + 1), 3)
    x_feat = jax.random.normal(value_keys[0], (VERTICES, FEAT_IN), jnp.float32).astype(jnp.bfloat16)
    edge_scale = jax.random.uniform(value_keys[1], (GROUP_SIZE * EDGE_CAP,), jnp.float32, 0.5, 1.5)
    edge_w = jnp.where(edge_live, edge_scale * EDGE_DEG ** -0.5, 0.0).astype(jnp.float32)
    grad_out = jax.random.normal(value_keys[2], (VERTICES, FEAT_OUT), jnp.float32)
    w_first = (jax.random.normal(weight_keys[0], (FEAT_IN, FEAT_HID), jnp.float32) * FEAT_IN ** -0.5).astype(jnp.bfloat16)
    b_first = 0.5 * jax.random.normal(weight_keys[1], (FEAT_HID,), jnp.float32)
    w_second = (jax.random.normal(weight_keys[2], (FEAT_HID, FEAT_OUT), jnp.float32) * FEAT_HID ** -0.5).astype(jnp.bfloat16)
    return {
        "x_feat": x_feat,
        "dst_local": dst_local,
        "src_slot": src_slot,
        "edge_w": edge_w,
        "send_idx": send_idx,
        "hub_ids": hub_ids,
        "w_first": w_first,
        "b_first": b_first,
        "w_second": w_second,
        "grad_out": grad_out,
    }


def source_ids(src_slot, send_idx, hub_ids):
    slot_ids = src_slot.reshape(GROUP_SIZE, EDGE_CAP)
    device = jnp.arange(GROUP_SIZE)[:, None]
    halo_pos = jnp.clip(slot_ids - NODES_DEV, 0, HALO_ROWS - 1)
    peer_dev = halo_pos // SEND_ROWS
    send_table = send_idx.reshape(GROUP_SIZE, GROUP_SIZE, SEND_ROWS)
    halo_src = peer_dev * NODES_DEV + send_table[peer_dev, device, halo_pos % SEND_ROWS]
    hub_src = hub_ids[jnp.clip(slot_ids - NODES_DEV - HALO_ROWS, 0, NUM_HUBS - 1)]
    return jnp.where(
        slot_ids < NODES_DEV,
        device * NODES_DEV + slot_ids,
        jnp.where(slot_ids < NODES_DEV + HALO_ROWS, halo_src, hub_src),
    )


def aggregate(features, dst_rows, src_ids, edge_rows, hub_ids):
    def one_device(dev_item):
        dst_dev, src_dev, w_dev = dev_item
        gathered = features[src_dev] * w_dev[:, None]
        return jax.ops.segment_sum(gathered, dst_dev, num_segments=NODES_DEV + NUM_HUBS)
    dev_sums = lax.map(one_device, (dst_rows, src_ids, edge_rows))
    local_rows = dev_sums[:, :NODES_DEV].reshape(VERTICES, -1)
    return local_rows.at[hub_ids].add(dev_sums[:, NODES_DEV:].sum(axis=0))


def reference(x_feat, dst_local, src_slot, edge_w, send_idx, hub_ids, w_first, b_first, w_second, grad_out):
    src_ids = source_ids(src_slot, send_idx, hub_ids)
    dst_rows = dst_local.reshape(GROUP_SIZE, EDGE_CAP)
    edge_rows = edge_w.reshape(GROUP_SIZE, EDGE_CAP)

    def layers(x_in, w_in, b_in, w_out):
        z_first = jnp.dot(x_in, w_in, preferred_element_type=jnp.float32).astype(jnp.bfloat16).astype(jnp.float32)
        pre_act = aggregate(z_first, dst_rows, src_ids, edge_rows, hub_ids) + b_in
        act_full = jax.nn.relu(pre_act)
        hidden = act_full + lax.stop_gradient(act_full.astype(jnp.bfloat16).astype(jnp.float32) - act_full)
        z_second = jnp.dot(hidden, w_out, preferred_element_type=jnp.float32).astype(jnp.bfloat16).astype(jnp.float32)
        return aggregate(z_second, dst_rows, src_ids, edge_rows, hub_ids)

    _, pullback = jax.vjp(
        layers,
        x_feat.astype(jnp.float32),
        w_first.astype(jnp.float32),
        b_first,
        w_second.astype(jnp.float32),
    )
    grad_x, grad_w1, grad_b1, grad_w2 = pullback(grad_out)
    return grad_x, grad_w1, grad_w2, grad_b1, grad_out.sum(axis=0)
```

```python
import functools

import jax
import jax.numpy as jnp
from jax import lax
from jax.experimental import pallas as pl
from jax.experimental.pallas import tpu as pltpu
from jax.sharding import PartitionSpec as P

F32, BF16, I32 = jnp.float32, jnp.bfloat16, jnp.int32
CONTRACT_ROWS = (((0,), (0,)), ((), ()))
CONTRACT_COLS = (((1,), (1,)), ((), ()))
LANES = 128
HID = 512
TILES = HID // LANES
CHUNK = 256
VMEM_LIMIT = 63 * 2**20
VMEM = pl.BlockSpec(memory_space=pltpu.VMEM)
SMEM = pl.BlockSpec(memory_space=pltpu.SMEM)


def dot(a, b, dims=(((1,), (0,)), ((), ()))):
    return lax.dot_general(a, b, dims, preferred_element_type=F32)


def iota(shape, dim):
    return lax.broadcasted_iota(I32, shape, dim)


def split3(value):
    high = value.astype(BF16)
    rest = value - high.astype(F32)
    mid = rest.astype(BF16)
    low = (rest - mid.astype(F32)).astype(BF16)
    return high, mid, low


def select_rows(onehot, value, dims=(((1,), (0,)), ((), ()))):
    high, mid, low = split3(value)
    return dot(onehot, low, dims) + dot(onehot, mid, dims) + dot(onehot, high, dims)


def pad_lanes(value):
    rows, cols = value.shape
    if cols == LANES:
        return value
    return jnp.concatenate([value, jnp.zeros((rows, LANES - cols), value.dtype)], axis=1)


def greet(groups, me):
    barrier = pltpu.get_barrier_semaphore()
    for step in range(1, groups):
        pl.semaphore_signal(barrier, inc=1, device_id={"graph": lax.rem(me + step, groups)}, device_id_type=pl.DeviceIdType.MESH)
    return barrier


def send(src, dst, send_sem, recv_sem, peer):
    copy = pltpu.make_async_remote_copy(
        src_ref=src, dst_ref=dst, send_sem=send_sem, recv_sem=recv_sem,
        device_id={"graph": peer}, device_id_type=pl.DeviceIdType.MESH)
    copy.start()
    return copy


def gather_kernel(groups, x_ref, dh_ref, send_ref, hub_ref, hubrow_ref, dst_ref, src_ref,
                  xh_ref, hx_ref, dhh_ref, d4_ref, s4_ref, db2_ref,
                  x32, xg, hxg, dhg, xs, xr, dhr, ssem, rsem):
    me = lax.axis_index("graph")
    barrier = greet(groups, me)
    nodes, feat = x_ref.shape
    hubs = hub_ref.shape[0]
    halo = send_ref.shape[0]
    block = halo // groups
    base = me * nodes
    eye = (iota((feat, LANES), 0) == iota((feat, LANES), 1)).astype(BF16)
    tags = jnp.where(iota((hubs, LANES), 1) == feat, iota((hubs, LANES), 0) + 1, 0).astype(F32).astype(BF16)
    hubrow = hubrow_ref[...]
    for row in range(0, nodes, CHUNK):
        owned = (iota((CHUNK, hubs), 0) + (base + row) == hubrow).astype(BF16)
        x32[pl.ds(row, CHUNK), :] = dot(x_ref[pl.ds(row, CHUNK), :], eye) + dot(owned, tags)

    def pick(i, carry):
        for u in range(16):
            j = i * 16 + u
            xg[pl.ds(j, 1), :] = x32[pl.ds(send_ref[j], 1), :]
        return carry

    lax.fori_loop(0, halo // 16, pick, 0)
    dhg[...] = jnp.zeros_like(dhg)

    def pick_hub(i, carry):
        for u in range(8):
            k = i * 8 + u
            row = hub_ref[k] - base
            own = jnp.logical_and(row >= 0, row < nodes)
            row = jnp.clip(row, 0, nodes - 1)
            hxg[pl.ds(k, 1), :] = jnp.where(own, x32[pl.ds(row, 1), :], 0.0)
            value = dh_ref[pl.ds(row, 1), :]
            dhg[pl.ds(k, 1), pl.ds(0, value.shape[1])] = jnp.where(own, value, 0.0)
        return carry

    lax.fori_loop(0, hubs // 8, pick_hub, 0)
    for q in range(groups):
        xs[q, pl.ds(0, block), :] = xg[pl.ds(q * block, block), :].astype(BF16)
        xs[q, pl.ds(block, hubs), :] = hxg[...].astype(BF16)
    pl.semaphore_wait(barrier, groups - 1)
    copies = []
    for step in range(1, groups):
        peer = lax.rem(me + step, groups)
        copies.append(send(xs.at[peer], xr.at[me], ssem.at[0, step], rsem.at[0, step], peer))
        copies.append(send(dhg, dhr.at[me], ssem.at[1, step], rsem.at[1, step], peer))
    d4_ref[...] = dst_ref[...] * TILES
    s4_ref[...] = src_ref[...] * TILES
    total = jnp.zeros((8, dh_ref.shape[1]), F32)
    for row in range(0, nodes, CHUNK):
        total = total + dh_ref[pl.ds(row, CHUNK), :].reshape(CHUNK // 8, 8, dh_ref.shape[1]).sum(axis=0)
    db2_ref[...] = jnp.broadcast_to(pad_lanes(total.sum(axis=0, keepdims=True)), db2_ref.shape)
    xr[me] = xs[me]
    dhr[me] = dhg[...]
    for copy in copies:
        copy.wait()
    hx = jnp.zeros((hubs, LANES), F32)
    dhh = jnp.zeros((hubs, LANES), F32)
    for q in range(groups):
        xh_ref[pl.ds(q * block, block), :] = xr[q, pl.ds(0, block), :]
        hx = hx + xr[q, pl.ds(block, hubs), :].astype(F32)
        dhh = dhh + dhr[q]
    hx_ref[...] = hx
    dhh_ref[...] = dhh


def hub_position(hub_ref, k, base, nodes):
    row = hub_ref[k] - base
    own = jnp.logical_and(row >= 0, row < nodes)
    return own, pl.multiple_of(jnp.clip(row, 0, nodes - 1) * TILES, TILES)


def strided(first, rows):
    return pl.ds(first, rows, stride=TILES)


def total_of(refs, where):
    value = refs[0][where, :]
    for ref in refs[1:]:
        value = value + ref[where, :]
    return value


def edges_forward_kernel(copies, unroll, d4_ref, s4_ref, w_ref, hub_ref, x_ref, xh_ref, hx_ref, dh_ref, dhh_ref, w1_ref, b1_ref,
                         h1_ref, dz_ref, hz_ref, hub_out, zt, dt, *accs):
    ya, da = accs[:copies], accs[copies:]
    me = lax.axis_index("graph")
    nodes, feat = x_ref.shape
    halo, hubs = xh_ref.shape[0], hx_ref.shape[0]
    edges = w_ref.shape[0]
    base = me * nodes
    for acc in ya:
        acc[...] = jnp.zeros_like(acc)
    for acc in da:
        acc[strided(0, nodes + halo + hubs), :] = jnp.zeros((nodes + halo + hubs, LANES), F32)
    w1 = w1_ref[...]

    def put_rows(first, x_rows):
        z = dot(x_rows, w1).astype(BF16).astype(F32)
        for c in range(TILES):
            zt[strided(first * TILES + c, x_rows.shape[0]), :] = z[:, c * LANES:(c + 1) * LANES]

    for row in range(0, nodes, CHUNK):
        put_rows(row, x_ref[pl.ds(row, CHUNK), :])
        dt[strided(row * TILES, CHUNK), :] = pad_lanes(dh_ref[pl.ds(row, CHUNK), :])
    for row in range(0, halo, CHUNK):
        put_rows(nodes + row, xh_ref[pl.ds(row, CHUNK), pl.ds(0, feat)])
    put_rows(nodes + halo, hx_ref[:, pl.ds(0, feat)].astype(BF16))
    dt[strided(nodes * TILES, hubs), :] = dhh_ref[...]

    def step(i, carry):
        for u0 in range(0, unroll, copies):
            new = []
            for u in range(copies):
                j = i * unroll + u0 + u
                s4 = pl.multiple_of(s4_ref[j], TILES)
                d4 = pl.multiple_of(d4_ref[j], TILES)
                w = w_ref[j]
                new.append((s4, d4, ya[u][pl.ds(d4, TILES), :] + w * zt[pl.ds(s4, TILES), :],
                            da[u][pl.ds(s4, 1), :] + w * dt[pl.ds(d4, 1), :]))
            for u, (s4, d4, y_new, z_new) in enumerate(new):
                ya[u][pl.ds(d4, TILES), :] = y_new
                da[u][pl.ds(s4, 1), :] = z_new
        return carry

    lax.fori_loop(0, edges // unroll, step, 0)

    def fold(k, carry):
        own, row = hub_position(hub_ref, k, base, nodes)
        here = pl.multiple_of((nodes + k) * TILES, TILES)
        ya[0][pl.ds(here, TILES), :] += jnp.where(own, total_of(ya, pl.ds(row, TILES)), 0.0)
        here = (nodes + halo + k) * TILES
        value = total_of(da, pl.ds(row, 1))
        da[0][pl.ds(here, 1), :] += jnp.where(own, value, 0.0)
        da[0][pl.ds(row, 1), :] = jnp.where(own, 0.0, value)
        for acc in da[1:]:
            acc[pl.ds(row, 1), :] = jnp.zeros((1, LANES), F32)
        return carry

    lax.fori_loop(0, hubs, fold, 0)
    for row in range(0, nodes, CHUNK):
        for c in range(TILES):
            cols = pl.ds(c * LANES, LANES)
            y = total_of(ya, strided(row * TILES + c, CHUNK)) + b1_ref[:, cols]
            h1_ref[pl.ds(row, CHUNK), cols] = jnp.maximum(y, 0.0).astype(BF16)
        dz_ref[pl.ds(row, CHUNK), :] = total_of(da, strided(row * TILES, CHUNK))
    hz = total_of(da, strided(nodes * TILES, halo))
    tag = xh_ref[...].astype(F32)[:, feat:feat + 1]
    onehot = (tag == (iota((halo, hubs), 1) + 1).astype(F32)).astype(BF16)
    hub_z = total_of(da, strided((nodes + halo) * TILES, hubs)) + select_rows(onehot, hz, CONTRACT_ROWS)
    hz_ref[...] = jnp.where(tag > 0.0, 0.0, hz)
    for c in range(TILES):
        hub_out[:, pl.ds(c * LANES, LANES)] = total_of(ya, strided(nodes * TILES + c, hubs))
    hub_out[:, pl.ds(HID, LANES)] = hub_z


def middle_kernel(groups, hz_ref, hub_ref, dz_ref, sendrow_ref, w2_ref, b1_ref,
                  dz2_ref, dyh_ref, h1h_ref, dz2h_ref,
                  hzr, hubr, dyr, dys, ssem, rsem):
    me = lax.axis_index("graph")
    barrier = greet(groups, me)
    nodes = dz_ref.shape[0]
    out = w2_ref.shape[1]
    home = hub_ref.shape[1]
    block = hz_ref.shape[1]
    halo = groups * block
    hubr[me] = hub_ref[me]
    hzr[me] = jnp.zeros(hzr.shape[1:], F32)
    pl.semaphore_wait(barrier, groups - 1)
    hub_copies, halo_copies, back = [], [], []
    for step in range(1, groups):
        peer = lax.rem(me + step, groups)
        hub_copies.append(send(hub_ref.at[peer], hubr.at[me], ssem.at[0, step], rsem.at[0, step], peer))
    for step in range(1, groups):
        peer = lax.rem(me + step, groups)
        halo_copies.append(send(hz_ref.at[peer], hzr.at[me], ssem.at[1, step], rsem.at[1, step], peer))
    for copy in hub_copies:
        copy.wait()
    total = hubr[0]
    for q in range(1, groups):
        total = total + hubr[q]
    pre = total[:, :HID] + b1_ref[...]
    dz2h = total[:, HID:].astype(BF16)
    h1h_ref[...] = jnp.maximum(pre, 0.0).astype(BF16)
    dz2h_ref[...] = dz2h
    dys[...] = jnp.where(pre > 0, dot(dz2h[:, :out], w2_ref[...], CONTRACT_COLS), 0.0)
    for step in range(1, groups):
        peer = lax.rem(me + step, groups)
        back.append(send(dys, dyr.at[me], ssem.at[2, step], rsem.at[2, step], peer))
    dyr[me] = dys[...]
    for copy in halo_copies:
        copy.wait()
    pieces = split3(hzr[...].reshape(halo, LANES))
    sendrow = sendrow_ref[...]
    for row in range(0, nodes, CHUNK):
        onehot = (iota((CHUNK, halo), 0) + row == sendrow).astype(BF16)
        value = dz_ref[pl.ds(row, CHUNK), :]
        for piece in reversed(pieces):
            value = value + dot(onehot, piece)
        dz2_ref[pl.ds(row, CHUNK), :] = value.astype(BF16)
    for copy in back:
        copy.wait()
    for q in range(groups):
        dyh_ref[pl.ds(q * home, home), :] = dyr[q]


def edges_backward_kernel(copies, unroll, d4_ref, s4_ref, w_ref, hub_ref, h1_ref, dz2_ref, dyh_ref, w2_ref, h1h_ref, dz2h_ref, xh_ref, db2_ref,
                          dz1_ref, hz_ref, hub_out, dw2_ref, bias_ref, yt, *za):
    me = lax.axis_index("graph")
    nodes = h1_ref.shape[0]
    out = w2_ref.shape[1]
    halo, hubs = xh_ref.shape[0], dyh_ref.shape[0]
    home = h1h_ref.shape[0]
    feat = 50
    edges = w_ref.shape[0]
    base = me * nodes
    for acc in za:
        acc[...] = jnp.zeros_like(acc)
    w2 = w2_ref[...]
    mine = dyh_ref[pl.ds(pl.multiple_of(me * home, 8), home), :]
    db1 = mine
    for row in range(0, nodes, CHUNK):
        rows = pl.ds(row, CHUNK)
        grad = dot(dz2_ref[rows, pl.ds(0, out)], w2, CONTRACT_COLS)
        grad = jnp.where(h1_ref[rows, :] > 0, grad, 0.0)
        db1 = db1 + grad.reshape(CHUNK // 8, 8, HID).sum(axis=0)
        for c in range(TILES):
            yt[strided(row * TILES + c, CHUNK), :] = grad[:, c * LANES:(c + 1) * LANES]
    db1 = db1.sum(axis=0, keepdims=True)
    bias_ref[...] = db2_ref[...]
    for c in range(TILES):
        bias_ref[pl.ds(c, 1), :] = db1[:, c * LANES:(c + 1) * LANES]
        yt[strided(nodes * TILES + c, hubs), :] = dyh_ref[:, pl.ds(c * LANES, LANES)]
    dw2_ref[...] = dot(h1_ref[...], dz2_ref[...], CONTRACT_ROWS) + dot(h1h_ref[...], dz2h_ref[...], CONTRACT_ROWS)

    def place(k, carry):
        own, row = hub_position(hub_ref, k, base, nodes)
        here = pl.multiple_of((nodes + k) * TILES, TILES)
        yt[pl.ds(row, TILES), :] = jnp.where(own, yt[pl.ds(here, TILES), :], yt[pl.ds(row, TILES), :])
        return carry

    lax.fori_loop(0, hubs, place, 0)

    def step(i, carry):
        for u0 in range(0, unroll, copies):
            new = []
            for u in range(copies):
                j = i * unroll + u0 + u
                s4 = pl.multiple_of(s4_ref[j], TILES)
                d4 = pl.multiple_of(d4_ref[j], TILES)
                w = w_ref[j]
                new.append((s4, za[u][pl.ds(s4, TILES), :] + w * yt[pl.ds(d4, TILES), :]))
            for u, (s4, z_new) in enumerate(new):
                za[u][pl.ds(s4, TILES), :] = z_new
        return carry

    lax.fori_loop(0, edges // unroll, step, 0)

    def fold(k, carry):
        own, row = hub_position(hub_ref, k, base, nodes)
        here = pl.multiple_of((nodes + halo + k) * TILES, TILES)
        value = total_of(za, pl.ds(row, TILES))
        za[0][pl.ds(here, TILES), :] += jnp.where(own, value, 0.0)
        za[0][pl.ds(row, TILES), :] = jnp.where(own, 0.0, value)
        for acc in za[1:]:
            acc[pl.ds(row, TILES), :] = jnp.zeros((TILES, LANES), F32)
        return carry

    lax.fori_loop(0, hubs, fold, 0)
    for row in range(0, nodes, CHUNK):
        for c in range(TILES):
            dz1_ref[pl.ds(row, CHUNK), pl.ds(c * LANES, LANES)] = total_of(za, strided(row * TILES + c, CHUNK))
    tag = xh_ref[...].astype(F32)[:, feat:feat + 1]
    onehot = (tag == (iota((halo, hubs), 1) + 1).astype(F32)).astype(BF16)
    for c in range(TILES):
        cols = pl.ds(c * LANES, LANES)
        hz = total_of(za, strided(nodes * TILES + c, halo))
        hub_out[:, cols] = total_of(za, strided((nodes + halo) * TILES + c, hubs)) + select_rows(onehot, hz, CONTRACT_ROWS)
        hz_ref[:, cols] = jnp.where(tag > 0.0, 0.0, hz)


def final_kernel(groups, hz_ref, hub_ref, dw2_ref, bias_ref, dz1_ref, x_ref, hx_ref, w1_ref, sendrow_ref, hubrow_ref,
                 gx_ref, gw1_ref, gw2_ref, gb1_ref, gb2_ref,
                 hzr, hubr, dw2r, biasr, pieces, dw2s, dw2a, dxs, dxa, dw1s, dw1r, dw1t, dw1a, ssem, rsem):
    me = lax.axis_index("graph")
    barrier = greet(groups, me)
    nodes, feat = x_ref.shape
    home = hub_ref.shape[1]
    hubs = groups * home
    block = hz_ref.shape[1]
    halo = groups * block
    out = gw2_ref.shape[1]
    part = dw2_ref.shape[1]
    base = me * nodes
    hubr[me] = hub_ref[me]
    dw2r[me] = dw2_ref[me]
    biasr[me] = bias_ref[...]
    hzr[me] = jnp.zeros(hzr.shape[1:], F32)
    pl.semaphore_wait(barrier, groups - 1)
    peers = [lax.rem(me + step, groups) for step in range(1, groups)]

    def to_all(slot, src, dst):
        return [send(src(peer), dst.at[me], ssem.at[slot, i], rsem.at[slot, i], peer) for i, peer in enumerate(peers)]

    hub_copies = to_all(0, lambda p: hub_ref.at[p], hubr)
    dw2_copies = to_all(1, lambda p: dw2_ref.at[p], dw2r)
    bias_copies = to_all(2, lambda p: bias_ref, biasr)
    halo_copies = to_all(3, lambda p: hz_ref.at[p], hzr)
    w1 = w1_ref[...]
    for copy in hub_copies:
        copy.wait()
    total = hubr[0]
    for q in range(1, groups):
        total = total + hubr[q]
    dz1h = total.astype(BF16)
    dxs[...] = pad_lanes(dot(dz1h, w1, CONTRACT_COLS))
    dx_copies = to_all(4, lambda p: dxs, dxa)
    dxa[me] = dxs[...]
    hx_mine = hx_ref[pl.ds(pl.multiple_of(me * home, 8), home), :].astype(BF16)
    dw1h = dot(hx_mine[:, :feat], dz1h, CONTRACT_ROWS)
    for copy in dw2_copies:
        copy.wait()
    total = dw2r[0]
    for q in range(1, groups):
        total = total + dw2r[q]
    dw2s[...] = total
    dw2_back = to_all(5, lambda p: dw2s, dw2a)
    dw2a[me] = dw2s[...]
    for copy in bias_copies:
        copy.wait()
    total = biasr[0]
    for q in range(1, groups):
        total = total + biasr[q]
    for c in range(TILES):
        gb1_ref[:, pl.ds(c * LANES, LANES)] = total[c:c + 1, :]
    gb2_ref[...] = total[TILES:TILES + 1, :out]
    for copy in halo_copies:
        copy.wait()
    for q in range(groups):
        high, mid, low = split3(hzr[q])
        pieces[0, pl.ds(q * block, block), :] = low
        pieces[1, pl.ds(q * block, block), :] = mid
        pieces[2, pl.ds(q * block, block), :] = high
    for copy in dx_copies:
        copy.wait()
    dx_pieces = split3(dxa[...].reshape(hubs, LANES))
    sendrow = sendrow_ref[...]
    hubrow = hubrow_ref[...]
    dw1s[...] = jnp.zeros_like(dw1s)
    dw1s[pl.ds(0, feat), :] = dw1h

    def rows_step(i, carry):
        row = pl.multiple_of(i * CHUNK, CHUNK)
        rows = pl.ds(row, CHUNK)
        onehot = (iota((CHUNK, halo), 0) + row == sendrow).astype(BF16)
        value = dz1_ref[rows, :]
        for k in range(3):
            value = value + dot(onehot, pieces[k])
        dz1 = value.astype(BF16)
        owned = (iota((CHUNK, hubs), 0) + (base + row) == hubrow).astype(BF16)
        dx = jnp.zeros((CHUNK, LANES), F32)
        for piece in reversed(dx_pieces):
            dx = dx + dot(owned, piece)
        gx_ref[rows, :] = dot(dz1, w1, CONTRACT_COLS) + dx[:, :feat]
        dw1s[pl.ds(0, feat), :] += dot(x_ref[rows, :], dz1, CONTRACT_ROWS)
        return carry

    lax.fori_loop(0, nodes // CHUNK, rows_step, 0)
    dw1_copies = to_all(6, lambda p: dw1s.at[pl.ds(pl.multiple_of(p * 8, 8), 8)], dw1r)
    dw1r[me] = dw1s[pl.ds(pl.multiple_of(me * 8, 8), 8), :]
    for copy in dw2_back:
        copy.wait()
    for q in range(groups):
        gw2_ref[pl.ds(q * part, part), :] = dw2a[q][:, :out]
    for copy in dw1_copies:
        copy.wait()
    total = dw1r[0]
    for q in range(1, groups):
        total = total + dw1r[q]
    dw1t[...] = total
    dw1_back = to_all(7, lambda p: dw1t, dw1a)
    dw1a[me] = dw1t[...]
    for copy in dw1_back:
        copy.wait()
    for q in range(groups):
        rows = min(8, feat - q * 8)
        if rows > 0:
            gw1_ref[pl.ds(q * 8, rows), :] = dw1a[q][:rows, :]


def shape(dims, dtype):
    return jax.ShapeDtypeStruct(dims, dtype)


def solution(mesh):
    groups = mesh.shape["graph"]
    vertex_spec = P(("data", "graph"))
    vertex_rows = P(("data", "graph"), None)
    part_spec = P("data")
    part_rows = P("data", None)
    replicated = P()
    copies1, unroll1 = 3, 48
    copies2, unroll2 = 4, 64

    def params(collective_id=None):
        if collective_id is None:
            return pltpu.CompilerParams(vmem_limit_bytes=VMEM_LIMIT)
        return pltpu.CompilerParams(vmem_limit_bytes=VMEM_LIMIT, collective_id=collective_id, has_side_effects=True)

    def device_step(x_loc, dst_loc, src_loc, w_loc, send_loc, hub_ids, w_first, b_first, w_second, dy_out):
        nodes, feat = x_loc.shape
        edges = dst_loc.shape[0]
        halo = send_loc.shape[0]
        hubs = hub_ids.shape[0]
        out = dy_out.shape[1]
        block, home = halo // groups, hubs // groups
        src_rows, dst_rows = nodes + halo + hubs, nodes + hubs
        hub_lanes = hub_ids.reshape(1, hubs)
        send_lanes = send_loc.reshape(1, halo)
        bias = b_first.reshape(1, HID)
        sems = lambda n: [pltpu.SemaphoreType.DMA((n, groups)), pltpu.SemaphoreType.DMA((n, groups))]

        xh, hx, dhh, d4, s4, db2 = pl.pallas_call(
            functools.partial(gather_kernel, groups),
            name="gather_rows",
            out_shape=(shape((halo, LANES), BF16), shape((hubs, LANES), F32), shape((hubs, LANES), F32),
                       shape((edges // LANES, LANES), I32), shape((edges // LANES, LANES), I32), shape((8, LANES), F32)),
            in_specs=[VMEM, VMEM, SMEM, SMEM, VMEM, VMEM, VMEM],
            out_specs=(VMEM,) * 6,
            scratch_shapes=[pltpu.VMEM((nodes, LANES), F32), pltpu.VMEM((halo, LANES), F32), pltpu.VMEM((hubs, LANES), F32),
                            pltpu.VMEM((hubs, LANES), F32), pltpu.VMEM((groups, block + hubs, LANES), BF16),
                            pltpu.VMEM((groups, block + hubs, LANES), BF16), pltpu.VMEM((groups, hubs, LANES), F32)] + sems(2),
            compiler_params=params(0),
        )(x_loc, dy_out, send_loc, hub_ids, hub_lanes, dst_loc.reshape(edges // LANES, LANES), src_loc.reshape(edges // LANES, LANES))
        d4, s4 = d4.reshape(edges), s4.reshape(edges)
        pad1, pad2 = -edges % unroll1, -edges % unroll2
        grow = lambda a, n: jnp.pad(a, (0, n)) if n else a

        h1, dz, hz, hub = pl.pallas_call(
            functools.partial(edges_forward_kernel, copies1, unroll1),
            name="edges_forward",
            out_shape=(shape((nodes, HID), BF16), shape((nodes, LANES), F32), shape((halo, LANES), F32), shape((hubs, HID + LANES), F32)),
            in_specs=[SMEM] * 4 + [VMEM] * 7,
            out_specs=(VMEM,) * 4,
            scratch_shapes=[pltpu.VMEM((src_rows * TILES, LANES), F32), pltpu.VMEM((dst_rows * TILES, LANES), F32)]
            + [pltpu.VMEM((dst_rows * TILES, LANES), F32)] * copies1 + [pltpu.VMEM((src_rows * TILES, LANES), F32)] * copies1,
            compiler_params=params(),
        )(grow(d4, pad1), grow(s4, pad1), grow(w_loc, pad1), hub_ids, x_loc, xh, hx, dy_out, dhh, w_first, bias)

        dz2, dyh, h1h, dz2h = pl.pallas_call(
            functools.partial(middle_kernel, groups),
            name="middle",
            out_shape=(shape((nodes, LANES), BF16), shape((hubs, HID), F32), shape((home, HID), BF16), shape((home, LANES), BF16)),
            in_specs=[VMEM] * 6,
            out_specs=(VMEM,) * 4,
            scratch_shapes=[pltpu.VMEM((groups, block, LANES), F32), pltpu.VMEM((groups, home, HID + LANES), F32),
                            pltpu.VMEM((groups, home, HID), F32), pltpu.VMEM((home, HID), F32)] + sems(3),
            compiler_params=params(1),
        )(hz.reshape(groups, block, LANES), hub.reshape(groups, home, HID + LANES), dz, send_lanes, w_second, bias)

        dz1, hz1, hub1, dw2, biases = pl.pallas_call(
            functools.partial(edges_backward_kernel, copies2, unroll2),
            name="edges_backward",
            out_shape=(shape((nodes, HID), F32), shape((halo, HID), F32), shape((hubs, HID), F32), shape((HID, LANES), F32), shape((8, LANES), F32)),
            in_specs=[SMEM] * 4 + [VMEM] * 8,
            out_specs=(VMEM,) * 5,
            scratch_shapes=[pltpu.VMEM((dst_rows * TILES, LANES), F32)] + [pltpu.VMEM((src_rows * TILES, LANES), F32)] * copies2,
            compiler_params=params(),
        )(grow(d4, pad2), grow(s4, pad2), grow(w_loc, pad2), hub_ids, h1, dz2, dyh, w_second, h1h, dz2h, xh, db2)

        grad_x, grad_w1, grad_w2, grad_b1, grad_b2 = pl.pallas_call(
            functools.partial(final_kernel, groups),
            name="final",
            out_shape=(shape((nodes, feat), F32), shape((feat, HID), F32), shape((HID, out), F32), shape((1, HID), F32), shape((1, out), F32)),
            in_specs=[VMEM] * 10,
            out_specs=(VMEM,) * 5,
            scratch_shapes=[pltpu.VMEM((groups, block, HID), F32), pltpu.VMEM((groups, home, HID), F32),
                            pltpu.VMEM((groups, HID // groups, LANES), F32), pltpu.VMEM((groups, 8, LANES), F32),
                            pltpu.VMEM((3, halo, HID), BF16), pltpu.VMEM((HID // groups, LANES), F32),
                            pltpu.VMEM((groups, HID // groups, LANES), F32), pltpu.VMEM((home, LANES), F32),
                            pltpu.VMEM((groups, home, LANES), F32), pltpu.VMEM((groups * 8, HID), F32),
                            pltpu.VMEM((groups, 8, HID), F32), pltpu.VMEM((8, HID), F32), pltpu.VMEM((groups, 8, HID), F32)] + sems(8),
            compiler_params=params(2),
        )(hz1.reshape(groups, block, HID), hub1.reshape(groups, home, HID), dw2.reshape(groups, HID // groups, LANES), biases, dz1,
          x_loc, hx, w_first, send_lanes, hub_lanes)
        return grad_x, grad_w1, grad_w2, grad_b1.reshape(HID), grad_b2.reshape(out)

    return jax.shard_map(
        device_step,
        mesh=mesh,
        in_specs=(vertex_rows, vertex_spec, vertex_spec, vertex_spec, vertex_spec, part_spec, replicated, replicated, replicated, vertex_rows),
        out_specs=(vertex_rows, part_rows, part_rows, part_spec, part_spec),
        check_vma=False,
    )
```

```python
import functools

import jax
import jax.numpy as jnp
from jax import lax
from jax.experimental import pallas as pl
from jax.experimental.pallas import tpu as pltpu
from jax.sharding import PartitionSpec as P

F32, BF16, I32 = jnp.float32, jnp.bfloat16, jnp.int32
CONTRACT_ROWS = (((0,), (0,)), ((), ()))
CONTRACT_COLS = (((1,), (1,)), ((), ()))
LANES = 128
HID = 512
TILES = HID // LANES
CHUNK = 256
VMEM = pl.BlockSpec(memory_space=pltpu.VMEM)
SMEM = pl.BlockSpec(memory_space=pltpu.SMEM)


def dot(a, b, dims=(((1,), (0,)), ((), ()))):
    return lax.dot_general(a, b, dims, preferred_element_type=F32)


def iota(shape, dim):
    return lax.broadcasted_iota(I32, shape, dim)


def split3(value):
    high = value.astype(BF16)
    rest = value - high.astype(F32)
    mid = rest.astype(BF16)
    low = (rest - mid.astype(F32)).astype(BF16)
    return high, mid, low


def select_rows(onehot, value, dims=(((1,), (0,)), ((), ()))):
    high, mid, low = split3(value)
    return dot(onehot, low, dims) + dot(onehot, mid, dims) + dot(onehot, high, dims)


def pad_lanes(value):
    rows, cols = value.shape
    if cols == LANES:
        return value
    return jnp.concatenate([value, jnp.zeros((rows, LANES - cols), value.dtype)], axis=1)


def greet(groups, me):
    barrier = pltpu.get_barrier_semaphore()
    for step in range(1, groups):
        pl.semaphore_signal(barrier, inc=1, device_id={"graph": lax.rem(me + step, groups)}, device_id_type=pl.DeviceIdType.MESH)
    return barrier


def send(src, dst, send_sem, recv_sem, peer):
    copy = pltpu.make_async_remote_copy(
        src_ref=src, dst_ref=dst, send_sem=send_sem, recv_sem=recv_sem,
        device_id={"graph": peer}, device_id_type=pl.DeviceIdType.MESH)
    copy.start()
    return copy


def pack_rows(value):
    half = value.shape[0] // 2
    low = iota((half, LANES), 1) < LANES // 2
    return jnp.where(low, value[:half], pltpu.roll(value[half:], LANES // 2, 1)).astype(BF16)


def unpack_rows(value):
    return jnp.concatenate([value, pltpu.roll(value, LANES // 2, 1)], axis=0)


def gather_kernel(groups, xt_ref, dh_ref, send_ref, hub_ref, hubrow_ref, dst_ref, src_ref, w_ref,
                  xh_ref, hx_ref, dhh_ref, d4_ref, s4_ref, used_ref, db2_ref,
                  x32, xg, hxg, dhg, xs, xr, dhr, ssem, rsem):
    me = lax.axis_index("graph")
    barrier = greet(groups, me)
    feat, nodes = xt_ref.shape
    hubs = hub_ref.shape[0]
    halo = send_ref.shape[0]
    block = halo // groups
    base = me * nodes
    eye = (iota((feat, LANES), 0) == iota((feat, LANES), 1)).astype(BF16)
    tags = jnp.where(iota((hubs, LANES), 1) == feat, iota((hubs, LANES), 0) + 1, 0).astype(F32).astype(BF16)
    hubrow = hubrow_ref[...]
    for row in range(0, nodes, CHUNK):
        owned = (iota((CHUNK, hubs), 0) + (base + row) == hubrow).astype(BF16)
        x32[pl.ds(row, CHUNK), :] = dot(xt_ref[:, pl.ds(row, CHUNK)], eye, CONTRACT_ROWS) + dot(owned, tags)

    def pick(i, carry):
        for u in range(16):
            j = i * 16 + u
            xg[pl.ds(j, 1), :] = x32[pl.ds(send_ref[j], 1), :]
        return carry

    lax.fori_loop(0, halo // 16, pick, 0)
    dhg[...] = jnp.zeros_like(dhg)

    def pick_hub(i, carry):
        for u in range(8):
            k = i * 8 + u
            row = hub_ref[k] - base
            own = jnp.logical_and(row >= 0, row < nodes)
            row = jnp.clip(row, 0, nodes - 1)
            hxg[pl.ds(k, 1), :] = jnp.where(own, x32[pl.ds(row, 1), :], 0.0)
            value = dh_ref[pl.ds(row, 1), :]
            dhg[pl.ds(k, 1), pl.ds(0, value.shape[1])] = jnp.where(own, value, 0.0)
        return carry

    lax.fori_loop(0, hubs // 8, pick_hub, 0)
    hub_rows = pack_rows(hxg[...])
    for q in range(groups):
        xs[q, pl.ds(0, block // 2), :] = pack_rows(xg[pl.ds(q * block, block), :])
        xs[q, pl.ds(block // 2, hubs // 2), :] = hub_rows
    pl.semaphore_wait(barrier, groups - 1)
    copies = []
    for step in range(1, groups):
        peer = lax.rem(me + step, groups)
        copies.append(send(xs.at[peer], xr.at[me], ssem.at[0, step], rsem.at[0, step], peer))
        copies.append(send(dhg, dhr.at[me], ssem.at[1, step], rsem.at[1, step], peer))
    d4_ref[...] = dst_ref[...] * TILES
    s4_ref[...] = src_ref[...] * TILES
    used = jnp.where(w_ref[...] > 0.0, 1.0, 0.0).sum(axis=0, keepdims=True).sum(axis=1, keepdims=True)
    used_ref[...] = jnp.broadcast_to(used, used_ref.shape).astype(I32)
    total = jnp.zeros((8, dh_ref.shape[1]), F32)
    for row in range(0, nodes, CHUNK):
        total = total + dh_ref[pl.ds(row, CHUNK), :].reshape(CHUNK // 8, 8, dh_ref.shape[1]).sum(axis=0)
    db2_ref[...] = jnp.broadcast_to(pad_lanes(total.sum(axis=0, keepdims=True)), db2_ref.shape)
    xr[me] = xs[me]
    dhr[me] = dhg[...]
    for copy in copies:
        copy.wait()
    hx = jnp.zeros((hubs // 2, LANES), F32)
    dhh = jnp.zeros((hubs, LANES), F32)
    for q in range(groups):
        xh_ref[pl.ds(q * block, block), :] = unpack_rows(xr[q, pl.ds(0, block // 2), :].astype(F32)).astype(BF16)
        hx = hx + xr[q, pl.ds(block // 2, hubs // 2), :].astype(F32)
        dhh = dhh + dhr[q]
    hx_ref[...] = unpack_rows(hx)
    dhh_ref[...] = dhh


def hub_position(hub_ref, k, base, nodes):
    row = hub_ref[k] - base
    own = jnp.logical_and(row >= 0, row < nodes)
    return own, pl.multiple_of(jnp.clip(row, 0, nodes - 1) * TILES, TILES)


def strided(first, rows):
    return pl.ds(first, rows, stride=TILES)


def total_of(refs, where):
    value = refs[0][where, :]
    for ref in refs[1:]:
        value = value + ref[where, :]
    return value


def edges_forward_kernel(copies, unroll, d4_ref, s4_ref, w_ref, hub_ref, used_ref, xt_ref, xh_ref, hx_ref, dh_ref, dhh_ref, w1_ref, b1_ref,
                         h1_ref, dz_ref, hz_ref, hub_out, zt, dt, *accs):
    ya, da = accs[:copies], accs[copies:]
    me = lax.axis_index("graph")
    feat, nodes = xt_ref.shape
    halo, hubs = xh_ref.shape[0], hx_ref.shape[0]
    base = me * nodes
    for acc in ya:
        acc[...] = jnp.zeros_like(acc)
    for acc in da:
        acc[strided(0, nodes + halo + hubs), :] = jnp.zeros((nodes + halo + hubs, LANES), F32)
    w1 = w1_ref[...]

    def put_rows(first, z):
        z = z.astype(BF16).astype(F32)
        for c in range(TILES):
            zt[strided(first * TILES + c, z.shape[0]), :] = z[:, c * LANES:(c + 1) * LANES]

    for row in range(0, nodes, CHUNK):
        put_rows(row, dot(xt_ref[:, pl.ds(row, CHUNK)], w1, CONTRACT_ROWS))
        dt[strided(row * TILES, CHUNK), :] = pad_lanes(dh_ref[pl.ds(row, CHUNK), :])
    for row in range(0, halo, CHUNK):
        put_rows(nodes + row, dot(xh_ref[pl.ds(row, CHUNK), pl.ds(0, feat)], w1))
    put_rows(nodes + halo, dot(hx_ref[:, pl.ds(0, feat)].astype(BF16), w1))
    dt[strided(nodes * TILES, hubs), :] = dhh_ref[...]

    def step(i, carry):
        for u0 in range(0, unroll, copies):
            new = []
            for u in range(min(copies, unroll - u0)):
                j = i * unroll + u0 + u
                s4 = pl.multiple_of(s4_ref[j], TILES)
                d4 = pl.multiple_of(d4_ref[j], TILES)
                w = w_ref[j]
                new.append((s4, d4, ya[u][pl.ds(d4, TILES), :] + w * zt[pl.ds(s4, TILES), :],
                            da[u][pl.ds(s4, 1), :] + w * dt[pl.ds(d4, 1), :]))
            for u, (s4, d4, y_new, z_new) in enumerate(new):
                ya[u][pl.ds(d4, TILES), :] = y_new
                da[u][pl.ds(s4, 1), :] = z_new
        return carry

    lax.fori_loop(0, (used_ref[0, 0] + (unroll - 1)) // unroll, step, 0)

    def fold(k, carry):
        own, row = hub_position(hub_ref, k, base, nodes)
        here = pl.multiple_of((nodes + k) * TILES, TILES)
        ya[0][pl.ds(here, TILES), :] += jnp.where(own, total_of(ya, pl.ds(row, TILES)), 0.0)
        here = (nodes + halo + k) * TILES
        value = total_of(da, pl.ds(row, 1))
        da[0][pl.ds(here, 1), :] += jnp.where(own, value, 0.0)
        da[0][pl.ds(row, 1), :] = jnp.where(own, 0.0, value)
        for acc in da[1:]:
            acc[pl.ds(row, 1), :] = jnp.zeros((1, LANES), F32)
        return carry

    lax.fori_loop(0, hubs, fold, 0)
    for row in range(0, nodes, CHUNK):
        for c in range(TILES):
            cols = pl.ds(c * LANES, LANES)
            y = total_of(ya, strided(row * TILES + c, CHUNK)) + b1_ref[:, cols]
            h1_ref[pl.ds(row, CHUNK), cols] = jnp.maximum(y, 0.0).astype(BF16)
        dz_ref[pl.ds(row, CHUNK), :] = total_of(da, strided(row * TILES, CHUNK))
    hz = total_of(da, strided(nodes * TILES, halo))
    tag = xh_ref[...].astype(F32)[:, feat:feat + 1]
    onehot = (tag == (iota((halo, hubs), 1) + 1).astype(F32)).astype(BF16)
    hub_z = total_of(da, strided((nodes + halo) * TILES, hubs)) + select_rows(onehot, hz, CONTRACT_ROWS)
    hz_ref[...] = jnp.where(tag > 0.0, 0.0, hz)
    for c in range(TILES):
        hub_out[:, pl.ds(c * LANES, LANES)] = total_of(ya, strided(nodes * TILES + c, hubs))
    hub_out[:, pl.ds(HID, LANES)] = hub_z


def middle_kernel(groups, hz_ref, hub_ref, dz_ref, sendrow_ref, w2_ref, b1_ref,
                  dz2_ref, dyh_ref, h1h_ref, dz2h_ref,
                  hzr, hubr, dyr, dys, ssem, rsem):
    me = lax.axis_index("graph")
    barrier = greet(groups, me)
    nodes = dz_ref.shape[0]
    out = w2_ref.shape[1]
    home = hub_ref.shape[1]
    block = hz_ref.shape[1]
    halo = groups * block
    hubr[me] = hub_ref[me]
    hzr[me] = jnp.zeros(hzr.shape[1:], F32)
    pl.semaphore_wait(barrier, groups - 1)
    hub_copies, halo_copies, back = [], [], []
    for step in range(1, groups):
        peer = lax.rem(me + step, groups)
        hub_copies.append(send(hub_ref.at[peer], hubr.at[me], ssem.at[0, step], rsem.at[0, step], peer))
    for step in range(1, groups):
        peer = lax.rem(me + step, groups)
        halo_copies.append(send(hz_ref.at[peer], hzr.at[me], ssem.at[1, step], rsem.at[1, step], peer))
    for copy in hub_copies:
        copy.wait()
    total = hubr[0]
    for q in range(1, groups):
        total = total + hubr[q]
    pre = total[:, :HID] + b1_ref[...]
    dz2h = total[:, HID:].astype(BF16)
    h1h_ref[...] = jnp.maximum(pre, 0.0).astype(BF16)
    dz2h_ref[...] = dz2h
    dys[...] = jnp.where(pre > 0, dot(dz2h[:, :out], w2_ref[...], CONTRACT_COLS), 0.0)
    for step in range(1, groups):
        peer = lax.rem(me + step, groups)
        back.append(send(dys, dyr.at[me], ssem.at[2, step], rsem.at[2, step], peer))
    dyr[me] = dys[...]
    for copy in halo_copies:
        copy.wait()
    pieces = split3(hzr[...].reshape(halo, LANES))
    sendrow = sendrow_ref[...]
    for row in range(0, nodes, CHUNK):
        onehot = (iota((CHUNK, halo), 0) + row == sendrow).astype(BF16)
        value = dz_ref[pl.ds(row, CHUNK), :]
        for piece in reversed(pieces):
            value = value + dot(onehot, piece)
        dz2_ref[pl.ds(row, CHUNK), :] = value.astype(BF16)
    for copy in back:
        copy.wait()
    for q in range(groups):
        dyh_ref[pl.ds(q * home, home), :] = dyr[q]


def edges_backward_kernel(copies, unroll, feat, d4_ref, s4_ref, w_ref, hub_ref, used_ref, h1_ref, dz2_ref, dyh_ref, w2_ref, h1h_ref, dz2h_ref, xh_ref, db2_ref,
                          dz1_ref, hz_ref, hub_out, dw2_ref, bias_ref, yt, *za):
    me = lax.axis_index("graph")
    nodes = h1_ref.shape[0]
    out = w2_ref.shape[1]
    halo, hubs = xh_ref.shape[0], dyh_ref.shape[0]
    home = h1h_ref.shape[0]
    base = me * nodes
    for acc in za:
        acc[...] = jnp.zeros_like(acc)
    w2 = w2_ref[...]
    mine = dyh_ref[pl.ds(pl.multiple_of(me * home, 8), home), :]
    db1 = mine
    for row in range(0, nodes, CHUNK):
        rows = pl.ds(row, CHUNK)
        grad = dot(dz2_ref[rows, pl.ds(0, out)], w2, CONTRACT_COLS)
        grad = jnp.where(h1_ref[rows, :] > 0, grad, 0.0)
        db1 = db1 + grad.reshape(CHUNK // 8, 8, HID).sum(axis=0)
        for c in range(TILES):
            yt[strided(row * TILES + c, CHUNK), :] = grad[:, c * LANES:(c + 1) * LANES]
    db1 = db1.sum(axis=0, keepdims=True)
    bias_ref[...] = db2_ref[...]
    for c in range(TILES):
        bias_ref[pl.ds(c, 1), :] = db1[:, c * LANES:(c + 1) * LANES]
        yt[strided(nodes * TILES + c, hubs), :] = dyh_ref[:, pl.ds(c * LANES, LANES)]
    dw2_ref[...] = dot(h1_ref[...], dz2_ref[...], CONTRACT_ROWS) + dot(h1h_ref[...], dz2h_ref[...], CONTRACT_ROWS)

    def place(k, carry):
        own, row = hub_position(hub_ref, k, base, nodes)
        here = pl.multiple_of((nodes + k) * TILES, TILES)
        yt[pl.ds(row, TILES), :] = jnp.where(own, yt[pl.ds(here, TILES), :], yt[pl.ds(row, TILES), :])
        return carry

    lax.fori_loop(0, hubs, place, 0)

    def step(i, carry):
        for u0 in range(0, unroll, copies):
            new = []
            for u in range(copies):
                j = i * unroll + u0 + u
                s4 = pl.multiple_of(s4_ref[j], TILES)
                d4 = pl.multiple_of(d4_ref[j], TILES)
                w = w_ref[j]
                new.append((s4, za[u][pl.ds(s4, TILES), :] + w * yt[pl.ds(d4, TILES), :]))
            for u, (s4, z_new) in enumerate(new):
                za[u][pl.ds(s4, TILES), :] = z_new
        return carry

    lax.fori_loop(0, (used_ref[0, 0] + (unroll - 1)) // unroll, step, 0)

    def fold(k, carry):
        own, row = hub_position(hub_ref, k, base, nodes)
        here = pl.multiple_of((nodes + halo + k) * TILES, TILES)
        value = total_of(za, pl.ds(row, TILES))
        za[0][pl.ds(here, TILES), :] += jnp.where(own, value, 0.0)
        za[0][pl.ds(row, TILES), :] = jnp.where(own, 0.0, value)
        for acc in za[1:]:
            acc[pl.ds(row, TILES), :] = jnp.zeros((TILES, LANES), F32)
        return carry

    lax.fori_loop(0, hubs, fold, 0)
    for row in range(0, nodes, CHUNK):
        for c in range(TILES):
            dz1_ref[pl.ds(row, CHUNK), pl.ds(c * LANES, LANES)] = total_of(za, strided(row * TILES + c, CHUNK))
    tag = xh_ref[...].astype(F32)[:, feat:feat + 1]
    onehot = (tag == (iota((halo, hubs), 1) + 1).astype(F32)).astype(BF16)
    for c in range(TILES):
        cols = pl.ds(c * LANES, LANES)
        hz = total_of(za, strided(nodes * TILES + c, halo))
        hub_out[:, cols] = total_of(za, strided((nodes + halo) * TILES + c, hubs)) + select_rows(onehot, hz, CONTRACT_ROWS)
        hz_ref[c] = jnp.where(tag > 0.0, 0.0, hz)


def last_kernel(groups, hz_ref, hub_ref, dw2_ref, bias_ref, dz1_ref, xt_ref, sendrow_ref, hubrow_ref,
                dz_out, dw1a, dw2a, bias_out,
                hzr, hubr, biasr, dhs, dha, dw2p, dw2h, dw2r, dw2s, dw1s, dw1r, dw1t, ssem, rsem):
    me = lax.axis_index("graph")
    barrier = greet(groups, me)
    feat, nodes = xt_ref.shape
    home = hub_ref.shape[1]
    hubs = groups * home
    block = hz_ref.shape[2]
    halo = groups * block
    base = me * nodes
    core = lax.rem(me, 2)
    partner = me + 1 - 2 * core
    chip = me // 2
    chips = groups // 2
    part = dw2_ref.shape[2]
    hubr[me] = hub_ref[me]
    biasr[me] = bias_ref[...]
    for c in range(TILES):
        hzr[c, me] = jnp.zeros((block, LANES), F32)
        dw1s[c] = jnp.zeros(dw1s.shape[1:], F32)
    pl.semaphore_wait(barrier, groups - 1)
    peers = [lax.rem(me + step, groups) for step in range(1, groups)]
    others = [lax.rem(me + 2 * step, groups) for step in range(1, chips)]

    def to(devices, slot, src, dst):
        return [send(src(peer), dst, ssem.at[slot, i], rsem.at[slot, i], peer) for i, peer in enumerate(devices)]

    def wait(pending):
        for copy in pending:
            copy.wait()

    hub_copies = to(peers, 0, lambda p: hub_ref.at[p], hubr.at[me])
    pair_copies = to([partner], 1, lambda p: dw2_ref.at[1 - core], dw2p)
    halo_copies = [to(peers, 5 + c, lambda p: hz_ref.at[c, p], hzr.at[c, me]) for c in range(2)]
    wait(hub_copies)
    total = hubr[0]
    for q in range(1, groups):
        total = total + hubr[q]
    dhs[...] = total.astype(BF16).astype(F32)
    back_copies = to(peers, 3, lambda p: dhs, dha.at[me])
    dha[me] = dhs[...]
    wait(pair_copies)
    dw2h[...] = dw2_ref[core] + dw2p[...]
    dw2r[chip] = dw2h[chip]
    dw2_copies = to(others, 2, lambda p: dw2h.at[p // 2], dw2r.at[chip])
    halo_copies += [to(peers, 5 + c, lambda p: hz_ref.at[c, p], hzr.at[c, me]) for c in range(2, TILES)]
    bias_copies = to(peers, 4, lambda p: bias_ref, biasr.at[me])
    sendrow = sendrow_ref[...]
    hubrow = hubrow_ref[...]
    wait(back_copies)
    hub_rows = dha[...].reshape(hubs, HID).astype(BF16)
    rs_copies, ag_copies = [None] * TILES, [None] * TILES

    def spread(c):
        wait(rs_copies[c])
        total = dw1r[c, 0]
        for q in range(1, groups):
            total = total + dw1r[c, q]
        dw1t[c] = total
        ag_copies[c] = to(peers, 13 + c, lambda p: dw1t.at[c], dw1a.at[c, me])
        dw1a[c, me] = total

    for c in range(TILES):
        wait(halo_copies[c])
        cols = pl.ds(c * LANES, LANES)
        pieces = split3(hzr[c].reshape(halo, LANES))
        hub_cols = hub_rows[:, c * LANES:(c + 1) * LANES]

        def rows_step(i, carry):
            row = pl.multiple_of(i * CHUNK, CHUNK)
            rows = pl.ds(row, CHUNK)
            onehot = (iota((CHUNK, halo), 0) + row == sendrow).astype(BF16)
            owned = (iota((CHUNK, hubs), 0) + (base + row) == hubrow).astype(BF16)
            value = dz1_ref[rows, cols] + dot(owned, hub_cols)
            for piece in reversed(pieces):
                value = value + dot(onehot, piece)
            dz_out[rows, cols] = value.astype(BF16)
            return carry

        lax.fori_loop(0, nodes // CHUNK, rows_step, 0)
        dw1s[c, pl.ds(0, feat), :] = dot(xt_ref[...], dz_out[:, cols])
        rs_copies[c] = to(peers, 9 + c, lambda p: dw1s.at[c, pl.ds(pl.multiple_of(p * 8, 8), 8)], dw1r.at[c, me])
        dw1r[c, me] = dw1s[c, pl.ds(pl.multiple_of(me * 8, 8), 8), :]
        if c == 0:
            wait(dw2_copies)
            total = dw2r[0]
            for q in range(1, chips):
                total = total + dw2r[q]
            dw2s[...] = total
            dw2_back = to(peers, 17, lambda p: dw2s, dw2a.at[core, chip])
            dw2a[core, chip] = total
        if c > 0:
            spread(c - 1)
    wait(bias_copies)
    total = biasr[0]
    for q in range(1, groups):
        total = total + biasr[q]
    bias_out[...] = total
    spread(TILES - 1)
    wait(dw2_back)
    for c in range(TILES):
        wait(ag_copies[c])


def outputs_kernel(dz_ref, w1_ref, dw1_ref, dw2_ref, bias_ref, gxt_ref, gw1_ref, gw2_ref, gb1_ref, gb2_ref):
    nodes = dz_ref.shape[0]
    feat = w1_ref.shape[0]
    out = gw2_ref.shape[1]
    w1 = w1_ref[...]
    for row in range(0, nodes, 2 * CHUNK):
        rows = pl.ds(row, 2 * CHUNK)
        gxt_ref[:, rows] = dot(w1, dz_ref[rows, :], CONTRACT_COLS)
    for c in range(TILES):
        cols = pl.ds(c * LANES, LANES)
        for q in range(dw1_ref.shape[1]):
            rows = min(8, feat - q * 8)
            if rows > 0:
                gw1_ref[pl.ds(q * 8, rows), cols] = dw1_ref[c, q, pl.ds(0, rows), :]
        gb1_ref[:, cols] = bias_ref[pl.ds(c, 1), :]
    gw2_ref[...] = dw2_ref[:, pl.ds(0, out)]
    gb2_ref[...] = bias_ref[pl.ds(TILES, 1), pl.ds(0, out)]


def shape(dims, dtype):
    return jax.ShapeDtypeStruct(dims, dtype)


def solution(mesh):
    groups = mesh.shape["graph"]
    vertex_spec = P(("data", "graph"))
    vertex_rows = P(("data", "graph"), None)
    part_spec = P("data")
    part_rows = P("data", None)
    replicated = P()
    copies1, unroll1 = 3, 64
    copies2, unroll2 = 4, 64

    def params(mib, collective_id=None):
        if collective_id is None:
            return pltpu.CompilerParams(vmem_limit_bytes=mib * 2**20)
        return pltpu.CompilerParams(vmem_limit_bytes=mib * 2**20, collective_id=collective_id, has_side_effects=True)

    def device_step(x_loc, dst_loc, src_loc, w_loc, send_loc, hub_ids, w_first, b_first, w_second, dy_out):
        nodes, feat = x_loc.shape
        edges = dst_loc.shape[0]
        halo = send_loc.shape[0]
        hubs = hub_ids.shape[0]
        out = dy_out.shape[1]
        block, home = halo // groups, hubs // groups
        src_rows, dst_rows = nodes + halo + hubs, nodes + hubs
        x_t = x_loc.T
        hub_lanes = hub_ids.reshape(1, hubs)
        send_lanes = send_loc.reshape(1, halo)
        bias = b_first.reshape(1, HID)
        sems = lambda n: [pltpu.SemaphoreType.DMA((n, groups)), pltpu.SemaphoreType.DMA((n, groups))]
        table = lambda a: a.reshape(edges // LANES, LANES)
        rows = (edges // LANES, LANES)
        packed = (block + hubs) // 2

        xh, hx, dhh, d4, s4, used, db2 = pl.pallas_call(
            functools.partial(gather_kernel, groups),
            name="gather_rows",
            out_shape=(shape((halo, LANES), BF16), shape((hubs, LANES), F32), shape((hubs, LANES), F32),
                       shape(rows, I32), shape(rows, I32), shape((8, LANES), I32), shape((8, LANES), F32)),
            in_specs=[VMEM, VMEM, SMEM, SMEM, VMEM, VMEM, VMEM, VMEM],
            out_specs=(VMEM,) * 7,
            scratch_shapes=[pltpu.VMEM((nodes, LANES), F32), pltpu.VMEM((halo, LANES), F32), pltpu.VMEM((hubs, LANES), F32),
                            pltpu.VMEM((hubs, LANES), F32), pltpu.VMEM((groups, packed, LANES), BF16),
                            pltpu.VMEM((groups, packed, LANES), BF16), pltpu.VMEM((groups, hubs, LANES), F32)] + sems(2),
            compiler_params=params(16, 0),
        )(x_t, dy_out, send_loc, hub_ids, hub_lanes, table(dst_loc), table(src_loc), table(w_loc))
        d4, s4 = d4.reshape(edges), s4.reshape(edges)

        h1, dz, hz, hub = pl.pallas_call(
            functools.partial(edges_forward_kernel, copies1, unroll1),
            name="edges_forward",
            out_shape=(shape((nodes, HID), BF16), shape((nodes, LANES), F32), shape((halo, LANES), F32), shape((hubs, HID + LANES), F32)),
            in_specs=[SMEM] * 5 + [VMEM] * 7,
            out_specs=(VMEM,) * 4,
            scratch_shapes=[pltpu.VMEM((src_rows * TILES, LANES), F32), pltpu.VMEM((dst_rows * TILES, LANES), F32)]
            + [pltpu.VMEM((dst_rows * TILES, LANES), F32)] * copies1 + [pltpu.VMEM((src_rows * TILES, LANES), F32)] * copies1,
            compiler_params=params(50),
        )(d4, s4, w_loc, hub_ids, used, x_t, xh, hx, dy_out, dhh, w_first, bias)

        dz2, dyh, h1h, dz2h = pl.pallas_call(
            functools.partial(middle_kernel, groups),
            name="middle",
            out_shape=(shape((nodes, LANES), BF16), shape((hubs, HID), F32), shape((home, HID), BF16), shape((home, LANES), BF16)),
            in_specs=[VMEM] * 6,
            out_specs=(VMEM,) * 4,
            scratch_shapes=[pltpu.VMEM((groups, block, LANES), F32), pltpu.VMEM((groups, home, HID + LANES), F32),
                            pltpu.VMEM((groups, home, HID), F32), pltpu.VMEM((home, HID), F32)] + sems(3),
            compiler_params=params(12, 1),
        )(hz.reshape(groups, block, LANES), hub.reshape(groups, home, HID + LANES), dz, send_lanes, w_second, bias)

        dz1, hz1, hub1, dw2, biases = pl.pallas_call(
            functools.partial(edges_backward_kernel, copies2, unroll2, feat),
            name="edges_backward",
            out_shape=(shape((nodes, HID), F32), shape((TILES, halo, LANES), F32), shape((hubs, HID), F32), shape((HID, LANES), F32), shape((8, LANES), F32)),
            in_specs=[SMEM] * 5 + [VMEM] * 8,
            out_specs=(VMEM,) * 5,
            scratch_shapes=[pltpu.VMEM((dst_rows * TILES, LANES), F32)] + [pltpu.VMEM((src_rows * TILES, LANES), F32)] * copies2,
            compiler_params=params(44),
        )(d4, s4, w_loc, hub_ids, used, h1, dz2, dyh, w_second, h1h, dz2h, xh, db2)

        chips = groups // 2
        part = HID // groups
        dz1, dw1, dw2, biases = pl.pallas_call(
            functools.partial(last_kernel, groups),
            name="last_exchange",
            out_shape=(shape((nodes, HID), BF16), shape((TILES, groups, 8, LANES), F32), shape((2, chips, part, LANES), F32), shape((8, LANES), F32)),
            in_specs=[VMEM] * 8,
            out_specs=(VMEM,) * 4,
            scratch_shapes=[pltpu.VMEM((TILES, groups, block, LANES), F32), pltpu.VMEM((groups, home, HID), F32),
                            pltpu.VMEM((groups, 8, LANES), F32), pltpu.VMEM((home, HID), F32), pltpu.VMEM((groups, home, HID), F32),
                            pltpu.VMEM((chips, part, LANES), F32), pltpu.VMEM((chips, part, LANES), F32), pltpu.VMEM((chips, part, LANES), F32),
                            pltpu.VMEM((part, LANES), F32),
                            pltpu.VMEM((TILES, groups * 8, LANES), F32), pltpu.VMEM((TILES, groups, 8, LANES), F32), pltpu.VMEM((TILES, 8, LANES), F32)] + sems(18),
            compiler_params=params(20, 2),
        )(hz1.reshape(TILES, groups, block, LANES), hub1.reshape(groups, home, HID), dw2.reshape(2, chips, part, LANES), biases, dz1,
          x_t, send_lanes, hub_lanes)

        grad_xt, grad_w1, grad_w2, grad_b1, grad_b2 = pl.pallas_call(
            outputs_kernel,
            name="outputs",
            out_shape=(shape((feat, nodes), F32), shape((feat, HID), F32), shape((HID, out), F32), shape((1, HID), F32), shape((1, out), F32)),
            in_specs=[VMEM] * 5,
            out_specs=(VMEM,) * 5,
            compiler_params=params(12),
        )(dz1, w_first, dw1, dw2.reshape(HID, LANES), biases)
        return grad_xt.T, grad_w1, grad_w2, grad_b1.reshape(HID), grad_b2.reshape(out)

    return jax.shard_map(
        device_step,
        mesh=mesh,
        in_specs=(vertex_rows, vertex_spec, vertex_spec, vertex_spec, vertex_spec, part_spec, replicated, replicated, replicated, vertex_rows),
        out_specs=(vertex_rows, part_rows, part_rows, part_spec, part_spec),
        check_vma=False,
    )
```

```python
import functools

import jax
import jax.numpy as jnp
from jax import lax
from jax.experimental import pallas as pl
from jax.experimental.pallas import tpu as pltpu
from jax.sharding import PartitionSpec as P

F32, BF16, I32 = jnp.float32, jnp.bfloat16, jnp.int32
CONTRACT_ROWS = (((0,), (0,)), ((), ()))
CONTRACT_COLS = (((1,), (1,)), ((), ()))
LANES = 128
HID = 512
TILES = HID // LANES
CHUNK = 256
VMEM_LIMIT = 67043328
HBM = pl.BlockSpec(memory_space=pltpu.HBM)


class Fetched:
    def __init__(self, src, dst, sem):
        self.copy, self.ref, self.pending = pltpu.make_async_copy(src, dst, sem), dst, True
        self.copy.start()

    def get(self):
        if self.pending:
            self.copy.wait()
            self.pending = False
        return self.ref


def call(kernel, args, out_shape, scratch_shapes, name, compiler_params):
    spaces = {"vmem": pltpu.VMEM, "smem": pltpu.SMEM}
    in_buffers = [spaces[space](array.shape, array.dtype) for array, space in args]
    out_buffers = [pltpu.VMEM(out.shape, out.dtype) for out in out_shape]
    n_in, n_out = len(args), len(out_shape)

    def body(*refs):
        inputs, outputs = refs[:n_in], refs[n_in:n_in + n_out]
        bufs = refs[n_in + n_out:2 * n_in + 2 * n_out]
        scratch, sems, out_sems = refs[2 * n_in + 2 * n_out:-2], refs[-2], refs[-1]
        fetched = [Fetched(ref, bufs[n], sems.at[n]) for n, ref in enumerate(inputs)]
        results = bufs[n_in:]
        stores = {}

        def flush(*buffers):
            for buffer in buffers:
                n = [k for k in range(n_out) if results[k] is buffer][0]
                stores[n] = pltpu.make_async_copy(results[n], outputs[n], out_sems.at[n])
                stores[n].start()

        kernel(*fetched, *results, *scratch, flush=flush)
        for item in fetched:
            item.get()
        flush(*[results[n] for n in range(n_out) if n not in stores])
        for n in range(n_out):
            stores[n].wait()

    return pl.pallas_call(
        body,
        name=name,
        out_shape=out_shape,
        in_specs=[HBM] * n_in,
        out_specs=(HBM,) * n_out,
        scratch_shapes=in_buffers + out_buffers + list(scratch_shapes) + [pltpu.SemaphoreType.DMA((n_in,)), pltpu.SemaphoreType.DMA((n_out,))],
        compiler_params=compiler_params,
    )(*[array for array, _ in args])


def dot(a, b, dims=(((1,), (0,)), ((), ()))):
    return lax.dot_general(a, b, dims, preferred_element_type=F32)


def iota(shape, dim):
    return lax.broadcasted_iota(I32, shape, dim)


def split3(value):
    high = value.astype(BF16)
    rest = value - high.astype(F32)
    mid = rest.astype(BF16)
    low = (rest - mid.astype(F32)).astype(BF16)
    return high, mid, low


def select_rows(onehot, value, dims=(((1,), (0,)), ((), ()))):
    high, mid, low = split3(value)
    return dot(onehot, low, dims) + dot(onehot, mid, dims) + dot(onehot, high, dims)


def pad_lanes(value):
    rows, cols = value.shape
    if cols == LANES:
        return value
    return jnp.concatenate([value, jnp.zeros((rows, LANES - cols), value.dtype)], axis=1)


def greet(groups, me):
    barrier = pltpu.get_barrier_semaphore()
    for step in range(1, groups):
        pl.semaphore_signal(barrier, inc=1, device_id={"graph": lax.rem(me + step, groups)}, device_id_type=pl.DeviceIdType.MESH)
    return barrier


def send(src, dst, send_sem, recv_sem, peer):
    copy = pltpu.make_async_remote_copy(
        src_ref=src, dst_ref=dst, send_sem=send_sem, recv_sem=recv_sem,
        device_id={"graph": peer}, device_id_type=pl.DeviceIdType.MESH)
    copy.start()
    return copy


def pack_rows(value):
    half = value.shape[0] // 2
    low = iota((half, LANES), 1) < LANES // 2
    return jnp.where(low, value[:half], pltpu.roll(value[half:], LANES // 2, 1)).astype(BF16)


def unpack_rows(value):
    return jnp.concatenate([value, pltpu.roll(value, LANES // 2, 1)], axis=0)


def gather_kernel(groups, hubrow, xt, send_idx, hub_ids, dh, dst, src, w,
                  xh_ref, hx_ref, dhh_ref, d4_ref, s4_ref, used_ref, db2_ref,
                  x32, xg, hxg, dhg, xs, xr, dhr, ssem, rsem, flush):
    me = lax.axis_index("graph")
    barrier = greet(groups, me)
    feat, nodes = xt.ref.shape
    hubs = hub_ids.ref.shape[0]
    halo = send_idx.ref.shape[0]
    block = halo // groups
    base = me * nodes
    eye = (iota((feat, LANES), 0) == iota((feat, LANES), 1)).astype(BF16)
    tags = jnp.where(iota((hubs, LANES), 1) == feat, iota((hubs, LANES), 0) + 1, 0).astype(F32).astype(BF16)
    hubrow = hubrow.get()[...]
    xt_ref = xt.get()
    for row in range(0, nodes, CHUNK):
        owned = (iota((CHUNK, hubs), 0) + (base + row) == hubrow).astype(BF16)
        x32[pl.ds(row, CHUNK), :] = dot(xt_ref[:, pl.ds(row, CHUNK)], eye, CONTRACT_ROWS) + dot(owned, tags)

    send_ref = send_idx.get()

    def pick(i, carry):
        for u in range(16):
            j = i * 16 + u
            xg[pl.ds(j, 1), :] = x32[pl.ds(send_ref[j], 1), :]
        return carry

    lax.fori_loop(0, halo // 16, pick, 0)
    dhg[...] = jnp.zeros_like(dhg)
    hub_ref, dh_ref = hub_ids.get(), dh.get()

    def pick_hub(i, carry):
        for u in range(8):
            k = i * 8 + u
            row = hub_ref[k] - base
            own = jnp.logical_and(row >= 0, row < nodes)
            row = jnp.clip(row, 0, nodes - 1)
            hxg[pl.ds(k, 1), :] = jnp.where(own, x32[pl.ds(row, 1), :], 0.0)
            value = dh_ref[pl.ds(row, 1), :]
            dhg[pl.ds(k, 1), pl.ds(0, value.shape[1])] = jnp.where(own, value, 0.0)
        return carry

    lax.fori_loop(0, hubs // 8, pick_hub, 0)
    hub_rows = pack_rows(hxg[...])
    for q in range(groups):
        xs[q, pl.ds(0, block // 2), :] = pack_rows(xg[pl.ds(q * block, block), :])
        xs[q, pl.ds(block // 2, hubs // 2), :] = hub_rows
    pl.semaphore_wait(barrier, groups - 1)
    copies = []
    for step in range(1, groups):
        peer = lax.rem(me + step, groups)
        copies.append(send(xs.at[peer], xr.at[me], ssem.at[0, step], rsem.at[0, step], peer))
        copies.append(send(dhg, dhr.at[me], ssem.at[1, step], rsem.at[1, step], peer))
    d4_ref[...] = dst.get()[...] * TILES
    s4_ref[...] = src.get()[...] * TILES
    used = jnp.where(w.get()[...] > 0.0, 1.0, 0.0).sum(axis=0, keepdims=True).sum(axis=1, keepdims=True)
    used_ref[...] = jnp.broadcast_to(used, used_ref.shape).astype(I32)
    total = jnp.zeros((8, dh_ref.shape[1]), F32)
    for row in range(0, nodes, CHUNK):
        total = total + dh_ref[pl.ds(row, CHUNK), :].reshape(CHUNK // 8, 8, dh_ref.shape[1]).sum(axis=0)
    db2_ref[...] = jnp.broadcast_to(pad_lanes(total.sum(axis=0, keepdims=True)), db2_ref.shape)
    flush(d4_ref, s4_ref, used_ref, db2_ref)
    xr[me] = xs[me]
    dhr[me] = dhg[...]
    for copy in copies:
        copy.wait()
    hx = jnp.zeros((hubs // 2, LANES), F32)
    dhh = jnp.zeros((hubs, LANES), F32)
    for q in range(groups):
        xh_ref[pl.ds(q * block, block), :] = unpack_rows(xr[q, pl.ds(0, block // 2), :].astype(F32)).astype(BF16)
        hx = hx + xr[q, pl.ds(block // 2, hubs // 2), :].astype(F32)
        dhh = dhh + dhr[q]
    hx_ref[...] = unpack_rows(hx)
    dhh_ref[...] = dhh


def hub_position(hub_ref, k, base, nodes):
    row = hub_ref[k] - base
    own = jnp.logical_and(row >= 0, row < nodes)
    return own, pl.multiple_of(jnp.clip(row, 0, nodes - 1) * TILES, TILES)


def strided(first, rows):
    return pl.ds(first, rows, stride=TILES)


def total_of(refs, where):
    value = refs[0][where, :]
    for ref in refs[1:]:
        value = value + ref[where, :]
    return value


def edges_forward_kernel(copies, unroll, w1, xt, dh, xh, hx, dhh, d4, s4, w, used, hub_ids, b1,
                         h1_ref, dz_ref, hz_ref, hub_out, zt, dt, *accs, flush):
    ya, da = accs[:copies], accs[copies:]
    me = lax.axis_index("graph")
    feat, nodes = xt.ref.shape
    halo, hubs = xh.ref.shape[0], hx.ref.shape[0]
    base = me * nodes
    for acc in ya:
        acc[...] = jnp.zeros_like(acc)
    for acc in da:
        acc[strided(0, nodes + halo + hubs), :] = jnp.zeros((nodes + halo + hubs, LANES), F32)
    w1 = w1.get()[...]
    xt_ref, dh_ref, xh_ref, hx_ref = xt.get(), dh.get(), xh.get(), hx.get()

    def put_rows(first, z):
        z = z.astype(BF16).astype(F32)
        for c in range(TILES):
            zt[strided(first * TILES + c, z.shape[0]), :] = z[:, c * LANES:(c + 1) * LANES]

    for row in range(0, nodes, CHUNK):
        put_rows(row, dot(xt_ref[:, pl.ds(row, CHUNK)], w1, CONTRACT_ROWS))
        dt[strided(row * TILES, CHUNK), :] = pad_lanes(dh_ref[pl.ds(row, CHUNK), :])
    for row in range(0, halo, CHUNK):
        put_rows(nodes + row, dot(xh_ref[pl.ds(row, CHUNK), pl.ds(0, feat)], w1))
    put_rows(nodes + halo, dot(hx_ref[:, pl.ds(0, feat)].astype(BF16), w1))
    dt[strided(nodes * TILES, hubs), :] = dhh.get()[...]
    d4_ref, s4_ref, used_ref, w_ref, hub_ref, b1_ref = d4.get(), s4.get(), used.get(), w.get(), hub_ids.get(), b1.get()

    def step(i, carry):
        for u0 in range(0, unroll, copies):
            new = []
            for u in range(min(copies, unroll - u0)):
                j = i * unroll + u0 + u
                s4 = pl.multiple_of(s4_ref[j], TILES)
                d4 = pl.multiple_of(d4_ref[j], TILES)
                w = w_ref[j]
                new.append((s4, d4, ya[u][pl.ds(d4, TILES), :] + w * zt[pl.ds(s4, TILES), :],
                            da[u][pl.ds(s4, 1), :] + w * dt[pl.ds(d4, 1), :]))
            for u, (s4, d4, y_new, z_new) in enumerate(new):
                ya[u][pl.ds(d4, TILES), :] = y_new
                da[u][pl.ds(s4, 1), :] = z_new
        return carry

    lax.fori_loop(0, (used_ref[0, 0] + (unroll - 1)) // unroll, step, 0)

    def fold(k, carry):
        own, row = hub_position(hub_ref, k, base, nodes)
        here = pl.multiple_of((nodes + k) * TILES, TILES)
        ya[0][pl.ds(here, TILES), :] += jnp.where(own, total_of(ya, pl.ds(row, TILES)), 0.0)
        here = (nodes + halo + k) * TILES
        value = total_of(da, pl.ds(row, 1))
        da[0][pl.ds(here, 1), :] += jnp.where(own, value, 0.0)
        da[0][pl.ds(row, 1), :] = jnp.where(own, 0.0, value)
        for acc in da[1:]:
            acc[pl.ds(row, 1), :] = jnp.zeros((1, LANES), F32)
        return carry

    lax.fori_loop(0, hubs, fold, 0)
    for row in range(0, nodes, CHUNK):
        for c in range(TILES):
            cols = pl.ds(c * LANES, LANES)
            y = total_of(ya, strided(row * TILES + c, CHUNK)) + b1_ref[:, cols]
            h1_ref[pl.ds(row, CHUNK), cols] = jnp.maximum(y, 0.0).astype(BF16)
    flush(h1_ref)
    for row in range(0, nodes, CHUNK):
        dz_ref[pl.ds(row, CHUNK), :] = total_of(da, strided(row * TILES, CHUNK))
    flush(dz_ref)
    hz = total_of(da, strided(nodes * TILES, halo))
    tag = xh_ref[...].astype(F32)[:, feat:feat + 1]
    onehot = (tag == (iota((halo, hubs), 1) + 1).astype(F32)).astype(BF16)
    hub_z = total_of(da, strided((nodes + halo) * TILES, hubs)) + select_rows(onehot, hz, CONTRACT_ROWS)
    hz_ref[...] = jnp.where(tag > 0.0, 0.0, hz)
    for c in range(TILES):
        hub_out[:, pl.ds(c * LANES, LANES)] = total_of(ya, strided(nodes * TILES + c, hubs))
    hub_out[:, pl.ds(HID, LANES)] = hub_z


def middle_kernel(groups, hub, hz, dz, b1, w2, sendrow,
                  dz2_ref, dyh_ref, h1h_ref, dz2h_ref,
                  hzr, hubr, dyr, dys, ssem, rsem, flush):
    me = lax.axis_index("graph")
    barrier = greet(groups, me)
    nodes = dz.ref.shape[0]
    out = w2.ref.shape[1]
    home = hub.ref.shape[1]
    block = hz.ref.shape[1]
    halo = groups * block
    hub_ref, hz_ref = hub.get(), hz.get()
    hubr[me] = hub_ref[me]
    hzr[me] = jnp.zeros(hzr.shape[1:], F32)
    pl.semaphore_wait(barrier, groups - 1)
    hub_copies, halo_copies, back = [], [], []
    for step in range(1, groups):
        peer = lax.rem(me + step, groups)
        hub_copies.append(send(hub_ref.at[peer], hubr.at[me], ssem.at[0, step], rsem.at[0, step], peer))
    for step in range(1, groups):
        peer = lax.rem(me + step, groups)
        halo_copies.append(send(hz_ref.at[peer], hzr.at[me], ssem.at[1, step], rsem.at[1, step], peer))
    for copy in hub_copies:
        copy.wait()
    total = hubr[0]
    for q in range(1, groups):
        total = total + hubr[q]
    b1_ref, w2_ref, sendrow = b1.get(), w2.get(), sendrow.get()[...]
    pre = total[:, :HID] + b1_ref[...]
    dz2h = total[:, HID:].astype(BF16)
    h1h_ref[...] = jnp.maximum(pre, 0.0).astype(BF16)
    dz2h_ref[...] = dz2h
    dys[...] = jnp.where(pre > 0, dot(dz2h[:, :out], w2_ref[...], CONTRACT_COLS), 0.0)
    for step in range(1, groups):
        peer = lax.rem(me + step, groups)
        back.append(send(dys, dyr.at[me], ssem.at[2, step], rsem.at[2, step], peer))
    dyr[me] = dys[...]
    for copy in halo_copies:
        copy.wait()
    pieces = split3(hzr[...].reshape(halo, LANES))
    dz_ref = dz.get()
    for row in range(0, nodes, CHUNK):
        onehot = (iota((CHUNK, halo), 0) + row == sendrow).astype(BF16)
        value = dz_ref[pl.ds(row, CHUNK), :]
        for piece in reversed(pieces):
            value = value + dot(onehot, piece)
        dz2_ref[pl.ds(row, CHUNK), :] = value.astype(BF16)
    for copy in back:
        copy.wait()
    for q in range(groups):
        dyh_ref[pl.ds(q * home, home), :] = dyr[q]


def edges_backward_kernel(copies, unroll, feat, w2, h1, dz2, dyh, h1h, dz2h, d4, s4, w, used, hub_ids, xh, db2,
                          dz1_ref, hz_ref, hub_out, dw2_ref, bias_ref, yt, *za, flush):
    me = lax.axis_index("graph")
    nodes = h1.ref.shape[0]
    out = w2.ref.shape[1]
    halo, hubs = xh.ref.shape[0], dyh.ref.shape[0]
    home = h1h.ref.shape[0]
    base = me * nodes
    for acc in za:
        acc[...] = jnp.zeros_like(acc)
    w2, h1_ref, dz2_ref, dyh_ref, h1h_ref, dz2h_ref = w2.get()[...], h1.get(), dz2.get(), dyh.get(), h1h.get(), dz2h.get()
    mine = dyh_ref[pl.ds(pl.multiple_of(me * home, 8), home), :]
    db1 = mine
    for row in range(0, nodes, CHUNK):
        rows = pl.ds(row, CHUNK)
        grad = dot(dz2_ref[rows, pl.ds(0, out)], w2, CONTRACT_COLS)
        grad = jnp.where(h1_ref[rows, :] > 0, grad, 0.0)
        db1 = db1 + grad.reshape(CHUNK // 8, 8, HID).sum(axis=0)
        for c in range(TILES):
            yt[strided(row * TILES + c, CHUNK), :] = grad[:, c * LANES:(c + 1) * LANES]
    db1 = db1.sum(axis=0, keepdims=True)
    bias_ref[...] = db2.get()[...]
    for c in range(TILES):
        bias_ref[pl.ds(c, 1), :] = db1[:, c * LANES:(c + 1) * LANES]
        yt[strided(nodes * TILES + c, hubs), :] = dyh_ref[:, pl.ds(c * LANES, LANES)]
    dw2_ref[...] = dot(h1_ref[...], dz2_ref[...], CONTRACT_ROWS) + dot(h1h_ref[...], dz2h_ref[...], CONTRACT_ROWS)
    flush(dw2_ref, bias_ref)
    d4_ref, s4_ref, used_ref, w_ref, hub_ref, xh_ref = d4.get(), s4.get(), used.get(), w.get(), hub_ids.get(), xh.get()

    def place(k, carry):
        own, row = hub_position(hub_ref, k, base, nodes)
        here = pl.multiple_of((nodes + k) * TILES, TILES)
        yt[pl.ds(row, TILES), :] = jnp.where(own, yt[pl.ds(here, TILES), :], yt[pl.ds(row, TILES), :])
        return carry

    lax.fori_loop(0, hubs, place, 0)

    def step(i, carry):
        for u0 in range(0, unroll, copies):
            new = []
            for u in range(copies):
                j = i * unroll + u0 + u
                s4 = pl.multiple_of(s4_ref[j], TILES)
                d4 = pl.multiple_of(d4_ref[j], TILES)
                w = w_ref[j]
                new.append((s4, za[u][pl.ds(s4, TILES), :] + w * yt[pl.ds(d4, TILES), :]))
            for u, (s4, z_new) in enumerate(new):
                za[u][pl.ds(s4, TILES), :] = z_new
        return carry

    lax.fori_loop(0, (used_ref[0, 0] + (unroll - 1)) // unroll, step, 0)

    def fold(k, carry):
        own, row = hub_position(hub_ref, k, base, nodes)
        here = pl.multiple_of((nodes + halo + k) * TILES, TILES)
        value = total_of(za, pl.ds(row, TILES))
        za[0][pl.ds(here, TILES), :] += jnp.where(own, value, 0.0)
        za[0][pl.ds(row, TILES), :] = jnp.where(own, 0.0, value)
        for acc in za[1:]:
            acc[pl.ds(row, TILES), :] = jnp.zeros((TILES, LANES), F32)
        return carry

    lax.fori_loop(0, hubs, fold, 0)
    for row in range(0, nodes, CHUNK):
        for c in range(TILES):
            dz1_ref[pl.ds(row, CHUNK), pl.ds(c * LANES, LANES)] = total_of(za, strided(row * TILES + c, CHUNK))
    flush(dz1_ref)
    tag = xh_ref[...].astype(F32)[:, feat:feat + 1]
    onehot = (tag == (iota((halo, hubs), 1) + 1).astype(F32)).astype(BF16)
    for c in range(TILES):
        cols = pl.ds(c * LANES, LANES)
        hz = total_of(za, strided(nodes * TILES + c, halo))
        hub_out[:, cols] = total_of(za, strided((nodes + halo) * TILES + c, hubs)) + select_rows(onehot, hz, CONTRACT_ROWS)
        hz_ref[c] = jnp.where(tag > 0.0, 0.0, hz)


def last_kernel(groups, hub, hz, dw2, bias, sendrow, xt, hx, dz1,
                dz_out, dha, dw1a, dw2a, bias_out,
                onehot, hzr, hubr, biasr, dhs, dw2p, dw2h, dw2r, dw2s, dw1s, dw1r, dw1t, ssem, rsem, flush):
    me = lax.axis_index("graph")
    barrier = greet(groups, me)
    feat, nodes = xt.ref.shape
    home = hub.ref.shape[1]
    block = hz.ref.shape[2]
    halo = groups * block
    hub_ref, hz_ref, dw2_ref, bias_ref = hub.get(), hz.get(), dw2.get(), bias.get()
    core = lax.rem(me, 2)
    partner = me + 1 - 2 * core
    chip = me // 2
    chips = groups // 2
    part = dw2_ref.shape[2]
    hubr[me] = hub_ref[me]
    biasr[me] = bias_ref[...]
    for c in range(TILES):
        hzr[c, me] = jnp.zeros((block, LANES), F32)
        dw1s[c] = jnp.zeros(dw1s.shape[1:], F32)
    pl.semaphore_wait(barrier, groups - 1)
    peers = [lax.rem(me + step, groups) for step in range(1, groups)]
    others = [lax.rem(me + 2 * step, groups) for step in range(1, chips)]

    def to(devices, slot, src, dst):
        return [send(src(peer), dst, ssem.at[slot, i], rsem.at[slot, i], peer) for i, peer in enumerate(devices)]

    def wait(pending):
        for copy in pending:
            copy.wait()

    hub_copies = to(peers, 0, lambda p: hub_ref.at[p], hubr.at[me])
    pair_copies = to([partner], 1, lambda p: dw2_ref.at[1 - core], dw2p)
    halo_copies = [to(peers, 5 + c, lambda p: hz_ref.at[c, p], hzr.at[c, me]) for c in range(2)]
    wait(hub_copies)
    total = hubr[0]
    for q in range(1, groups):
        total = total + hubr[q]
    dz1h = total.astype(BF16)
    dhs[...] = dz1h
    back_copies = to(peers, 3, lambda p: dhs, dha.at[me])
    dha[me] = dhs[...]
    wait(pair_copies)
    dw2h[...] = dw2_ref[core] + dw2p[...]
    dw2r[chip] = dw2h[chip]
    dw2_copies = to(others, 2, lambda p: dw2h.at[p // 2], dw2r.at[chip])
    halo_copies += [to(peers, 5 + c, lambda p: hz_ref.at[c, p], hzr.at[c, me]) for c in range(2, TILES)]
    bias_copies = to(peers, 4, lambda p: bias_ref, biasr.at[me])
    hx_mine = hx.get()[pl.ds(pl.multiple_of(me * home, 8), home), :].astype(BF16)
    dw1h = dot(hx_mine[:, :feat], dz1h, CONTRACT_ROWS)
    sendrow, xt_ref, dz1_ref = sendrow.get()[...], xt.get(), dz1.get()
    for row in range(0, nodes, CHUNK):
        onehot[pl.ds(row, CHUNK), :] = (iota((CHUNK, halo), 0) + row == sendrow).astype(BF16)
    rs_copies, ag_copies = [None] * TILES, [None] * TILES

    def spread(c):
        wait(rs_copies[c])
        total = dw1r[c, 0]
        for q in range(1, groups):
            total = total + dw1r[c, q]
        dw1t[c] = total
        ag_copies[c] = to(peers, 13 + c, lambda p: dw1t.at[c], dw1a.at[c, me])
        dw1a[c, me] = total

    for c in range(TILES):
        wait(halo_copies[c])
        cols = pl.ds(c * LANES, LANES)
        pieces = jnp.concatenate(split3(hzr[c].reshape(halo, LANES)), axis=1)

        def rows_step(i, carry):
            rows = pl.ds(pl.multiple_of(i * CHUNK, CHUNK), CHUNK)
            value = dot(onehot[rows, :], pieces)
            value = value[:, 2 * LANES:] + value[:, LANES:2 * LANES] + value[:, :LANES]
            dz_out[rows, cols] = (dz1_ref[rows, cols] + value).astype(BF16)
            return carry

        lax.fori_loop(0, nodes // CHUNK, rows_step, 0)
        dw1s[c, pl.ds(0, feat), :] = dot(xt_ref[...], dz_out[:, cols]) + dw1h[:, c * LANES:(c + 1) * LANES]
        rs_copies[c] = to(peers, 9 + c, lambda p: dw1s.at[c, pl.ds(pl.multiple_of(p * 8, 8), 8)], dw1r.at[c, me])
        dw1r[c, me] = dw1s[c, pl.ds(pl.multiple_of(me * 8, 8), 8), :]
        if c == 0:
            wait(dw2_copies)
            total = dw2r[0]
            for q in range(1, chips):
                total = total + dw2r[q]
            dw2s[...] = total
            dw2_back = to(peers, 17, lambda p: dw2s, dw2a.at[core, chip])
            dw2a[core, chip] = total
        if c > 0:
            spread(c - 1)
    flush(dz_out)
    wait(bias_copies)
    total = biasr[0]
    for q in range(1, groups):
        total = total + biasr[q]
    bias_out[...] = total
    spread(TILES - 1)
    wait(dw2_back)
    wait(back_copies)
    for c in range(TILES):
        wait(ag_copies[c])


def outputs_kernel(w1, hubrow, dzh, dw1, dw2, bias, dz, gxt_ref, gw1_ref, gw2_ref, gb1_ref, gb2_ref, flush):
    nodes = dz.ref.shape[0]
    hubs = dzh.ref.shape[0]
    feat = w1.ref.shape[0]
    out = gw2_ref.shape[1]
    base = lax.axis_index("graph") * nodes
    w1, hubrow, dzh_ref, dz_ref = w1.get()[...], hubrow.get()[...], dzh.get(), dz.get()
    for row in range(0, nodes, 2 * CHUNK):
        rows = pl.ds(row, 2 * CHUNK)
        owned = (iota((2 * CHUNK, hubs), 0) + (base + row) == hubrow).astype(BF16)
        dz = (dz_ref[rows, :].astype(F32) + dot(owned, dzh_ref[...])).astype(BF16)
        gxt_ref[:, rows] = dot(w1, dz, CONTRACT_COLS)
    flush(gxt_ref)
    dw1_ref, dw2_ref, bias_ref = dw1.get(), dw2.get(), bias.get()
    for c in range(TILES):
        cols = pl.ds(c * LANES, LANES)
        for q in range(dw1_ref.shape[1]):
            rows = min(8, feat - q * 8)
            if rows > 0:
                gw1_ref[pl.ds(q * 8, rows), cols] = dw1_ref[c, q, pl.ds(0, rows), :]
        gb1_ref[:, cols] = bias_ref[pl.ds(c, 1), :]
    gw2_ref[...] = dw2_ref[:, pl.ds(0, out)]
    gb2_ref[...] = bias_ref[pl.ds(TILES, 1), pl.ds(0, out)]


def shape(dims, dtype):
    return jax.ShapeDtypeStruct(dims, dtype)


def solution(mesh):
    groups = mesh.shape["graph"]
    vertex_spec = P(("data", "graph"))
    vertex_rows = P(("data", "graph"), None)
    part_spec = P("data")
    part_rows = P("data", None)
    replicated = P()
    copies1, unroll1 = 3, 64
    copies2, unroll2 = 4, 64

    def params(collective_id=None):
        if collective_id is None:
            return pltpu.CompilerParams(vmem_limit_bytes=VMEM_LIMIT)
        return pltpu.CompilerParams(vmem_limit_bytes=VMEM_LIMIT, collective_id=collective_id, has_side_effects=True)

    def device_step(x_loc, dst_loc, src_loc, w_loc, send_loc, hub_ids, w_first, b_first, w_second, dy_out):
        nodes, feat = x_loc.shape
        edges = dst_loc.shape[0]
        halo = send_loc.shape[0]
        hubs = hub_ids.shape[0]
        out = dy_out.shape[1]
        block, home = halo // groups, hubs // groups
        src_rows, dst_rows = nodes + halo + hubs, nodes + hubs
        x_t = x_loc.T
        hub_lanes = hub_ids.reshape(1, hubs)
        send_lanes = send_loc.reshape(1, halo)
        bias = b_first.reshape(1, HID)
        sems = lambda n: [pltpu.SemaphoreType.DMA((n, groups)), pltpu.SemaphoreType.DMA((n, groups))]
        table = lambda a: a.reshape(edges // LANES, LANES)
        rows = (edges // LANES, LANES)
        packed = (block + hubs) // 2

        xh, hx, dhh, d4, s4, used, db2 = call(
            functools.partial(gather_kernel, groups),
            [(hub_lanes, "vmem"), (x_t, "vmem"), (send_loc, "smem"), (hub_ids, "smem"), (dy_out, "vmem"),
             (table(dst_loc), "vmem"), (table(src_loc), "vmem"), (table(w_loc), "vmem")],
            (shape((halo, LANES), BF16), shape((hubs, LANES), F32), shape((hubs, LANES), F32),
             shape(rows, I32), shape(rows, I32), shape((8, LANES), I32), shape((8, LANES), F32)),
            [pltpu.VMEM((nodes, LANES), F32), pltpu.VMEM((halo, LANES), F32), pltpu.VMEM((hubs, LANES), F32),
             pltpu.VMEM((hubs, LANES), F32), pltpu.VMEM((groups, packed, LANES), BF16),
             pltpu.VMEM((groups, packed, LANES), BF16), pltpu.VMEM((groups, hubs, LANES), F32)] + sems(2),
            "gather_rows", params(0))
        d4, s4 = d4.reshape(edges), s4.reshape(edges)

        h1, dz, hz, hub = call(
            functools.partial(edges_forward_kernel, copies1, unroll1),
            [(w_first, "vmem"), (x_t, "vmem"), (dy_out, "vmem"), (xh, "vmem"), (hx, "vmem"), (dhh, "vmem"),
             (d4, "smem"), (s4, "smem"), (w_loc, "smem"), (used, "smem"), (hub_ids, "smem"), (bias, "vmem")],
            (shape((nodes, HID), BF16), shape((nodes, LANES), F32), shape((halo, LANES), F32), shape((hubs, HID + LANES), F32)),
            [pltpu.VMEM((src_rows * TILES, LANES), F32), pltpu.VMEM((dst_rows * TILES, LANES), F32)]
            + [pltpu.VMEM((dst_rows * TILES, LANES), F32)] * copies1 + [pltpu.VMEM((src_rows * TILES, LANES), F32)] * copies1,
            "edges_forward", params())

        dz2, dyh, h1h, dz2h = call(
            functools.partial(middle_kernel, groups),
            [(hub.reshape(groups, home, HID + LANES), "vmem"), (hz.reshape(groups, block, LANES), "vmem"), (dz, "vmem"),
             (bias, "vmem"), (w_second, "vmem"), (send_lanes, "vmem")],
            (shape((nodes, LANES), BF16), shape((hubs, HID), F32), shape((home, HID), BF16), shape((home, LANES), BF16)),
            [pltpu.VMEM((groups, block, LANES), F32), pltpu.VMEM((groups, home, HID + LANES), F32),
             pltpu.VMEM((groups, home, HID), F32), pltpu.VMEM((home, HID), F32)] + sems(3),
            "middle", params(1))

        dz1, hz1, hub1, dw2, biases = call(
            functools.partial(edges_backward_kernel, copies2, unroll2, feat),
            [(w_second, "vmem"), (h1, "vmem"), (dz2, "vmem"), (dyh, "vmem"), (h1h, "vmem"), (dz2h, "vmem"),
             (d4, "smem"), (s4, "smem"), (w_loc, "smem"), (used, "smem"), (hub_ids, "smem"), (xh, "vmem"), (db2, "vmem")],
            (shape((nodes, HID), F32), shape((TILES, halo, LANES), F32), shape((hubs, HID), F32), shape((HID, LANES), F32), shape((8, LANES), F32)),
            [pltpu.VMEM((dst_rows * TILES, LANES), F32)] + [pltpu.VMEM((src_rows * TILES, LANES), F32)] * copies2,
            "edges_backward", params())

        chips = groups // 2
        part = HID // groups
        dz1, dz1h, dw1, dw2, biases = call(
            functools.partial(last_kernel, groups),
            [(hub1.reshape(groups, home, HID), "vmem"), (hz1.reshape(TILES, groups, block, LANES), "vmem"),
             (dw2.reshape(2, chips, part, LANES), "vmem"), (biases, "vmem"), (send_lanes, "vmem"), (x_t, "vmem"), (hx, "vmem"), (dz1, "vmem")],
            (shape((nodes, HID), BF16), shape((groups, home, HID), BF16), shape((TILES, groups, 8, LANES), F32),
             shape((2, chips, part, LANES), F32), shape((8, LANES), F32)),
            [pltpu.VMEM((nodes, halo), BF16), pltpu.VMEM((TILES, groups, block, LANES), F32), pltpu.VMEM((groups, home, HID), F32),
             pltpu.VMEM((groups, 8, LANES), F32), pltpu.VMEM((home, HID), BF16),
             pltpu.VMEM((chips, part, LANES), F32), pltpu.VMEM((chips, part, LANES), F32), pltpu.VMEM((chips, part, LANES), F32),
             pltpu.VMEM((part, LANES), F32),
             pltpu.VMEM((TILES, groups * 8, LANES), F32), pltpu.VMEM((TILES, groups, 8, LANES), F32), pltpu.VMEM((TILES, 8, LANES), F32)] + sems(18),
            "last_exchange", params(2))

        grad_xt, grad_w1, grad_w2, grad_b1, grad_b2 = call(
            outputs_kernel,
            [(w_first, "vmem"), (hub_lanes, "vmem"), (dz1h.reshape(hubs, HID), "vmem"), (dw1, "vmem"), (dw2.reshape(HID, LANES), "vmem"), (biases, "vmem"), (dz1, "vmem")],
            (shape((feat, nodes), F32), shape((feat, HID), F32), shape((HID, out), F32), shape((1, HID), F32), shape((1, out), F32)),
            [], "outputs", params())
        return grad_xt.T, grad_w1, grad_w2, grad_b1.reshape(HID), grad_b2.reshape(out)

    return jax.shard_map(
        device_step,
        mesh=mesh,
        in_specs=(vertex_rows, vertex_spec, vertex_spec, vertex_spec, vertex_spec, part_spec, replicated, replicated, replicated, vertex_rows),
        out_specs=(vertex_rows, part_rows, part_rows, part_spec, part_spec),
        check_vma=False,
    )
```

```python
import functools

import jax
import jax.numpy as jnp
from jax import lax
from jax.experimental import pallas as pl
from jax.experimental.pallas import tpu as pltpu
from jax.sharding import PartitionSpec as P

F32, BF16, I32 = jnp.float32, jnp.bfloat16, jnp.int32
CONTRACT_ROWS = (((0,), (0,)), ((), ()))
CONTRACT_COLS = (((1,), (1,)), ((), ()))
LANES = 128
WAYS = 4
HID = 512
TILES = HID // LANES
CHUNK = 256
VMEM_LIMIT = 67043328
HBM = pl.BlockSpec(memory_space=pltpu.HBM)


class Fetched:
    def __init__(self, src, dst, sem):
        self.copy, self.ref, self.pending = pltpu.make_async_copy(src, dst, sem), dst, True
        self.copy.start()

    def get(self):
        if self.pending:
            self.copy.wait()
            self.pending = False
        return self.ref


def call(kernel, args, out_shape, scratch_shapes, name, compiler_params):
    spaces = {"vmem": pltpu.VMEM, "smem": pltpu.SMEM}
    in_buffers = [spaces[space](array.shape, array.dtype) for array, space in args]
    out_buffers = [pltpu.VMEM(out.shape, out.dtype) for out in out_shape]
    n_in, n_out = len(args), len(out_shape)

    def body(*refs):
        inputs, outputs = refs[:n_in], refs[n_in:n_in + n_out]
        bufs = refs[n_in + n_out:2 * n_in + 2 * n_out]
        scratch, sems, out_sems = refs[2 * n_in + 2 * n_out:-2], refs[-2], refs[-1]
        fetched = [Fetched(ref, bufs[n], sems.at[n]) for n, ref in enumerate(inputs)]
        results = bufs[n_in:]
        stores = {}

        def flush(*buffers):
            for buffer in buffers:
                n = [k for k in range(n_out) if results[k] is buffer][0]
                stores[n] = pltpu.make_async_copy(results[n], outputs[n], out_sems.at[n])
                stores[n].start()

        kernel(*fetched, *results, *scratch, flush=flush)
        for item in fetched:
            item.get()
        flush(*[results[n] for n in range(n_out) if n not in stores])
        for n in range(n_out):
            stores[n].wait()

    return pl.pallas_call(
        body,
        name=name,
        out_shape=out_shape,
        in_specs=[HBM] * n_in,
        out_specs=(HBM,) * n_out,
        scratch_shapes=in_buffers + out_buffers + list(scratch_shapes) + [pltpu.SemaphoreType.DMA((n_in,)), pltpu.SemaphoreType.DMA((n_out,))],
        compiler_params=compiler_params,
    )(*[array for array, _ in args])


def dot(a, b, dims=(((1,), (0,)), ((), ()))):
    return lax.dot_general(a, b, dims, preferred_element_type=F32)


def iota(shape, dim):
    return lax.broadcasted_iota(I32, shape, dim)


def split3(value):
    high = value.astype(BF16)
    rest = value - high.astype(F32)
    mid = rest.astype(BF16)
    low = (rest - mid.astype(F32)).astype(BF16)
    return high, mid, low


def select_rows(onehot, value, dims=(((1,), (0,)), ((), ()))):
    high, mid, low = split3(value)
    return dot(onehot, low, dims) + dot(onehot, mid, dims) + dot(onehot, high, dims)


def pad_lanes(value):
    rows, cols = value.shape
    if cols == LANES:
        return value
    return jnp.concatenate([value, jnp.zeros((rows, LANES - cols), value.dtype)], axis=1)


def hub_block(device, groups):
    return lax.rem(device, 2) * (groups // 2) + device // 2


def greet(groups, me):
    barrier = pltpu.get_barrier_semaphore()
    for step in range(1, groups):
        pl.semaphore_signal(barrier, inc=1, device_id={"graph": lax.rem(me + step, groups)}, device_id_type=pl.DeviceIdType.MESH)
    return barrier


def send(src, dst, send_sem, recv_sem, peer):
    copy = pltpu.make_async_remote_copy(
        src_ref=src, dst_ref=dst, send_sem=send_sem, recv_sem=recv_sem,
        device_id={"graph": peer}, device_id_type=pl.DeviceIdType.MESH)
    copy.start()
    return copy


def pack_rows(value):
    half = value.shape[0] // 2
    low = iota((half, LANES), 1) < LANES // 2
    return jnp.where(low, value[:half], pltpu.roll(value[half:], LANES // 2, 1)).astype(BF16)


def unpack_rows(value):
    return jnp.concatenate([value, pltpu.roll(value, LANES // 2, 1)], axis=0)


def gather_kernel(groups, hubrow, xt, send_idx, hub_ids, dh, dst, src, w,
                  xh_ref, hx_ref, dhh_ref, used_ref, db2_ref, wide_ref, *rest, flush):
    lists, (x32, xg, hxg, dhg, xs, xr, dhr, ssem, rsem) = rest[:3 * WAYS], rest[3 * WAYS:]
    me = lax.axis_index("graph")
    barrier = greet(groups, me)
    feat, nodes = xt.ref.shape
    hubs = hub_ids.ref.shape[0]
    halo = send_idx.ref.shape[0]
    block = halo // groups
    base = me * nodes
    eye = (iota((feat, LANES), 0) == iota((feat, LANES), 1)).astype(BF16)
    tags = jnp.where(iota((hubs, LANES), 1) == feat, iota((hubs, LANES), 0) + 1, 0).astype(F32).astype(BF16)
    hubrow = hubrow.get()[...]
    xt_ref = xt.get()
    for row in range(0, nodes, CHUNK):
        owned = (iota((CHUNK, hubs), 0) + (base + row) == hubrow).astype(BF16)
        x32[pl.ds(row, CHUNK), :] = dot(xt_ref[:, pl.ds(row, CHUNK)], eye, CONTRACT_ROWS) + dot(owned, tags)

    send_ref = send_idx.get()

    def pick(i, carry):
        for u in range(16):
            j = i * 16 + u
            xg[pl.ds(j, 1), :] = x32[pl.ds(send_ref[j], 1), :]
        return carry

    lax.fori_loop(0, halo // 16, pick, 0)
    dhg[...] = jnp.zeros_like(dhg)
    hub_ref, dh_ref = hub_ids.get(), dh.get()

    def pick_hub(i, carry):
        for u in range(8):
            k = i * 8 + u
            row = hub_ref[k] - base
            own = jnp.logical_and(row >= 0, row < nodes)
            row = jnp.clip(row, 0, nodes - 1)
            hxg[pl.ds(k, 1), :] = jnp.where(own, x32[pl.ds(row, 1), :], 0.0)
            value = dh_ref[pl.ds(row, 1), :]
            dhg[pl.ds(k, 1), pl.ds(0, value.shape[1])] = jnp.where(own, value, 0.0)
        return carry

    lax.fori_loop(0, hubs // 8, pick_hub, 0)
    hub_rows = pack_rows(hxg[...])
    for q in range(groups):
        xs[q, pl.ds(0, block // 2), :] = pack_rows(xg[pl.ds(q * block, block), :])
        xs[q, pl.ds(block // 2, hubs // 2), :] = hub_rows
    pl.semaphore_wait(barrier, groups - 1)
    copies = []
    for step in range(1, groups):
        peer = lax.rem(me + step, groups)
        copies.append(send(xs.at[peer], xr.at[me], ssem.at[0, step], rsem.at[0, step], peer))
        copies.append(send(dhg, dhr.at[me], ssem.at[1, step], rsem.at[1, step], peer))
    dst_ref, src_ref, w_ref = dst.get(), src.get(), w.get()
    blocks = w_ref.shape[0]
    for q in range(WAYS):
        part = pl.ds(q, blocks // WAYS, stride=WAYS)
        lists[q][...] = dst_ref[part, :] * TILES
        lists[WAYS + q][...] = src_ref[part, :] * TILES
        lists[2 * WAYS + q][...] = w_ref[part, :]
    flush(*lists)
    diagonal = iota((LANES, LANES), 0) == iota((LANES, LANES), 1)
    ones = jnp.ones((LANES, LANES), BF16)

    def widen(i, carry):
        for q in range(WAYS):
            row = lists[2 * WAYS + q][pl.ds(i, 1), :]
            spread = jnp.zeros((LANES, LANES), F32)
            for piece in reversed(split3(row)):
                column = jnp.where(diagonal, jnp.broadcast_to(piece.astype(F32), (LANES, LANES)), 0.0).astype(BF16)
                spread = spread + dot(column, ones)
            wide_ref[pl.ds(pl.multiple_of((q * (blocks // WAYS) + i) * LANES, LANES), LANES), :] = spread
        return carry

    lax.fori_loop(0, blocks // WAYS, widen, 0)
    flush(wide_ref)
    used = jnp.where(w_ref[...] > 0.0, 1.0, 0.0).sum(axis=0, keepdims=True).sum(axis=1, keepdims=True)
    used_ref[...] = jnp.broadcast_to(used, used_ref.shape).astype(I32)
    total = jnp.zeros((8, dh_ref.shape[1]), F32)
    for row in range(0, nodes, CHUNK):
        total = total + dh_ref[pl.ds(row, CHUNK), :].reshape(CHUNK // 8, 8, dh_ref.shape[1]).sum(axis=0)
    db2_ref[...] = jnp.broadcast_to(pad_lanes(total.sum(axis=0, keepdims=True)), db2_ref.shape)
    flush(used_ref, db2_ref)
    xr[me] = xs[me]
    dhr[me] = dhg[...]
    for copy in copies:
        copy.wait()
    hx = jnp.zeros((hubs // 2, LANES), F32)
    dhh = jnp.zeros((hubs, LANES), F32)
    for q in range(groups):
        xh_ref[pl.ds(q * block, block), :] = unpack_rows(xr[q, pl.ds(0, block // 2), :].astype(F32)).astype(BF16)
        hx = hx + xr[q, pl.ds(block // 2, hubs // 2), :].astype(F32)
        dhh = dhh + dhr[q]
    hx_ref[...] = unpack_rows(hx)
    dhh_ref[...] = dhh


def hub_position(hub_ref, k, base, nodes):
    row = hub_ref[k] - base
    own = jnp.logical_and(row >= 0, row < nodes)
    return own, pl.multiple_of(jnp.clip(row, 0, nodes - 1) * TILES, TILES)


def trips(used_ref, unroll):
    return (used_ref[0, 0] + (WAYS * LANES - 1)) // (WAYS * LANES) * (LANES // unroll)


def strided(first, rows):
    return pl.ds(first, rows, stride=TILES)


def total_of(refs, where):
    value = refs[0][where, :]
    for ref in refs[1:]:
        value = value + ref[where, :]
    return value


def edges_forward_kernel(copies, unroll, w1, xt, dh, xh, hx, dhh, used, hub_ids, b1, *rest, flush):
    lists, (h1_ref, dz_ref, hz_ref, hub_out, zt, dt), accs = rest[:3 * WAYS], rest[3 * WAYS:3 * WAYS + 6], rest[3 * WAYS + 6:]
    ya, da = accs[:copies], accs[copies:]
    me = lax.axis_index("graph")
    feat, nodes = xt.ref.shape
    halo, hubs = xh.ref.shape[0], hx.ref.shape[0]
    base = me * nodes
    for acc in ya:
        acc[...] = jnp.zeros_like(acc)
    for acc in da:
        acc[strided(0, nodes + halo + hubs), :] = jnp.zeros((nodes + halo + hubs, LANES), F32)
    w1 = w1.get()[...]
    xt_ref, dh_ref, xh_ref, hx_ref = xt.get(), dh.get(), xh.get(), hx.get()

    def put_rows(first, z):
        z = z.astype(BF16).astype(F32)
        for c in range(TILES):
            zt[strided(first * TILES + c, z.shape[0]), :] = z[:, c * LANES:(c + 1) * LANES]

    for row in range(0, nodes, CHUNK):
        put_rows(row, dot(xt_ref[:, pl.ds(row, CHUNK)], w1, CONTRACT_ROWS))
        dt[strided(row * TILES, CHUNK), :] = pad_lanes(dh_ref[pl.ds(row, CHUNK), :])
    for row in range(0, halo, CHUNK):
        put_rows(nodes + row, dot(xh_ref[pl.ds(row, CHUNK), pl.ds(0, feat)], w1))
    put_rows(nodes + halo, dot(hx_ref[:, pl.ds(0, feat)].astype(BF16), w1))
    dt[strided(nodes * TILES, hubs), :] = dhh.get()[...]
    used_ref, hub_ref, b1_ref = used.get(), hub_ids.get(), b1.get()
    lists = [item.get() for item in lists]

    def step(i, carry):
        for n in range(unroll * WAYS):
            q, u = n % WAYS, n % copies
            j = i * unroll + n // WAYS
            d4 = pl.multiple_of(lists[q][j], TILES)
            s4 = pl.multiple_of(lists[WAYS + q][j], TILES)
            w = lists[2 * WAYS + q][j]
            y_new = ya[u][pl.ds(d4, TILES), :] + w * zt[pl.ds(s4, TILES), :]
            z_new = da[u][pl.ds(s4, 1), :] + w * dt[pl.ds(d4, 1), :]
            ya[u][pl.ds(d4, TILES), :] = y_new
            da[u][pl.ds(s4, 1), :] = z_new
        return carry

    lax.fori_loop(0, trips(used_ref, unroll), step, 0)

    def fold(k, carry):
        own, row = hub_position(hub_ref, k, base, nodes)
        here = pl.multiple_of((nodes + k) * TILES, TILES)
        ya[0][pl.ds(here, TILES), :] += jnp.where(own, total_of(ya, pl.ds(row, TILES)), 0.0)
        here = (nodes + halo + k) * TILES
        value = total_of(da, pl.ds(row, 1))
        da[0][pl.ds(here, 1), :] += jnp.where(own, value, 0.0)
        da[0][pl.ds(row, 1), :] = jnp.where(own, 0.0, value)
        for acc in da[1:]:
            acc[pl.ds(row, 1), :] = jnp.zeros((1, LANES), F32)
        return carry

    lax.fori_loop(0, hubs, fold, 0)
    for row in range(0, nodes, CHUNK):
        for c in range(TILES):
            cols = pl.ds(c * LANES, LANES)
            y = total_of(ya, strided(row * TILES + c, CHUNK)) + b1_ref[:, cols]
            h1_ref[pl.ds(row, CHUNK), cols] = jnp.maximum(y, 0.0).astype(BF16)
    flush(h1_ref)
    for row in range(0, nodes, CHUNK):
        dz_ref[pl.ds(row, CHUNK), :] = total_of(da, strided(row * TILES, CHUNK))
    flush(dz_ref)
    hz = total_of(da, strided(nodes * TILES, halo))
    tag = xh_ref[...].astype(F32)[:, feat:feat + 1]
    onehot = (tag == (iota((halo, hubs), 1) + 1).astype(F32)).astype(BF16)
    hub_z = total_of(da, strided((nodes + halo) * TILES, hubs)) + select_rows(onehot, hz, CONTRACT_ROWS)
    hz_ref[...] = jnp.where(tag > 0.0, 0.0, hz)
    for c in range(TILES):
        hub_out[:, pl.ds(c * LANES, LANES)] = total_of(ya, strided(nodes * TILES + c, hubs))
    hub_out[:, pl.ds(HID, LANES)] = hub_z


def middle_kernel(groups, hub, hz, dz, b1, w2, sendrow,
                  dz2_ref, dyh_ref, h1h_ref, dz2h_ref,
                  hzr, hubr, dyr, dys, ssem, rsem, flush):
    me = lax.axis_index("graph")
    barrier = greet(groups, me)
    nodes = dz.ref.shape[0]
    out = w2.ref.shape[1]
    home = hub.ref.shape[1]
    block = hz.ref.shape[1]
    halo = groups * block
    hub_ref, hz_ref = hub.get(), hz.get()
    own = hub_block(me, groups)
    hubr[me] = hub_ref[own]
    hzr[me] = jnp.zeros(hzr.shape[1:], F32)
    pl.semaphore_wait(barrier, groups - 1)
    hub_copies, halo_copies, back = [], [], []
    for step in range(1, groups):
        peer = lax.rem(me + step, groups)
        hub_copies.append(send(hub_ref.at[hub_block(peer, groups)], hubr.at[me], ssem.at[0, step], rsem.at[0, step], peer))
    for step in range(1, groups):
        peer = lax.rem(me + step, groups)
        halo_copies.append(send(hz_ref.at[peer], hzr.at[me], ssem.at[1, step], rsem.at[1, step], peer))
    for copy in hub_copies:
        copy.wait()
    total = hubr[0]
    for q in range(1, groups):
        total = total + hubr[q]
    b1_ref, w2_ref, sendrow = b1.get(), w2.get(), sendrow.get()[...]
    pre = total[:, :HID] + b1_ref[...]
    dz2h = total[:, HID:].astype(BF16)
    h1h_ref[...] = jnp.maximum(pre, 0.0).astype(BF16)
    dz2h_ref[...] = dz2h
    dys[...] = jnp.where(pre > 0, dot(dz2h[:, :out], w2_ref[...], CONTRACT_COLS), 0.0)
    for step in range(1, groups):
        peer = lax.rem(me + step, groups)
        back.append(send(dys, dyr.at[own], ssem.at[2, step], rsem.at[2, step], peer))
    dyr[own] = dys[...]
    for copy in halo_copies:
        copy.wait()
    pieces = split3(hzr[...].reshape(halo, LANES))
    dz_ref = dz.get()
    for row in range(0, nodes, CHUNK):
        onehot = (iota((CHUNK, halo), 0) + row == sendrow).astype(BF16)
        value = dz_ref[pl.ds(row, CHUNK), :]
        for piece in reversed(pieces):
            value = value + dot(onehot, piece)
        dz2_ref[pl.ds(row, CHUNK), :] = value.astype(BF16)
    for copy in back:
        copy.wait()
    for q in range(groups):
        dyh_ref[pl.ds(q * home, home), :] = dyr[q]


def edges_backward_kernel(copies, unroll, feat, groups, w2, h1, dz2, dyh, h1h, dz2h, used, hub_ids, xh, db2, wide, *rest, flush):
    lists, rest = rest[:2 * WAYS], rest[2 * WAYS:]
    (dz1_ref, hz_ref, hub_out, dw2_ref, bias_ref, yt), za = rest[:6], rest[6:]
    me = lax.axis_index("graph")
    nodes = h1.ref.shape[0]
    out = w2.ref.shape[1]
    halo, hubs = xh.ref.shape[0], dyh.ref.shape[0]
    home = h1h.ref.shape[0]
    base = me * nodes
    for acc in za:
        acc[...] = jnp.zeros_like(acc)
    w2, h1_ref, dz2_ref, dyh_ref, h1h_ref, dz2h_ref = w2.get()[...], h1.get(), dz2.get(), dyh.get(), h1h.get(), dz2h.get()
    mine = dyh_ref[pl.ds(pl.multiple_of(hub_block(me, groups) * home, 8), home), :]
    db1 = mine
    for row in range(0, nodes, CHUNK):
        rows = pl.ds(row, CHUNK)
        grad = dot(dz2_ref[rows, pl.ds(0, out)], w2, CONTRACT_COLS)
        grad = jnp.where(h1_ref[rows, :] > 0, grad, 0.0)
        db1 = db1 + grad.reshape(CHUNK // 8, 8, HID).sum(axis=0)
        for c in range(TILES):
            yt[strided(row * TILES + c, CHUNK), :] = grad[:, c * LANES:(c + 1) * LANES]
    db1 = db1.sum(axis=0, keepdims=True)
    bias_ref[...] = db2.get()[...]
    for c in range(TILES):
        bias_ref[pl.ds(c, 1), :] = db1[:, c * LANES:(c + 1) * LANES]
        yt[strided(nodes * TILES + c, hubs), :] = dyh_ref[:, pl.ds(c * LANES, LANES)]
    dw2_ref[...] = dot(h1_ref[...], dz2_ref[...], CONTRACT_ROWS) + dot(h1h_ref[...], dz2h_ref[...], CONTRACT_ROWS)
    flush(dw2_ref, bias_ref)
    used_ref, hub_ref, xh_ref, wide_ref = used.get(), hub_ids.get(), xh.get(), wide.get()
    lists = [item.get() for item in lists]
    length = wide_ref.shape[0] // WAYS

    def place(k, carry):
        own, row = hub_position(hub_ref, k, base, nodes)
        here = pl.multiple_of((nodes + k) * TILES, TILES)
        yt[pl.ds(row, TILES), :] = jnp.where(own, yt[pl.ds(here, TILES), :], yt[pl.ds(row, TILES), :])
        return carry

    lax.fori_loop(0, hubs, place, 0)

    def step(i, carry):
        for n in range(unroll * WAYS):
            q, u = n % WAYS, n % copies
            j = pl.multiple_of(i * unroll, unroll) + n // WAYS
            d4 = pl.multiple_of(lists[q][j], TILES)
            s4 = pl.multiple_of(lists[WAYS + q][j], TILES)
            w = wide_ref[pl.ds(q * length + j, 1), :]
            za[u][pl.ds(s4, TILES), :] = za[u][pl.ds(s4, TILES), :] + w * yt[pl.ds(d4, TILES), :]
        return carry

    lax.fori_loop(0, trips(used_ref, unroll), step, 0)

    def fold(k, carry):
        own, row = hub_position(hub_ref, k, base, nodes)
        here = pl.multiple_of((nodes + halo + k) * TILES, TILES)
        value = total_of(za, pl.ds(row, TILES))
        za[0][pl.ds(here, TILES), :] += jnp.where(own, value, 0.0)
        za[0][pl.ds(row, TILES), :] = jnp.where(own, 0.0, value)
        for acc in za[1:]:
            acc[pl.ds(row, TILES), :] = jnp.zeros((TILES, LANES), F32)
        return carry

    lax.fori_loop(0, hubs, fold, 0)
    for row in range(0, nodes, CHUNK):
        for c in range(TILES):
            dz1_ref[pl.ds(row, CHUNK), pl.ds(c * LANES, LANES)] = total_of(za, strided(row * TILES + c, CHUNK))
    flush(dz1_ref)
    tag = xh_ref[...].astype(F32)[:, feat:feat + 1]
    onehot = (tag == (iota((halo, hubs), 1) + 1).astype(F32)).astype(BF16)
    for c in range(TILES):
        cols = pl.ds(c * LANES, LANES)
        hz = total_of(za, strided(nodes * TILES + c, halo))
        hub_out[:, cols] = total_of(za, strided((nodes + halo) * TILES + c, hubs)) + select_rows(onehot, hz, CONTRACT_ROWS)
        hz_ref[c] = jnp.where(tag > 0.0, 0.0, hz)


def last_kernel(groups, hub, hz, dw2, bias, sendrow, xt, hx, dz1, w1, hubrow,
                gxt_ref, dw1a, dw2a, bias_out,
                dz_out, onehot, hzr, hubp, hubh, hubr, biasp, biash, biasr, dhs, dha, dw2p, dw2h, dw2r, dw2s, dw1s, dw1r, dw1t, ssem, rsem, flush):
    me = lax.axis_index("graph")
    barrier = greet(groups, me)
    feat, nodes = xt.ref.shape
    chips, home = hub.ref.shape[1:3]
    hubs = groups * home
    block = hz.ref.shape[2]
    halo = groups * block
    base = me * nodes
    core, chip = lax.rem(me, 2), me // 2
    partner = me + 1 - 2 * core
    own = hub_block(me, groups)
    peers = [lax.rem(me + step, groups) for step in range(1, groups)]
    others = [lax.rem(me + 2 * step, groups) for step in range(1, chips)]
    hub_ref, hz_ref, dw2_ref, bias_ref = hub.get(), hz.get(), dw2.get(), bias.get()
    pl.semaphore_wait(barrier, groups - 1)

    def to(devices, slot, src, dst):
        return [send(src(peer), dst, ssem.at[slot, i], rsem.at[slot, i], peer) for i, peer in enumerate(devices)]

    def wait(pending):
        for copy in pending:
            copy.wait()

    pair_copies = (to([partner], 0, lambda p: hub_ref.at[1 - core], hubp) + to([partner], 1, lambda p: dw2_ref.at[1 - core], dw2p)
                   + to([partner], 2, lambda p: bias_ref, biasp))
    halo_copies = [to(peers, 9, lambda p: hz_ref.at[0, p], hzr.at[0, me])]
    sendrow = sendrow.get()[...]
    for row in range(0, nodes, CHUNK):
        onehot[pl.ds(row, CHUNK), :] = (iota((CHUNK, halo), 0) + row == sendrow).astype(BF16)
    for c in range(TILES):
        hzr[c, me] = jnp.zeros((block, LANES), F32)
        dw1s[c] = jnp.zeros(dw1s.shape[1:], F32)
    wait(pair_copies)
    hubh[...] = hub_ref[core] + hubp[...]
    dw2h[...] = dw2_ref[core] + dw2p[...]
    biash[...] = bias_ref[...] + biasp[...]
    hubr[chip] = hubh[chip]
    dw2r[chip] = dw2h[chip]
    biasr[chip] = biash[...]
    hub_copies = to(others, 3, lambda p: hubh.at[p // 2], hubr.at[chip])
    dw2_copies = to(others, 4, lambda p: dw2h.at[p // 2], dw2r.at[chip])
    bias_copies = to(others, 5, lambda p: biash, biasr.at[chip])
    halo_copies += [to(peers, 9 + c, lambda p: hz_ref.at[c, p], hzr.at[c, me]) for c in range(1, TILES)]

    def total_over(ref, count):
        total = ref[0]
        for q in range(1, count):
            total = total + ref[q]
        return total

    xt_ref, dz1_ref, hx_ref, w1, hubrow = xt.get(), dz1.get(), hx.get(), w1.get()[...], hubrow.get()[...]
    wait(hub_copies)
    dz1h = total_over(hubr, chips).astype(BF16)
    dhs[...] = dz1h
    back_copies = to(peers, 6, lambda p: dhs, dha.at[own])
    dha[own] = dz1h
    hx_mine = hx_ref[pl.ds(pl.multiple_of(own * home, 8), home), :].astype(BF16)
    dw1h = dot(hx_mine[:, :feat], dz1h, CONTRACT_ROWS)
    rs_copies, ag_copies = [None] * TILES, [None] * TILES

    def spread(c):
        wait(rs_copies[c])
        total = total_over(dw1r.at[c], groups)
        dw1t[c] = total
        ag_copies[c] = to(peers, 17 + c, lambda p: dw1t.at[c], dw1a.at[c, me])
        dw1a[c, me] = total

    for c in range(TILES):
        wait(halo_copies[c])
        cols = pl.ds(c * LANES, LANES)
        pieces = jnp.concatenate(split3(hzr[c].reshape(halo, LANES)), axis=1)

        def rows_step(i, carry):
            rows = pl.ds(pl.multiple_of(i * CHUNK, CHUNK), CHUNK)
            value = dot(onehot[rows, :], pieces)
            value = value[:, 2 * LANES:] + value[:, LANES:2 * LANES] + value[:, :LANES]
            dz_out[rows, cols] = (dz1_ref[rows, cols] + value).astype(BF16)
            return carry

        lax.fori_loop(0, nodes // CHUNK, rows_step, 0)
        dw1s[c, pl.ds(0, feat), :] = dot(xt_ref[...], dz_out[:, cols]) + dw1h[:, c * LANES:(c + 1) * LANES]
        rs_copies[c] = to(peers, 13 + c, lambda p: dw1s.at[c, pl.ds(pl.multiple_of(p * 8, 8), 8)], dw1r.at[c, me])
        dw1r[c, me] = dw1s[c, pl.ds(pl.multiple_of(me * 8, 8), 8), :]
        if c == 0:
            wait(dw2_copies)
            total = total_over(dw2r, chips)
            dw2s[...] = total
            dw2_back = to(others, 7, lambda p: dw2s, dw2a.at[core, chip])
            dw2a[core, chip] = total
        if c > 0:
            spread(c - 1)
        if c == 2:
            wait(dw2_back)
            dw2_pair = to([partner], 8, lambda p: dw2a.at[core], dw2a.at[core])
    wait(back_copies)
    hub_rows = dha[...].reshape(hubs, HID)
    for row in range(0, nodes, 2 * CHUNK):
        rows = pl.ds(row, 2 * CHUNK)
        owned = (iota((2 * CHUNK, hubs), 0) + (base + row) == hubrow).astype(BF16)
        dz = (dz_out[rows, :].astype(F32) + dot(owned, hub_rows)).astype(BF16)
        gxt_ref[:, rows] = dot(w1, dz, CONTRACT_COLS)
    flush(gxt_ref)
    wait(bias_copies)
    bias_out[...] = total_over(biasr, chips)
    flush(bias_out)
    spread(TILES - 1)
    wait(dw2_pair)
    flush(dw2a)
    for c in range(TILES):
        wait(ag_copies[c])


def outputs_kernel(gxt, dw2, bias, dw1, gxt_ref, gw1_ref, gw2_ref, gb1_ref, gb2_ref, flush):
    feat, out = gw1_ref.shape[0], gw2_ref.shape[1]
    gxt_ref[...] = gxt.get()[...]
    flush(gxt_ref)
    gw2_ref[...] = dw2.get()[:, pl.ds(0, out)]
    flush(gw2_ref)
    bias_ref, dw1_ref = bias.get(), dw1.get()
    for c in range(TILES):
        cols = pl.ds(c * LANES, LANES)
        for q in range(dw1_ref.shape[1]):
            rows = min(8, feat - q * 8)
            if rows > 0:
                gw1_ref[pl.ds(q * 8, rows), cols] = dw1_ref[c, q, pl.ds(0, rows), :]
        gb1_ref[:, cols] = bias_ref[pl.ds(c, 1), :]
    gb2_ref[...] = bias_ref[pl.ds(TILES, 1), pl.ds(0, out)]


def shape(dims, dtype):
    return jax.ShapeDtypeStruct(dims, dtype)


def solution(mesh):
    groups = mesh.shape["graph"]
    vertex_spec = P(("data", "graph"))
    vertex_rows = P(("data", "graph"), None)
    part_spec = P("data")
    part_rows = P("data", None)
    replicated = P()
    copies1, unroll1 = 3, 16
    copies2, unroll2 = 5, 16

    def params(collective_id=None):
        if collective_id is None:
            return pltpu.CompilerParams(vmem_limit_bytes=VMEM_LIMIT)
        return pltpu.CompilerParams(vmem_limit_bytes=VMEM_LIMIT, collective_id=collective_id, has_side_effects=True)

    def device_step(x_loc, dst_loc, src_loc, w_loc, send_loc, hub_ids, w_first, b_first, w_second, dy_out):
        nodes, feat = x_loc.shape
        edges = dst_loc.shape[0]
        halo = send_loc.shape[0]
        hubs = hub_ids.shape[0]
        out = dy_out.shape[1]
        block, home = halo // groups, hubs // groups
        src_rows, dst_rows = nodes + halo + hubs, nodes + hubs
        x_t = x_loc.T
        hub_lanes = hub_ids.reshape(1, hubs)
        send_lanes = send_loc.reshape(1, halo)
        bias = b_first.reshape(1, HID)
        sems = lambda n: [pltpu.SemaphoreType.DMA((n, groups)), pltpu.SemaphoreType.DMA((n, groups))]
        table = lambda a: a.reshape(edges // LANES, LANES)
        part_list = (edges // LANES // WAYS, LANES)
        packed = (block + hubs) // 2

        xh, hx, dhh, used, db2, wide, *lists = call(
            functools.partial(gather_kernel, groups),
            [(hub_lanes, "vmem"), (x_t, "vmem"), (send_loc, "smem"), (hub_ids, "smem"), (dy_out, "vmem"),
             (table(dst_loc), "vmem"), (table(src_loc), "vmem"), (table(w_loc), "vmem")],
            (shape((halo, LANES), BF16), shape((hubs, LANES), F32), shape((hubs, LANES), F32),
             shape((8, LANES), I32), shape((8, LANES), F32), shape((edges, LANES), F32))
            + (shape(part_list, I32),) * (2 * WAYS) + (shape(part_list, F32),) * WAYS,
            [pltpu.VMEM((nodes, LANES), F32), pltpu.VMEM((halo, LANES), F32), pltpu.VMEM((hubs, LANES), F32),
             pltpu.VMEM((hubs, LANES), F32), pltpu.VMEM((groups, packed, LANES), BF16),
             pltpu.VMEM((groups, packed, LANES), BF16), pltpu.VMEM((groups, hubs, LANES), F32)] + sems(2),
            "gather_rows", params(0))
        lists = [(item.reshape(edges // WAYS), "smem") for item in lists]

        h1, dz, hz, hub = call(
            functools.partial(edges_forward_kernel, copies1, unroll1),
            [(w_first, "vmem"), (x_t, "vmem"), (dy_out, "vmem"), (xh, "vmem"), (hx, "vmem"), (dhh, "vmem"),
             (used, "smem"), (hub_ids, "smem"), (bias, "vmem")] + lists,
            (shape((nodes, HID), BF16), shape((nodes, LANES), F32), shape((halo, LANES), F32), shape((hubs, HID + LANES), F32)),
            [pltpu.VMEM((src_rows * TILES, LANES), F32), pltpu.VMEM((dst_rows * TILES, LANES), F32)]
            + [pltpu.VMEM((dst_rows * TILES, LANES), F32)] * copies1 + [pltpu.VMEM((src_rows * TILES, LANES), F32)] * copies1,
            "edges_forward", params())

        dz2, dyh, h1h, dz2h = call(
            functools.partial(middle_kernel, groups),
            [(hub.reshape(groups, home, HID + LANES), "vmem"), (hz.reshape(groups, block, LANES), "vmem"), (dz, "vmem"),
             (bias, "vmem"), (w_second, "vmem"), (send_lanes, "vmem")],
            (shape((nodes, LANES), BF16), shape((hubs, HID), F32), shape((home, HID), BF16), shape((home, LANES), BF16)),
            [pltpu.VMEM((groups, block, LANES), F32), pltpu.VMEM((groups, home, HID + LANES), F32),
             pltpu.VMEM((groups, home, HID), F32), pltpu.VMEM((home, HID), F32)] + sems(3),
            "middle", params(1))

        dz1, hz1, hub1, dw2, biases = call(
            functools.partial(edges_backward_kernel, copies2, unroll2, feat, groups),
            [(w_second, "vmem"), (h1, "vmem"), (dz2, "vmem"), (dyh, "vmem"), (h1h, "vmem"), (dz2h, "vmem"),
             (used, "smem"), (hub_ids, "smem"), (xh, "vmem"), (db2, "vmem"), (wide, "vmem")] + lists[:2 * WAYS],
            (shape((nodes, HID), F32), shape((TILES, halo, LANES), F32), shape((hubs, HID), F32), shape((HID, LANES), F32), shape((8, LANES), F32)),
            [pltpu.VMEM((dst_rows * TILES, LANES), F32)] + [pltpu.VMEM((src_rows * TILES, LANES), F32)] * copies2,
            "edges_backward", params())

        chips = groups // 2
        part = HID // groups
        grad_xt, dw1, dw2, biases = call(
            functools.partial(last_kernel, groups),
            [(hub1.reshape(2, chips, home, HID), "vmem"), (hz1.reshape(TILES, groups, block, LANES), "vmem"),
             (dw2.reshape(2, chips, part, LANES), "vmem"), (biases, "vmem"), (send_lanes, "vmem"), (x_t, "vmem"), (hx, "vmem"),
             (dz1, "vmem"), (w_first, "vmem"), (hub_lanes, "vmem")],
            (shape((feat, nodes), F32), shape((TILES, groups, 8, LANES), F32), shape((2, chips, part, LANES), F32), shape((8, LANES), F32)),
            [pltpu.VMEM((nodes, HID), BF16), pltpu.VMEM((nodes, halo), BF16), pltpu.VMEM((TILES, groups, block, LANES), F32)]
            + [pltpu.VMEM((chips, home, HID), F32)] * 3 + [pltpu.VMEM((8, LANES), F32)] * 2 + [pltpu.VMEM((chips, 8, LANES), F32)]
            + [pltpu.VMEM((home, HID), BF16), pltpu.VMEM((groups, home, HID), BF16)]
            + [pltpu.VMEM((chips, part, LANES), F32)] * 3 + [pltpu.VMEM((part, LANES), F32)]
            + [pltpu.VMEM((TILES, groups * 8, LANES), F32), pltpu.VMEM((TILES, groups, 8, LANES), F32), pltpu.VMEM((TILES, 8, LANES), F32)] + sems(21),
            "last_exchange", params(2))

        grad_xt, grad_w1, grad_w2, grad_b1, grad_b2 = call(
            outputs_kernel,
            [(grad_xt, "vmem"), (dw2.reshape(HID, LANES), "vmem"), (biases, "vmem"), (dw1, "vmem")],
            (shape((feat, nodes), F32), shape((feat, HID), F32), shape((HID, out), F32), shape((1, HID), F32), shape((1, out), F32)),
            [], "outputs", params())
        return grad_xt.T, grad_w1, grad_w2, grad_b1.reshape(HID), grad_b2.reshape(out)

    return jax.shard_map(
        device_step,
        mesh=mesh,
        in_specs=(vertex_rows, vertex_spec, vertex_spec, vertex_spec, vertex_spec, part_spec, replicated, replicated, replicated, vertex_rows),
        out_specs=(vertex_rows, part_rows, part_rows, part_spec, part_spec),
        check_vma=False,
    )
```

```python
import functools

import jax
import jax.numpy as jnp
from jax import lax
from jax.experimental import pallas as pl
from jax.experimental.pallas import tpu as pltpu
from jax.sharding import PartitionSpec as P

F32, BF16, I32 = jnp.float32, jnp.bfloat16, jnp.int32
CONTRACT_ROWS = (((0,), (0,)), ((), ()))
CONTRACT_COLS = (((1,), (1,)), ((), ()))
LANES = 128
WAYS = 4
HID = 512
TILES = HID // LANES
CHUNK = 256
VMEM_LIMIT = 67043328
HBM = pl.BlockSpec(memory_space=pltpu.HBM)


class Fetched:
    def __init__(self, src, dst, sem):
        self.copy, self.ref, self.pending = pltpu.make_async_copy(src, dst, sem), dst, True
        self.copy.start()

    def get(self):
        if self.pending:
            self.copy.wait()
            self.pending = False
        return self.ref


def call(kernel, args, out_shape, scratch_shapes, name, compiler_params):
    spaces = {"vmem": pltpu.VMEM, "smem": pltpu.SMEM}
    moved = [n for n, (_, space) in enumerate(args) if space != "hbm"]
    in_buffers = [spaces[args[n][1]](args[n][0].shape, args[n][0].dtype) for n in moved]
    out_buffers = [pltpu.VMEM(out.shape, out.dtype) for out in out_shape]
    n_in, n_out = len(args), len(out_shape)

    def body(*refs):
        inputs, outputs = refs[:n_in], refs[n_in:n_in + n_out]
        bufs = refs[n_in + n_out:n_in + 2 * n_out + len(moved)]
        scratch, sems, out_sems = refs[n_in + 2 * n_out + len(moved):-2], refs[-2], refs[-1]
        fetched = list(inputs)
        for k, n in enumerate(moved):
            fetched[n] = Fetched(inputs[n], bufs[k], sems.at[k])
        results = bufs[len(moved):]
        stores = {}

        def flush(*buffers):
            for buffer in buffers:
                n = [k for k in range(n_out) if results[k] is buffer][0]
                stores[n] = pltpu.make_async_copy(results[n], outputs[n], out_sems.at[n])
                stores[n].start()

        kernel(*fetched, *results, *scratch, flush=flush)
        for n in moved:
            fetched[n].get()
        flush(*[results[n] for n in range(n_out) if n not in stores])
        for n in range(n_out):
            stores[n].wait()

    return pl.pallas_call(
        body,
        name=name,
        out_shape=out_shape,
        in_specs=[HBM] * n_in,
        out_specs=(HBM,) * n_out,
        scratch_shapes=in_buffers + out_buffers + list(scratch_shapes) + [pltpu.SemaphoreType.DMA((n_in,)), pltpu.SemaphoreType.DMA((n_out,))],
        compiler_params=compiler_params,
    )(*[array for array, _ in args])


def dot(a, b, dims=(((1,), (0,)), ((), ()))):
    return lax.dot_general(a, b, dims, preferred_element_type=F32)


def iota(shape, dim):
    return lax.broadcasted_iota(I32, shape, dim)


def split3(value):
    high = value.astype(BF16)
    rest = value - high.astype(F32)
    mid = rest.astype(BF16)
    low = (rest - mid.astype(F32)).astype(BF16)
    return high, mid, low


def select_rows(onehot, value, dims=(((1,), (0,)), ((), ()))):
    width = value.shape[1]
    picked = dot(onehot, jnp.concatenate(split3(value), axis=1), dims)
    return picked[:, 2 * width:] + picked[:, width:2 * width] + picked[:, :width]


def pad_lanes(value):
    rows, cols = value.shape
    if cols == LANES:
        return value
    return jnp.concatenate([value, jnp.zeros((rows, LANES - cols), value.dtype)], axis=1)


def hub_block(device, groups):
    return lax.rem(device, 2) * (groups // 2) + device // 2


def greet(groups, me):
    barrier = pltpu.get_barrier_semaphore()
    for step in range(1, groups):
        pl.semaphore_signal(barrier, inc=1, device_id={"graph": lax.rem(me + step, groups)}, device_id_type=pl.DeviceIdType.MESH)
    return barrier


def send(src, dst, send_sem, recv_sem, peer):
    copy = pltpu.make_async_remote_copy(
        src_ref=src, dst_ref=dst, send_sem=send_sem, recv_sem=recv_sem,
        device_id={"graph": peer}, device_id_type=pl.DeviceIdType.MESH)
    copy.start()
    return copy


def pack_rows(value):
    half = value.shape[0] // 2
    low = iota((half, LANES), 1) < LANES // 2
    return jnp.where(low, value[:half], pltpu.roll(value[half:], LANES // 2, 1)).astype(BF16)


def unpack_rows(value):
    return jnp.concatenate([value, pltpu.roll(value, LANES // 2, 1)], axis=0)


def gather_kernel(groups, hub_ids, dh, hubrow, xt, send_idx, dst, src, w,
                  xh_ref, hx_ref, dhh_ref, used_ref, db2_ref, wide_ref, *rest, flush):
    lists, (x32, xg, hxg, dhg, dhp, dhs, xs, xr, dhr, ssem, rsem) = rest[:3 * WAYS], rest[3 * WAYS:]
    me = lax.axis_index("graph")
    barrier = greet(groups, me)
    feat, nodes = xt.ref.shape
    hubs = hub_ids.ref.shape[0]
    halo = send_idx.ref.shape[0]
    block = halo // groups
    base = me * nodes
    chips = groups // 2
    core, chip = lax.rem(me, 2), me // 2
    dhg[...] = jnp.zeros_like(dhg)
    hub_ref, dh_ref = hub_ids.get(), dh.get()

    def hub_position_of(k):
        row = hub_ref[k] - base
        return jnp.logical_and(row >= 0, row < nodes), jnp.clip(row, 0, nodes - 1)

    def pick_grad(i, carry):
        for u in range(8):
            k = i * 8 + u
            own, row = hub_position_of(k)
            value = dh_ref[pl.ds(row, 1), :]
            dhg[pl.ds(k, 1), pl.ds(0, value.shape[1])] = jnp.where(own, value, 0.0)
        return carry

    lax.fori_loop(0, hubs // 8, pick_grad, 0)
    pl.semaphore_wait(barrier, groups - 1)
    pair = send(dhg, dhp, ssem.at[1, 0], rsem.at[1, 0], me + 1 - 2 * core)
    eye = (iota((feat, LANES), 0) == iota((feat, LANES), 1)).astype(BF16)
    tags = jnp.where(iota((hubs, LANES), 1) == feat, iota((hubs, LANES), 0) + 1, 0).astype(F32).astype(BF16)
    hubrow = hubrow.get()[...]
    xt_ref = xt.get()
    for row in range(0, nodes, CHUNK):
        owned = (iota((CHUNK, hubs), 0) + (base + row) == hubrow).astype(BF16)
        x32[pl.ds(row, CHUNK), :] = dot(xt_ref[:, pl.ds(row, CHUNK)], eye, CONTRACT_ROWS) + dot(owned, tags)
    send_ref = send_idx.get()

    def pick(i, carry):
        for u in range(16):
            j = i * 16 + u
            xg[pl.ds(j, 1), :] = x32[pl.ds(send_ref[j], 1), :]
        return carry

    lax.fori_loop(0, halo // 16, pick, 0)

    def pick_hub(i, carry):
        for u in range(8):
            k = i * 8 + u
            own, row = hub_position_of(k)
            hxg[pl.ds(k, 1), :] = jnp.where(own, x32[pl.ds(row, 1), :], 0.0)
        return carry

    lax.fori_loop(0, hubs // 8, pick_hub, 0)
    hub_rows = pack_rows(hxg[...])
    for q in range(groups):
        xs[q, pl.ds(0, block // 2), :] = pack_rows(xg[pl.ds(q * block, block), :])
        xs[q, pl.ds(block // 2, hubs // 2), :] = hub_rows
    copies = []
    for step in range(1, groups):
        peer = lax.rem(me + step, groups)
        copies.append(send(xs.at[peer], xr.at[me], ssem.at[0, step], rsem.at[0, step], peer))
    pair.wait()
    dhs[...] = dhg[...] + dhp[...]
    dhr[chip] = dhs[...]
    half = pl.ds(pl.multiple_of(core * (hubs // 2), 8), hubs // 2)
    for step in range(1, chips):
        for other in range(2):
            n = 2 * step + other
            peer = 2 * lax.rem(chip + step, chips) + lax.rem(core + other, 2)
            copies.append(send(dhs.at[half], dhr.at[chip, half], ssem.at[1, n], rsem.at[1, n], peer))
    dst_ref, src_ref, w_ref = dst.get(), src.get(), w.get()
    blocks = w_ref.shape[0]
    for q in range(WAYS):
        part = pl.ds(q, blocks // WAYS, stride=WAYS)
        lists[q][...] = dst_ref[part, :] * TILES
        lists[WAYS + q][...] = src_ref[part, :] * TILES
        lists[2 * WAYS + q][...] = w_ref[part, :]
    flush(*lists)
    diagonal = iota((LANES, LANES), 0) == iota((LANES, LANES), 1)
    ones = jnp.ones((LANES, LANES), BF16)

    def widen(i, carry):
        for q in range(WAYS):
            row = lists[2 * WAYS + q][pl.ds(i, 1), :]
            spread = jnp.zeros((LANES, LANES), F32)
            for piece in reversed(split3(row)):
                column = jnp.where(diagonal, jnp.broadcast_to(piece.astype(F32), (LANES, LANES)), 0.0).astype(BF16)
                spread = spread + dot(column, ones)
            wide_ref[pl.ds(pl.multiple_of((q * (blocks // WAYS) + i) * LANES, LANES), LANES), :] = spread
        return carry

    lax.fori_loop(0, blocks // WAYS, widen, 0)
    flush(wide_ref)
    used = jnp.where(w_ref[...] > 0.0, 1.0, 0.0).sum(axis=0, keepdims=True).sum(axis=1, keepdims=True)
    used_ref[...] = jnp.broadcast_to(used, used_ref.shape).astype(I32)
    total = jnp.zeros((8, dh_ref.shape[1]), F32)
    for row in range(0, nodes, CHUNK):
        total = total + dh_ref[pl.ds(row, CHUNK), :].reshape(CHUNK // 8, 8, dh_ref.shape[1]).sum(axis=0)
    db2_ref[...] = jnp.broadcast_to(pad_lanes(total.sum(axis=0, keepdims=True)), db2_ref.shape)
    flush(used_ref, db2_ref)
    xr[me] = xs[me]
    for copy in copies:
        copy.wait()
    hx = jnp.zeros((hubs // 2, LANES), F32)
    dhh = jnp.zeros((hubs, LANES), F32)
    for q in range(groups):
        xh_ref[pl.ds(q * block, block), :] = unpack_rows(xr[q, pl.ds(0, block // 2), :].astype(F32)).astype(BF16)
        hx = hx + xr[q, pl.ds(block // 2, hubs // 2), :].astype(F32)
    for q in range(chips):
        dhh = dhh + dhr[q]
    hx_ref[...] = unpack_rows(hx)
    dhh_ref[...] = dhh


def hub_position(hub_ref, k, base, nodes, spare):
    row = hub_ref[k] - base
    own = jnp.logical_and(row >= 0, row < nodes)
    return pl.multiple_of(jnp.where(own, row, spare + k) * TILES, TILES)


def trips(used_ref, unroll):
    return (used_ref[0, 0] + (WAYS * LANES - 1)) // (WAYS * LANES) * (LANES // unroll)


def strided(first, rows):
    return pl.ds(first, rows, stride=TILES)


def total_of(refs, where):
    value = refs[0][where, :]
    for ref in refs[1:]:
        value = value + ref[where, :]
    return value


def edges_forward_kernel(copies, unroll, w1, xt, dh, xh, hx, dhh, used, hub_ids, b1, *rest, flush):
    lists, (h1_ref, dz_ref, hz_ref, hub_out, zt, dt), accs = rest[:3 * WAYS], rest[3 * WAYS:3 * WAYS + 6], rest[3 * WAYS + 6:]
    ya, da = accs[:copies], accs[copies:]
    me = lax.axis_index("graph")
    feat, nodes = xt.ref.shape
    halo, hubs = xh.ref.shape[0], hx.ref.shape[0]
    base = me * nodes
    for acc in ya:
        acc[...] = jnp.zeros_like(acc)
    for acc in da:
        acc[strided(0, nodes + halo + 2 * hubs), :] = jnp.zeros((nodes + halo + 2 * hubs, LANES), F32)
    w1 = w1.get()[...]
    xt_ref, dh_ref, xh_ref, hx_ref = xt.get(), dh.get(), xh.get(), hx.get()

    def put_rows(first, z):
        z = z.astype(BF16).astype(F32)
        for c in range(TILES):
            zt[strided(first * TILES + c, z.shape[0]), :] = z[:, c * LANES:(c + 1) * LANES]

    for row in range(0, nodes, CHUNK):
        put_rows(row, dot(xt_ref[:, pl.ds(row, CHUNK)], w1, CONTRACT_ROWS))
        dt[strided(row * TILES, CHUNK), :] = pad_lanes(dh_ref[pl.ds(row, CHUNK), :])
    for row in range(0, halo, CHUNK):
        put_rows(nodes + row, dot(xh_ref[pl.ds(row, CHUNK), pl.ds(0, feat)], w1))
    put_rows(nodes + halo, dot(hx_ref[:, pl.ds(0, feat)].astype(BF16), w1))
    dt[strided(nodes * TILES, hubs), :] = dhh.get()[...]
    used_ref, hub_ref, b1_ref = used.get(), hub_ids.get(), b1.get()
    lists = [item.get() for item in lists]

    def step(i, carry):
        for n in range(unroll * WAYS):
            q, u = n % WAYS, n % copies
            j = i * unroll + n // WAYS
            d4 = pl.multiple_of(lists[q][j], TILES)
            s4 = pl.multiple_of(lists[WAYS + q][j], TILES)
            w = lists[2 * WAYS + q][j]
            y_new = ya[u][pl.ds(d4, TILES), :] + w * zt[pl.ds(s4, TILES), :]
            z_new = da[u][pl.ds(s4, 1), :] + w * dt[pl.ds(d4, 1), :]
            ya[u][pl.ds(d4, TILES), :] = y_new
            da[u][pl.ds(s4, 1), :] = z_new
        return carry

    lax.fori_loop(0, trips(used_ref, unroll), step, 0)

    def fold(i, carry):
        new = []
        for u in range(8):
            k = i * 8 + u
            y_row = hub_position(hub_ref, k, base, nodes, nodes + hubs)
            z_row = hub_position(hub_ref, k, base, nodes, nodes + halo + hubs)
            y_hub = pl.ds(pl.multiple_of((nodes + k) * TILES, TILES), TILES)
            z_hub = pl.ds(pl.multiple_of((nodes + halo + k) * TILES, TILES), 1)
            new.append((y_hub, z_hub, z_row, ya[0][y_hub, :] + total_of(ya, pl.ds(y_row, TILES)), da[0][z_hub, :] + total_of(da, pl.ds(z_row, 1))))
        for y_hub, z_hub, z_row, y_new, z_new in new:
            ya[0][y_hub, :] = y_new
            da[0][z_hub, :] = z_new
            for acc in da:
                acc[pl.ds(z_row, 1), :] = jnp.zeros((1, LANES), F32)
        return carry

    lax.fori_loop(0, hubs // 8, fold, 0)
    for row in range(0, nodes, CHUNK):
        for c in range(TILES):
            cols = pl.ds(c * LANES, LANES)
            y = total_of(ya, strided(row * TILES + c, CHUNK)) + b1_ref[:, cols]
            h1_ref[pl.ds(row, CHUNK), cols] = jnp.maximum(y, 0.0).astype(BF16)
    flush(h1_ref)
    for row in range(0, nodes, CHUNK):
        dz_ref[pl.ds(row, CHUNK), :] = total_of(da, strided(row * TILES, CHUNK))
    flush(dz_ref)
    hz = total_of(da, strided(nodes * TILES, halo))
    tag = xh_ref[...].astype(F32)[:, feat:feat + 1]
    onehot = (tag == (iota((halo, hubs), 1) + 1).astype(F32)).astype(BF16)
    hub_z = total_of(da, strided((nodes + halo) * TILES, hubs)) + select_rows(onehot, hz, CONTRACT_ROWS)
    hz_ref[...] = jnp.where(tag > 0.0, 0.0, hz)
    for c in range(TILES):
        hub_out[:, pl.ds(c * LANES, LANES)] = total_of(ya, strided(nodes * TILES + c, hubs))
    hub_out[:, pl.ds(HID, LANES)] = hub_z


def middle_kernel(groups, hub, hz, dz, b1, w2, sendrow,
                  dz2_ref, dyh_ref, h1h_ref, dz2h_ref,
                  hzr, hubr, dyr, dys, ssem, rsem, flush):
    me = lax.axis_index("graph")
    barrier = greet(groups, me)
    nodes = dz.ref.shape[0]
    out = w2.ref.shape[1]
    home = hub.ref.shape[1]
    block = hz.ref.shape[1]
    halo = groups * block
    hub_ref, hz_ref = hub.get(), hz.get()
    own = hub_block(me, groups)
    hubr[me] = hub_ref[own]
    hzr[me] = jnp.zeros(hzr.shape[1:], F32)
    pl.semaphore_wait(barrier, groups - 1)
    hub_copies, halo_copies, back = [], [], []
    for step in range(1, groups):
        peer = lax.rem(me + step, groups)
        hub_copies.append(send(hub_ref.at[hub_block(peer, groups)], hubr.at[me], ssem.at[0, step], rsem.at[0, step], peer))
    for step in range(1, groups):
        peer = lax.rem(me + step, groups)
        halo_copies.append(send(hz_ref.at[peer], hzr.at[me], ssem.at[1, step], rsem.at[1, step], peer))
    for copy in hub_copies:
        copy.wait()
    total = hubr[0]
    for q in range(1, groups):
        total = total + hubr[q]
    b1_ref, w2_ref, sendrow = b1.get(), w2.get(), sendrow.get()[...]
    pre = total[:, :HID] + b1_ref[...]
    dz2h = total[:, HID:].astype(BF16)
    h1h_ref[...] = jnp.maximum(pre, 0.0).astype(BF16)
    dz2h_ref[...] = dz2h
    dys[...] = jnp.where(pre > 0, dot(dz2h[:, :out], w2_ref[...], CONTRACT_COLS), 0.0)
    for step in range(1, groups):
        peer = lax.rem(me + step, groups)
        back.append(send(dys, dyr.at[own], ssem.at[2, step], rsem.at[2, step], peer))
    dyr[own] = dys[...]
    for copy in halo_copies:
        copy.wait()
    pieces = split3(hzr[...].reshape(halo, LANES))
    dz_ref = dz.get()
    for row in range(0, nodes, CHUNK):
        onehot = (iota((CHUNK, halo), 0) + row == sendrow).astype(BF16)
        value = dz_ref[pl.ds(row, CHUNK), :]
        for piece in reversed(pieces):
            value = value + dot(onehot, piece)
        dz2_ref[pl.ds(row, CHUNK), :] = value.astype(BF16)
    for copy in back:
        copy.wait()
    for q in range(groups):
        dyh_ref[pl.ds(q * home, home), :] = dyr[q]


def edges_backward_kernel(copies, unroll, feat, groups, w2, h1, dz2, dyh, h1h, dz2h, used, hub_ids, xh, db2, wide, *rest, flush):
    lists, rest = rest[:2 * WAYS], rest[2 * WAYS:]
    (dz1_ref, hz_ref, hub_out, dw2_ref, bias_ref, yt), za = rest[:6], rest[6:]
    me = lax.axis_index("graph")
    nodes = h1.ref.shape[0]
    out = w2.ref.shape[1]
    halo, hubs = xh.ref.shape[0], dyh.ref.shape[0]
    home = h1h.ref.shape[0]
    base = me * nodes
    for acc in za:
        acc[...] = jnp.zeros_like(acc)
    w2, h1_ref, dz2_ref, dyh_ref, h1h_ref, dz2h_ref = w2.get()[...], h1.get(), dz2.get(), dyh.get(), h1h.get(), dz2h.get()
    mine = dyh_ref[pl.ds(pl.multiple_of(hub_block(me, groups) * home, 8), home), :]
    db1 = mine
    for row in range(0, nodes, CHUNK):
        rows = pl.ds(row, CHUNK)
        grad = dot(dz2_ref[rows, pl.ds(0, out)], w2, CONTRACT_COLS)
        grad = jnp.where(h1_ref[rows, :] > 0, grad, 0.0)
        db1 = db1 + grad.reshape(CHUNK // 8, 8, HID).sum(axis=0)
        for c in range(TILES):
            yt[strided(row * TILES + c, CHUNK), :] = grad[:, c * LANES:(c + 1) * LANES]
    db1 = db1.sum(axis=0, keepdims=True)
    bias_ref[...] = db2.get()[...]
    for c in range(TILES):
        bias_ref[pl.ds(c, 1), :] = db1[:, c * LANES:(c + 1) * LANES]
        yt[strided(nodes * TILES + c, hubs), :] = dyh_ref[:, pl.ds(c * LANES, LANES)]
    dw2_ref[...] = dot(dz2_ref[...], h1_ref[...], CONTRACT_ROWS) + dot(dz2h_ref[...], h1h_ref[...], CONTRACT_ROWS)
    flush(dw2_ref, bias_ref)
    used_ref, hub_ref, xh_ref, wide_ref = used.get(), hub_ids.get(), xh.get(), wide.get()
    lists = [item.get() for item in lists]
    length = wide_ref.shape[0] // WAYS

    def place(i, carry):
        new = []
        for u in range(8):
            k = i * 8 + u
            new.append((hub_position(hub_ref, k, base, nodes, nodes + hubs), yt[pl.ds(pl.multiple_of((nodes + k) * TILES, TILES), TILES), :]))
        for row, value in new:
            yt[pl.ds(row, TILES), :] = value
        return carry

    lax.fori_loop(0, hubs // 8, place, 0)

    def step(i, carry):
        for n in range(unroll * WAYS):
            q, u = n % WAYS, n % copies
            j = pl.multiple_of(i * unroll, unroll) + n // WAYS
            d4 = pl.multiple_of(lists[q][j], TILES)
            s4 = pl.multiple_of(lists[WAYS + q][j], TILES)
            w = wide_ref[pl.ds(q * length + j, 1), :]
            za[u][pl.ds(s4, TILES), :] = za[u][pl.ds(s4, TILES), :] + w * yt[pl.ds(d4, TILES), :]
        return carry

    lax.fori_loop(0, trips(used_ref, unroll), step, 0)

    def fold(i, carry):
        new = []
        for u in range(8):
            k = i * 8 + u
            row = hub_position(hub_ref, k, base, nodes, nodes + halo + hubs)
            here = pl.ds(pl.multiple_of((nodes + halo + k) * TILES, TILES), TILES)
            new.append((row, here, za[0][here, :] + total_of(za, pl.ds(row, TILES))))
        for row, here, value in new:
            za[0][here, :] = value
            for acc in za:
                acc[pl.ds(row, TILES), :] = jnp.zeros((TILES, LANES), F32)
        return carry

    lax.fori_loop(0, hubs // 8, fold, 0)
    for row in range(0, nodes, CHUNK):
        for c in range(TILES):
            dz1_ref[pl.ds(row, CHUNK), pl.ds(c * LANES, LANES)] = total_of(za, strided(row * TILES + c, CHUNK))
    flush(dz1_ref)
    tag = xh_ref[...].astype(F32)[:, feat:feat + 1]
    onehot = (tag == (iota((halo, hubs), 1) + 1).astype(F32)).astype(BF16)
    for c in range(TILES):
        cols = pl.ds(c * LANES, LANES)
        hz = total_of(za, strided(nodes * TILES + c, halo))
        hub_out[:, cols] = total_of(za, strided((nodes + halo) * TILES + c, hubs)) + select_rows(onehot, hz, CONTRACT_ROWS)
        hz_ref[c] = jnp.where(tag > 0.0, 0.0, hz)


def last_kernel(groups, hub, hz, dw2, bias, sendrow, xt, hx, dz1, w1, hubrow,
                gxt_ref, dw1a, dw2a, bias_out,
                dz_out, onehot, hzr, hubp, hubh, hubr, biasp, biash, biasr, dhs, dha, dw2p, dw2h, dw2r, dw2s, dw1s, dw1r, dw1t, ssem, rsem, flush):
    me = lax.axis_index("graph")
    barrier = greet(groups, me)
    feat, nodes = xt.ref.shape
    chips, home = hub.ref.shape[1:3]
    hubs = groups * home
    block = hz.ref.shape[2]
    halo = groups * block
    base = me * nodes
    core, chip = lax.rem(me, 2), me // 2
    partner = me + 1 - 2 * core
    own = hub_block(me, groups)
    peers = [lax.rem(me + step, groups) for step in range(1, groups)]
    others = [lax.rem(me + 2 * step, groups) for step in range(1, chips)]
    hub_ref, hz_ref, dw2_ref, bias_ref = hub.get(), hz.get(), dw2.get(), bias.get()
    pl.semaphore_wait(barrier, groups - 1)

    def to(devices, slot, src, dst):
        return [send(src(peer), dst, ssem.at[slot, i], rsem.at[slot, i], peer) for i, peer in enumerate(devices)]

    def wait(pending):
        for copy in pending:
            copy.wait()

    pair_copies = (to([partner], 0, lambda p: hub_ref.at[1 - core], hubp) + to([partner], 1, lambda p: dw2_ref.at[1 - core], dw2p)
                   + to([partner], 2, lambda p: bias_ref, biasp))
    halo_copies = [to(peers, 9, lambda p: hz_ref.at[0, p], hzr.at[0, me])]
    sendrow = sendrow.get()[...]
    for row in range(0, nodes, CHUNK):
        onehot[pl.ds(row, CHUNK), :] = (iota((CHUNK, halo), 0) + row == sendrow).astype(BF16)
    for c in range(TILES):
        hzr[c, me] = jnp.zeros((block, LANES), F32)
        dw1s[c] = jnp.zeros(dw1s.shape[1:], F32)
    wait(pair_copies)
    hubh[...] = hub_ref[core] + hubp[...]
    dw2h[...] = dw2_ref[core] + dw2p[...]
    biash[...] = bias_ref[...] + biasp[...]
    hubr[chip] = hubh[chip]
    dw2r[chip] = dw2h[chip]
    biasr[chip] = biash[...]
    hub_copies = to(others, 3, lambda p: hubh.at[p // 2], hubr.at[chip])
    dw2_copies = to(others, 4, lambda p: dw2h.at[p // 2], dw2r.at[chip])
    bias_copies = to(others, 5, lambda p: biash, biasr.at[chip])
    halo_copies += [to(peers, 9 + c, lambda p: hz_ref.at[c, p], hzr.at[c, me]) for c in range(1, TILES)]

    def total_over(ref, count):
        total = ref[0]
        for q in range(1, count):
            total = total + ref[q]
        return total

    xt_ref, dz1_ref, hx_ref, w1, hubrow = xt.get(), dz1.get(), hx.get(), w1.get()[...], hubrow.get()[...]
    wait(hub_copies)
    dz1h = total_over(hubr, chips).astype(BF16)
    dhs[...] = dz1h
    back_copies = to(peers, 6, lambda p: dhs, dha.at[own])
    dha[own] = dz1h
    hx_mine = hx_ref[pl.ds(pl.multiple_of(own * home, 8), home), :].astype(BF16)
    dw1h = dot(hx_mine[:, :feat], dz1h, CONTRACT_ROWS)
    rs_copies, ag_copies = [None] * TILES, [None] * TILES

    def spread(c):
        wait(rs_copies[c])
        total = total_over(dw1r.at[c], groups)
        dw1t[c] = total
        ag_copies[c] = to(peers, 17 + c, lambda p: dw1t.at[c], dw1a.at[c, me])
        dw1a[c, me] = total

    for c in range(TILES):
        wait(halo_copies[c])
        cols = pl.ds(c * LANES, LANES)
        pieces = jnp.concatenate(split3(hzr[c].reshape(halo, LANES)), axis=1)

        def rows_step(i, carry):
            rows = pl.ds(pl.multiple_of(i * CHUNK, CHUNK), CHUNK)
            value = dot(onehot[rows, :], pieces)
            value = value[:, 2 * LANES:] + value[:, LANES:2 * LANES] + value[:, :LANES]
            dz_out[rows, cols] = (dz1_ref[rows, cols] + value).astype(BF16)
            return carry

        lax.fori_loop(0, nodes // CHUNK, rows_step, 0)
        dw1s[c, pl.ds(0, feat), :] = dot(xt_ref[...], dz_out[:, cols]) + dw1h[:, c * LANES:(c + 1) * LANES]
        rs_copies[c] = to(peers, 13 + c, lambda p: dw1s.at[c, pl.ds(pl.multiple_of(p * 8, 8), 8)], dw1r.at[c, me])
        dw1r[c, me] = dw1s[c, pl.ds(pl.multiple_of(me * 8, 8), 8), :]
        if c == 0:
            wait(dw2_copies)
            total = total_over(dw2r, chips)
            dw2s[...] = total
            dw2_back = to(others, 7, lambda p: dw2s, dw2a.at[core, chip])
            dw2a[core, chip] = total
    for c in range(TILES - 1):
        spread(c)
    wait(dw2_back)
    dw2_pair = to([partner], 8, lambda p: dw2a.at[core], dw2a.at[core])
    wait(back_copies)
    hub_rows = dha[...].reshape(hubs, HID)
    for row in range(0, nodes, 2 * CHUNK):
        rows = pl.ds(row, 2 * CHUNK)
        owned = (iota((2 * CHUNK, hubs), 0) + (base + row) == hubrow).astype(BF16)
        dz = (dz_out[rows, :].astype(F32) + dot(owned, hub_rows)).astype(BF16)
        gxt_ref[:, rows] = dot(w1, dz, CONTRACT_COLS)
    flush(gxt_ref)
    wait(bias_copies)
    bias_out[...] = total_over(biasr, chips)
    flush(bias_out)
    spread(TILES - 1)
    wait(dw2_pair)
    flush(dw2a)
    for c in range(TILES):
        wait(ag_copies[c])


def outputs_kernel(gxt, dw2, bias, dw1, gxt_ref, gw1_ref, gw2_ref, gb1_ref, gb2_ref, flush):
    feat, out = gw1_ref.shape[0], gw2_ref.shape[1]
    gxt_ref[...] = gxt.get()[...]
    flush(gxt_ref)
    gw2_ref[...] = dw2.get()[...].T[:, :out]
    flush(gw2_ref)
    bias_ref, dw1_ref = bias.get(), dw1.get()
    for c in range(TILES):
        cols = pl.ds(c * LANES, LANES)
        for q in range(dw1_ref.shape[1]):
            rows = min(8, feat - q * 8)
            if rows > 0:
                gw1_ref[pl.ds(q * 8, rows), cols] = dw1_ref[c, q, pl.ds(0, rows), :]
        gb1_ref[:, cols] = bias_ref[pl.ds(c, 1), :]
    gb2_ref[...] = bias_ref[pl.ds(TILES, 1), pl.ds(0, out)]


def shape(dims, dtype):
    return jax.ShapeDtypeStruct(dims, dtype)


def solution(mesh):
    groups = mesh.shape["graph"]
    vertex_spec = P(("data", "graph"))
    vertex_rows = P(("data", "graph"), None)
    part_spec = P("data")
    part_rows = P("data", None)
    replicated = P()
    copies1, unroll1 = 3, 16
    copies2, unroll2 = 5, 16

    def params(collective_id=None):
        if collective_id is None:
            return pltpu.CompilerParams(vmem_limit_bytes=VMEM_LIMIT)
        return pltpu.CompilerParams(vmem_limit_bytes=VMEM_LIMIT, collective_id=collective_id, has_side_effects=True)

    def device_step(x_loc, dst_loc, src_loc, w_loc, send_loc, hub_ids, w_first, b_first, w_second, dy_out):
        nodes, feat = x_loc.shape
        edges = dst_loc.shape[0]
        halo = send_loc.shape[0]
        hubs = hub_ids.shape[0]
        out = dy_out.shape[1]
        block, home = halo // groups, hubs // groups
        src_rows, dst_rows = nodes + halo + 2 * hubs, nodes + 2 * hubs
        x_t = x_loc.T
        hub_lanes = hub_ids.reshape(1, hubs)
        send_lanes = send_loc.reshape(1, halo)
        bias = b_first.reshape(1, HID)
        sems = lambda n: [pltpu.SemaphoreType.DMA((n, groups)), pltpu.SemaphoreType.DMA((n, groups))]
        table = lambda a: a.reshape(edges // LANES, LANES)
        part_list = (edges // LANES // WAYS, LANES)
        packed = (block + hubs) // 2

        xh, hx, dhh, used, db2, wide, *lists = call(
            functools.partial(gather_kernel, groups),
            [(hub_ids, "smem"), (dy_out, "vmem"), (hub_lanes, "vmem"), (x_t, "vmem"), (send_loc, "smem"),
             (table(dst_loc), "vmem"), (table(src_loc), "vmem"), (table(w_loc), "vmem")],
            (shape((halo, LANES), BF16), shape((hubs, LANES), F32), shape((hubs, LANES), F32),
             shape((8, LANES), I32), shape((8, LANES), F32), shape((edges, LANES), F32))
            + (shape(part_list, I32),) * (2 * WAYS) + (shape(part_list, F32),) * WAYS,
            [pltpu.VMEM((nodes, LANES), F32), pltpu.VMEM((halo, LANES), F32), pltpu.VMEM((hubs, LANES), F32),
             pltpu.VMEM((hubs, LANES), F32), pltpu.VMEM((hubs, LANES), F32), pltpu.VMEM((hubs, LANES), F32),
             pltpu.VMEM((groups, packed, LANES), BF16), pltpu.VMEM((groups, packed, LANES), BF16),
             pltpu.VMEM((groups // 2, hubs, LANES), F32)] + sems(2),
            "gather_rows", params(0))
        lists = [(item.reshape(edges // WAYS), "smem") for item in lists]

        h1, dz, hz, hub = call(
            functools.partial(edges_forward_kernel, copies1, unroll1),
            [(w_first, "vmem"), (x_t, "vmem"), (dy_out, "vmem"), (xh, "vmem"), (hx, "vmem"), (dhh, "vmem"),
             (used, "smem"), (hub_ids, "smem"), (bias, "vmem")] + lists,
            (shape((nodes, HID), BF16), shape((nodes, LANES), F32), shape((halo, LANES), F32), shape((hubs, HID + LANES), F32)),
            [pltpu.VMEM((src_rows * TILES, LANES), F32), pltpu.VMEM((dst_rows * TILES, LANES), F32)]
            + [pltpu.VMEM((dst_rows * TILES, LANES), F32)] * copies1 + [pltpu.VMEM((src_rows * TILES, LANES), F32)] * copies1,
            "edges_forward", params())

        dz2, dyh, h1h, dz2h = call(
            functools.partial(middle_kernel, groups),
            [(hub.reshape(groups, home, HID + LANES), "vmem"), (hz.reshape(groups, block, LANES), "vmem"), (dz, "vmem"),
             (bias, "vmem"), (w_second, "vmem"), (send_lanes, "vmem")],
            (shape((nodes, LANES), BF16), shape((hubs, HID), F32), shape((home, HID), BF16), shape((home, LANES), BF16)),
            [pltpu.VMEM((groups, block, LANES), F32), pltpu.VMEM((groups, home, HID + LANES), F32),
             pltpu.VMEM((groups, home, HID), F32), pltpu.VMEM((home, HID), F32)] + sems(3),
            "middle", params(1))

        dz1, hz1, hub1, dw2, biases = call(
            functools.partial(edges_backward_kernel, copies2, unroll2, feat, groups),
            [(w_second, "vmem"), (h1, "vmem"), (dz2, "vmem"), (dyh, "vmem"), (h1h, "vmem"), (dz2h, "vmem"),
             (used, "smem"), (hub_ids, "smem"), (xh, "vmem"), (db2, "vmem"), (wide, "vmem")] + lists[:2 * WAYS],
            (shape((nodes, HID), F32), shape((TILES, halo, LANES), F32), shape((hubs, HID), F32), shape((LANES, HID), F32), shape((8, LANES), F32)),
            [pltpu.VMEM((dst_rows * TILES, LANES), F32)] + [pltpu.VMEM((src_rows * TILES, LANES), F32)] * copies2,
            "edges_backward", params())

        chips = groups // 2
        part = LANES // groups
        grad_xt, dw1, dw2, biases = call(
            functools.partial(last_kernel, groups),
            [(hub1.reshape(2, chips, home, HID), "vmem"), (hz1.reshape(TILES, groups, block, LANES), "vmem"),
             (dw2.reshape(2, chips, part, HID), "vmem"), (biases, "vmem"), (send_lanes, "vmem"), (x_t, "vmem"), (hx, "vmem"),
             (dz1, "vmem"), (w_first, "vmem"), (hub_lanes, "vmem")],
            (shape((feat, nodes), F32), shape((TILES, groups, 8, LANES), F32), shape((2, chips, part, HID), F32), shape((8, LANES), F32)),
            [pltpu.VMEM((nodes, HID), BF16), pltpu.VMEM((nodes, halo), BF16), pltpu.VMEM((TILES, groups, block, LANES), F32)]
            + [pltpu.VMEM((chips, home, HID), F32)] * 3 + [pltpu.VMEM((8, LANES), F32)] * 2 + [pltpu.VMEM((chips, 8, LANES), F32)]
            + [pltpu.VMEM((home, HID), BF16), pltpu.VMEM((groups, home, HID), BF16)]
            + [pltpu.VMEM((chips, part, HID), F32)] * 3 + [pltpu.VMEM((part, HID), F32)]
            + [pltpu.VMEM((TILES, groups * 8, LANES), F32), pltpu.VMEM((TILES, groups, 8, LANES), F32), pltpu.VMEM((TILES, 8, LANES), F32)] + sems(21),
            "last_exchange", params(2))

        grad_xt, grad_w1, grad_w2, grad_b1, grad_b2 = call(
            outputs_kernel,
            [(grad_xt, "vmem"), (dw2.reshape(LANES, HID), "vmem"), (biases, "vmem"), (dw1, "vmem")],
            (shape((feat, nodes), F32), shape((feat, HID), F32), shape((HID, out), F32), shape((1, HID), F32), shape((1, out), F32)),
            [], "outputs", params())
        return grad_xt.T, grad_w1, grad_w2, grad_b1.reshape(HID), grad_b2.reshape(out)

    return jax.shard_map(
        device_step,
        mesh=mesh,
        in_specs=(vertex_rows, vertex_spec, vertex_spec, vertex_spec, vertex_spec, part_spec, replicated, replicated, replicated, vertex_rows),
        out_specs=(vertex_rows, part_rows, part_rows, part_spec, part_spec),
        check_vma=False,
    )
```

```python
import functools

import jax
import jax.numpy as jnp
from jax import lax
from jax.experimental import pallas as pl
from jax.experimental.pallas import tpu as pltpu
from jax.sharding import PartitionSpec as P

F32, BF16, I32 = jnp.float32, jnp.bfloat16, jnp.int32
CONTRACT_ROWS = (((0,), (0,)), ((), ()))
CONTRACT_COLS = (((1,), (1,)), ((), ()))
LANES = 128
WAYS = 4
HID = 512
TILES = HID // LANES
CHUNK = 256
TALL = 1024
VMEM_LIMIT = 67043328
HBM = pl.BlockSpec(memory_space=pltpu.HBM)


class Fetched:
    def __init__(self, src, dst, sem):
        self.copy, self.ref, self.pending = pltpu.make_async_copy(src, dst, sem), dst, True
        self.copy.start()

    def get(self):
        if self.pending:
            self.copy.wait()
            self.pending = False
        return self.ref


def call(kernel, args, out_shape, scratch_shapes, name, compiler_params):
    spaces = {"vmem": pltpu.VMEM, "smem": pltpu.SMEM}
    moved = [n for n, (_, space) in enumerate(args) if space != "hbm"]
    in_buffers = [spaces[args[n][1]](args[n][0].shape, args[n][0].dtype) for n in moved]
    out_buffers = [pltpu.VMEM(out.shape, out.dtype) for out in out_shape]
    n_in, n_out = len(args), len(out_shape)

    def body(*refs):
        inputs, outputs = refs[:n_in], refs[n_in:n_in + n_out]
        bufs = refs[n_in + n_out:n_in + 2 * n_out + len(moved)]
        scratch, sems, out_sems = refs[n_in + 2 * n_out + len(moved):-2], refs[-2], refs[-1]
        fetched = list(inputs)
        for k, n in enumerate(moved):
            fetched[n] = Fetched(inputs[n], bufs[k], sems.at[k])
        results = bufs[len(moved):]
        stores = {}

        def flush(*buffers):
            for buffer in buffers:
                n = [k for k in range(n_out) if results[k] is buffer][0]
                stores[n] = pltpu.make_async_copy(results[n], outputs[n], out_sems.at[n])
                stores[n].start()

        kernel(*fetched, *results, *scratch, flush=flush)
        for n in moved:
            fetched[n].get()
        flush(*[results[n] for n in range(n_out) if n not in stores])
        for n in range(n_out):
            stores[n].wait()

    return pl.pallas_call(
        body,
        name=name,
        out_shape=out_shape,
        in_specs=[HBM] * n_in,
        out_specs=(HBM,) * n_out,
        scratch_shapes=in_buffers + out_buffers + list(scratch_shapes) + [pltpu.SemaphoreType.DMA((n_in,)), pltpu.SemaphoreType.DMA((n_out,))],
        compiler_params=compiler_params,
    )(*[array for array, _ in args])


def dot(a, b, dims=(((1,), (0,)), ((), ()))):
    return lax.dot_general(a, b, dims, preferred_element_type=F32)


def iota(shape, dim):
    return lax.broadcasted_iota(I32, shape, dim)


def split3(value):
    high = value.astype(BF16)
    rest = value - high.astype(F32)
    mid = rest.astype(BF16)
    low = (rest - mid.astype(F32)).astype(BF16)
    return high, mid, low


def select_rows(onehot, value, dims=(((1,), (0,)), ((), ()))):
    width = value.shape[1]
    picked = dot(onehot, jnp.concatenate(split3(value), axis=1), dims)
    return picked[:, 2 * width:] + picked[:, width:2 * width] + picked[:, :width]


def pad_lanes(value):
    rows, cols = value.shape
    if cols == LANES:
        return value
    return jnp.concatenate([value, jnp.zeros((rows, LANES - cols), value.dtype)], axis=1)


def hub_block(device, groups):
    return lax.rem(device, 2) * (groups // 2) + device // 2


def greet(groups, me):
    barrier = pltpu.get_barrier_semaphore()
    for step in range(1, groups):
        pl.semaphore_signal(barrier, inc=1, device_id={"graph": lax.rem(me + step, groups)}, device_id_type=pl.DeviceIdType.MESH)
    return barrier


def send(src, dst, send_sem, recv_sem, peer):
    copy = pltpu.make_async_remote_copy(
        src_ref=src, dst_ref=dst, send_sem=send_sem, recv_sem=recv_sem,
        device_id={"graph": peer}, device_id_type=pl.DeviceIdType.MESH)
    copy.start()
    return copy


def pack_rows(value):
    half = value.shape[0] // 2
    low = iota((half, LANES), 1) < LANES // 2
    return jnp.where(low, value[:half], pltpu.roll(value[half:], LANES // 2, 1)).astype(BF16)


def unpack_rows(value):
    return jnp.concatenate([value, pltpu.roll(value, LANES // 2, 1)], axis=0)


def gather_kernel(groups, hub_ids, dh, hubrow, xt, send_idx, dst, src, w,
                  xh_ref, hx_ref, dhh_ref, used_ref, db2_ref, wide_ref, *rest, flush):
    lists, (x32, xg, hxg, dhg, dhp, dhs, xs, xr, dhr, ssem, rsem) = rest[:3 * WAYS], rest[3 * WAYS:]
    me = lax.axis_index("graph")
    barrier = greet(groups, me)
    feat, nodes = xt.ref.shape
    hubs = hub_ids.ref.shape[0]
    halo = send_idx.ref.shape[0]
    block = halo // groups
    base = me * nodes
    chips = groups // 2
    core, chip = lax.rem(me, 2), me // 2
    dhg[...] = jnp.zeros_like(dhg)
    hub_ref, dh_ref = hub_ids.get(), dh.get()

    def hub_position_of(k):
        row = hub_ref[k] - base
        return jnp.logical_and(row >= 0, row < nodes), jnp.clip(row, 0, nodes - 1)

    def pick_grad(i, carry):
        for u in range(8):
            k = i * 8 + u
            own, row = hub_position_of(k)
            value = dh_ref[pl.ds(row, 1), :]
            dhg[pl.ds(k, 1), pl.ds(0, value.shape[1])] = jnp.where(own, value, 0.0)
        return carry

    lax.fori_loop(0, hubs // 8, pick_grad, 0)
    pl.semaphore_wait(barrier, groups - 1)
    pair = send(dhg, dhp, ssem.at[1, 0], rsem.at[1, 0], me + 1 - 2 * core)
    eye = (iota((feat, LANES), 0) == iota((feat, LANES), 1)).astype(BF16)
    tags = jnp.where(iota((hubs, LANES), 1) == feat, iota((hubs, LANES), 0) + 1, 0).astype(F32).astype(BF16)
    hubrow = hubrow.get()[...]
    xt_ref = xt.get()
    for row in range(0, nodes, CHUNK):
        owned = (iota((CHUNK, hubs), 0) + (base + row) == hubrow).astype(BF16)
        x32[pl.ds(row, CHUNK), :] = dot(xt_ref[:, pl.ds(row, CHUNK)], eye, CONTRACT_ROWS) + dot(owned, tags)
    send_ref = send_idx.get()

    def pick(i, carry):
        for u in range(16):
            j = i * 16 + u
            xg[pl.ds(j, 1), :] = x32[pl.ds(send_ref[j], 1), :]
        return carry

    lax.fori_loop(0, halo // 16, pick, 0)

    def pick_hub(i, carry):
        for u in range(8):
            k = i * 8 + u
            own, row = hub_position_of(k)
            hxg[pl.ds(k, 1), :] = jnp.where(own, x32[pl.ds(row, 1), :], 0.0)
        return carry

    lax.fori_loop(0, hubs // 8, pick_hub, 0)
    hub_rows = pack_rows(hxg[...])
    for q in range(groups):
        xs[q, pl.ds(0, block // 2), :] = pack_rows(xg[pl.ds(q * block, block), :])
        xs[q, pl.ds(block // 2, hubs // 2), :] = hub_rows
    copies = []
    for step in range(1, groups):
        peer = lax.rem(me + step, groups)
        copies.append(send(xs.at[peer], xr.at[me], ssem.at[0, step], rsem.at[0, step], peer))
    pair.wait()
    dhs[...] = dhg[...] + dhp[...]
    dhr[chip] = dhs[...]
    half = pl.ds(pl.multiple_of(core * (hubs // 2), 8), hubs // 2)
    for step in range(1, chips):
        for other in range(2):
            n = 2 * step + other
            peer = 2 * lax.rem(chip + step, chips) + lax.rem(core + other, 2)
            copies.append(send(dhs.at[half], dhr.at[chip, half], ssem.at[1, n], rsem.at[1, n], peer))
    dst_ref, src_ref, w_ref = dst.get(), src.get(), w.get()
    blocks = w_ref.shape[0]
    for q in range(WAYS):
        part = pl.ds(q, blocks // WAYS, stride=WAYS)
        lists[q][...] = dst_ref[part, :] * TILES
        lists[WAYS + q][...] = src_ref[part, :] * TILES
        lists[2 * WAYS + q][...] = w_ref[part, :]
    flush(*lists)
    diagonal = iota((LANES, LANES), 0) == iota((LANES, LANES), 1)
    ones = jnp.ones((LANES, LANES), BF16)

    def widen(i, carry):
        for q in range(WAYS):
            row = lists[2 * WAYS + q][pl.ds(i, 1), :]
            spread = jnp.zeros((LANES, LANES), F32)
            for piece in reversed(split3(row)):
                column = jnp.where(diagonal, jnp.broadcast_to(piece.astype(F32), (LANES, LANES)), 0.0).astype(BF16)
                spread = spread + dot(column, ones)
            wide_ref[pl.ds(pl.multiple_of((q * (blocks // WAYS) + i) * LANES, LANES), LANES), :] = spread
        return carry

    lax.fori_loop(0, blocks // WAYS, widen, 0)
    flush(wide_ref)
    used = jnp.where(w_ref[...] > 0.0, 1.0, 0.0).sum(axis=0, keepdims=True).sum(axis=1, keepdims=True)
    used_ref[...] = jnp.broadcast_to(used, used_ref.shape).astype(I32)
    total = jnp.zeros((8, dh_ref.shape[1]), F32)
    for row in range(0, nodes, CHUNK):
        total = total + dh_ref[pl.ds(row, CHUNK), :].reshape(CHUNK // 8, 8, dh_ref.shape[1]).sum(axis=0)
    db2_ref[...] = jnp.broadcast_to(pad_lanes(total.sum(axis=0, keepdims=True)), db2_ref.shape)
    flush(used_ref, db2_ref)
    xr[me] = xs[me]
    for copy in copies:
        copy.wait()
    hx = jnp.zeros((hubs // 2, LANES), F32)
    dhh = jnp.zeros((hubs, LANES), F32)
    for q in range(groups):
        xh_ref[pl.ds(q * block, block), :] = unpack_rows(xr[q, pl.ds(0, block // 2), :].astype(F32)).astype(BF16)
        hx = hx + xr[q, pl.ds(block // 2, hubs // 2), :].astype(F32)
    for q in range(chips):
        dhh = dhh + dhr[q]
    hx_ref[...] = unpack_rows(hx)
    dhh_ref[...] = dhh


def hub_position(hub_ref, k, base, nodes, spare):
    row = hub_ref[k] - base
    own = jnp.logical_and(row >= 0, row < nodes)
    return pl.multiple_of(jnp.where(own, row, spare + k) * TILES, TILES)


def trips(used_ref, unroll):
    return (used_ref[0, 0] + (WAYS * LANES - 1)) // (WAYS * LANES) * (LANES // unroll)


def strided(first, rows):
    return pl.ds(first, rows, stride=TILES)


def total_of(refs, where):
    value = refs[0][where, :]
    for ref in refs[1:]:
        value = value + ref[where, :]
    return value


def edges_forward_kernel(copies, unroll, w1, xt, dh, xh, hx, dhh, used, hub_ids, b1, *rest, flush):
    lists, (h1_ref, dz_ref, hz_ref, hub_out, zt, dt), accs = rest[:3 * WAYS], rest[3 * WAYS:3 * WAYS + 6], rest[3 * WAYS + 6:]
    ya, da = accs[:copies], accs[copies:]
    me = lax.axis_index("graph")
    feat, nodes = xt.ref.shape
    halo, hubs = xh.ref.shape[0], hx.ref.shape[0]
    base = me * nodes
    for acc in ya:
        acc[...] = jnp.zeros_like(acc)
    for acc in da:
        acc[strided(0, nodes + halo + 2 * hubs), :] = jnp.zeros((nodes + halo + 2 * hubs, LANES), F32)
    w1 = w1.get()[...]
    xt_ref, dh_ref, xh_ref, hx_ref = xt.get(), dh.get(), xh.get(), hx.get()

    def put_rows(first, z):
        z = z.astype(BF16).astype(F32)
        for c in range(TILES):
            zt[strided(first * TILES + c, z.shape[0]), :] = z[:, c * LANES:(c + 1) * LANES]

    for row in range(0, nodes, CHUNK):
        put_rows(row, dot(xt_ref[:, pl.ds(row, CHUNK)], w1, CONTRACT_ROWS))
        dt[strided(row * TILES, CHUNK), :] = pad_lanes(dh_ref[pl.ds(row, CHUNK), :])
    for row in range(0, halo, CHUNK):
        put_rows(nodes + row, dot(xh_ref[pl.ds(row, CHUNK), pl.ds(0, feat)], w1))
    put_rows(nodes + halo, dot(hx_ref[:, pl.ds(0, feat)].astype(BF16), w1))
    dt[strided(nodes * TILES, hubs), :] = dhh.get()[...]
    used_ref, hub_ref, b1_ref = used.get(), hub_ids.get(), b1.get()
    lists = [item.get() for item in lists]

    def step(i, carry):
        for n in range(unroll * WAYS):
            q, u = n % WAYS, n % copies
            j = i * unroll + n // WAYS
            d4 = pl.multiple_of(lists[q][j], TILES)
            s4 = pl.multiple_of(lists[WAYS + q][j], TILES)
            w = lists[2 * WAYS + q][j]
            y_new = ya[u][pl.ds(d4, TILES), :] + w * zt[pl.ds(s4, TILES), :]
            z_new = da[u][pl.ds(s4, 1), :] + w * dt[pl.ds(d4, 1), :]
            ya[u][pl.ds(d4, TILES), :] = y_new
            da[u][pl.ds(s4, 1), :] = z_new
        return carry

    lax.fori_loop(0, trips(used_ref, unroll), step, 0)

    def fold(i, carry):
        new = []
        for u in range(8):
            k = i * 8 + u
            y_row = hub_position(hub_ref, k, base, nodes, nodes + hubs)
            z_row = hub_position(hub_ref, k, base, nodes, nodes + halo + hubs)
            y_hub = pl.ds(pl.multiple_of((nodes + k) * TILES, TILES), TILES)
            z_hub = pl.ds(pl.multiple_of((nodes + halo + k) * TILES, TILES), 1)
            new.append((y_hub, z_hub, z_row, ya[0][y_hub, :] + total_of(ya, pl.ds(y_row, TILES)), da[0][z_hub, :] + total_of(da, pl.ds(z_row, 1))))
        for y_hub, z_hub, z_row, y_new, z_new in new:
            ya[0][y_hub, :] = y_new
            da[0][z_hub, :] = z_new
            for acc in da:
                acc[pl.ds(z_row, 1), :] = jnp.zeros((1, LANES), F32)
        return carry

    lax.fori_loop(0, hubs // 8, fold, 0)
    for row in range(0, nodes, CHUNK):
        for c in range(TILES):
            cols = pl.ds(c * LANES, LANES)
            y = total_of(ya, strided(row * TILES + c, CHUNK)) + b1_ref[:, cols]
            h1_ref[pl.ds(row, CHUNK), cols] = jnp.maximum(y, 0.0).astype(BF16)
    flush(h1_ref)
    for row in range(0, nodes, CHUNK):
        dz_ref[pl.ds(row, CHUNK), :] = total_of(da, strided(row * TILES, CHUNK))
    flush(dz_ref)
    hz = total_of(da, strided(nodes * TILES, halo))
    tag = xh_ref[...].astype(F32)[:, feat:feat + 1]
    onehot = (tag == (iota((halo, hubs), 1) + 1).astype(F32)).astype(BF16)
    hub_z = total_of(da, strided((nodes + halo) * TILES, hubs)) + select_rows(onehot, hz, CONTRACT_ROWS)
    hz_ref[...] = jnp.where(tag > 0.0, 0.0, hz)
    for c in range(TILES):
        hub_out[:, pl.ds(c * LANES, LANES)] = total_of(ya, strided(nodes * TILES + c, hubs))
    hub_out[:, pl.ds(HID, LANES)] = hub_z


def middle_kernel(groups, hub, hz, dz, b1, w2, sendrow,
                  dz2_ref, dyh_ref, h1h_ref, dz2h_ref,
                  hzr, hubr, dyr, dys, ssem, rsem, flush):
    me = lax.axis_index("graph")
    barrier = greet(groups, me)
    nodes = dz.ref.shape[0]
    out = w2.ref.shape[1]
    home = hub.ref.shape[1]
    block = hz.ref.shape[1]
    halo = groups * block
    hub_ref, hz_ref = hub.get(), hz.get()
    own = hub_block(me, groups)
    hubr[me] = hub_ref[own]
    hzr[me] = jnp.zeros(hzr.shape[1:], F32)
    pl.semaphore_wait(barrier, groups - 1)
    hub_copies, halo_copies, back = [], [], []
    for step in range(1, groups):
        peer = lax.rem(me + step, groups)
        hub_copies.append(send(hub_ref.at[hub_block(peer, groups)], hubr.at[me], ssem.at[0, step], rsem.at[0, step], peer))
    for step in range(1, groups):
        peer = lax.rem(me + step, groups)
        halo_copies.append(send(hz_ref.at[peer], hzr.at[me], ssem.at[1, step], rsem.at[1, step], peer))
    for copy in hub_copies:
        copy.wait()
    total = hubr[0]
    for q in range(1, groups):
        total = total + hubr[q]
    b1_ref, w2_ref, sendrow = b1.get(), w2.get(), sendrow.get()[...]
    pre = total[:, :HID] + b1_ref[...]
    dz2h = total[:, HID:].astype(BF16)
    h1h_ref[...] = jnp.maximum(pre, 0.0).astype(BF16)
    dz2h_ref[...] = dz2h
    dys[...] = jnp.where(pre > 0, dot(dz2h[:, :out], w2_ref[...], CONTRACT_COLS), 0.0)
    for step in range(1, groups):
        peer = lax.rem(me + step, groups)
        back.append(send(dys, dyr.at[own], ssem.at[2, step], rsem.at[2, step], peer))
    dyr[own] = dys[...]
    for copy in halo_copies:
        copy.wait()
    pieces = split3(hzr[...].reshape(halo, LANES))
    dz_ref = dz.get()
    for row in range(0, nodes, CHUNK):
        onehot = (iota((CHUNK, halo), 0) + row == sendrow).astype(BF16)
        value = dz_ref[pl.ds(row, CHUNK), :]
        for piece in reversed(pieces):
            value = value + dot(onehot, piece)
        dz2_ref[pl.ds(row, CHUNK), :] = value.astype(BF16)
    for copy in back:
        copy.wait()
    for q in range(groups):
        dyh_ref[pl.ds(q * home, home), :] = dyr[q]


def edges_backward_kernel(copies, unroll, feat, groups, w2, h1, dz2, dyh, h1h, dz2h, used, hub_ids, xh, db2, wide, *rest, flush):
    lists, rest = rest[:2 * WAYS], rest[2 * WAYS:]
    (dz1_ref, hz_ref, hub_out, dw2_ref, bias_ref, yt), za = rest[:6], rest[6:]
    me = lax.axis_index("graph")
    nodes = h1.ref.shape[0]
    out = w2.ref.shape[1]
    halo, hubs = xh.ref.shape[0], dyh.ref.shape[0]
    home = h1h.ref.shape[0]
    base = me * nodes
    for acc in za:
        acc[...] = jnp.zeros_like(acc)
    w2, h1_ref, dz2_ref, dyh_ref, h1h_ref, dz2h_ref = w2.get()[...], h1.get(), dz2.get(), dyh.get(), h1h.get(), dz2h.get()
    mine = dyh_ref[pl.ds(pl.multiple_of(hub_block(me, groups) * home, 8), home), :]
    db1 = mine
    for row in range(0, nodes, CHUNK):
        rows = pl.ds(row, CHUNK)
        grad = dot(dz2_ref[rows, pl.ds(0, out)], w2, CONTRACT_COLS)
        grad = jnp.where(h1_ref[rows, :] > 0, grad, 0.0)
        db1 = db1 + grad.reshape(CHUNK // 8, 8, HID).sum(axis=0)
        for c in range(TILES):
            yt[strided(row * TILES + c, CHUNK), :] = grad[:, c * LANES:(c + 1) * LANES]
    db1 = db1.sum(axis=0, keepdims=True)
    bias_ref[...] = db2.get()[...]
    for c in range(TILES):
        bias_ref[pl.ds(c, 1), :] = db1[:, c * LANES:(c + 1) * LANES]
        yt[strided(nodes * TILES + c, hubs), :] = dyh_ref[:, pl.ds(c * LANES, LANES)]
    dw2_ref[...] = dot(dz2_ref[...], h1_ref[...], CONTRACT_ROWS) + dot(dz2h_ref[...], h1h_ref[...], CONTRACT_ROWS)
    flush(dw2_ref, bias_ref)
    used_ref, hub_ref, xh_ref, wide_ref = used.get(), hub_ids.get(), xh.get(), wide.get()
    lists = [item.get() for item in lists]
    length = wide_ref.shape[0] // WAYS

    def place(i, carry):
        new = []
        for u in range(8):
            k = i * 8 + u
            new.append((hub_position(hub_ref, k, base, nodes, nodes + hubs), yt[pl.ds(pl.multiple_of((nodes + k) * TILES, TILES), TILES), :]))
        for row, value in new:
            yt[pl.ds(row, TILES), :] = value
        return carry

    lax.fori_loop(0, hubs // 8, place, 0)

    def step(i, carry):
        for n in range(unroll * WAYS):
            q, u = n % WAYS, n % copies
            j = pl.multiple_of(i * unroll, unroll) + n // WAYS
            d4 = pl.multiple_of(lists[q][j], TILES)
            s4 = pl.multiple_of(lists[WAYS + q][j], TILES)
            w = wide_ref[pl.ds(q * length + j, 1), :]
            za[u][pl.ds(s4, TILES), :] = za[u][pl.ds(s4, TILES), :] + w * yt[pl.ds(d4, TILES), :]
        return carry

    lax.fori_loop(0, trips(used_ref, unroll), step, 0)

    def fold(i, carry):
        new = []
        for u in range(8):
            k = i * 8 + u
            row = hub_position(hub_ref, k, base, nodes, nodes + halo + hubs)
            here = pl.ds(pl.multiple_of((nodes + halo + k) * TILES, TILES), TILES)
            new.append((row, here, za[0][here, :] + total_of(za, pl.ds(row, TILES))))
        for row, here, value in new:
            za[0][here, :] = value
            for acc in za:
                acc[pl.ds(row, TILES), :] = jnp.zeros((TILES, LANES), F32)
        return carry

    lax.fori_loop(0, hubs // 8, fold, 0)
    for row in range(0, nodes, CHUNK):
        for c in range(TILES):
            dz1_ref[pl.ds(row, CHUNK), pl.ds(c * LANES, LANES)] = total_of(za, strided(row * TILES + c, CHUNK))
    flush(dz1_ref)
    tag = xh_ref[...].astype(F32)[:, feat:feat + 1]
    onehot = (tag == (iota((halo, hubs), 1) + 1).astype(F32)).astype(BF16)
    for c in range(TILES):
        cols = pl.ds(c * LANES, LANES)
        hz = total_of(za, strided(nodes * TILES + c, halo))
        hub_out[:, cols] = total_of(za, strided((nodes + halo) * TILES + c, hubs)) + select_rows(onehot, hz, CONTRACT_ROWS)
        hz_ref[c] = jnp.where(tag > 0.0, 0.0, hz)


def last_kernel(groups, hub, hz, dw2, bias, sendrow, xt, hx, dz1, w1, hubrow,
                gxt_ref, dw1a, dw2a, bias_out,
                dz_out, onehot, hzr, hubp, hubh, hubr, biasp, biash, biasr, dhs, dha, dw2p, dw2h, dw2r, dw2s, dw1s, dw1r, dw1t, ssem, rsem, flush):
    me = lax.axis_index("graph")
    barrier = greet(groups, me)
    feat, nodes = xt.ref.shape
    chips, home = hub.ref.shape[1:3]
    hubs = groups * home
    block = hz.shape[2]
    halo = groups * block
    base = me * nodes
    core, chip = lax.rem(me, 2), me // 2
    partner = me + 1 - 2 * core
    own = hub_block(me, groups)
    peers = [lax.rem(me + step, groups) for step in range(1, groups)]
    others = [lax.rem(me + 2 * step, groups) for step in range(1, chips)]
    pl.semaphore_wait(barrier, groups - 1)

    def to(devices, slot, src, dst):
        return [send(src(peer), dst, ssem.at[slot, i], rsem.at[slot, i], peer) for i, peer in enumerate(devices)]

    def wait(pending):
        for copy in pending:
            copy.wait()

    halo_copies = [to(peers, 9, lambda p: hz.at[0, p], hzr.at[0, me])]
    hub_ref, dw2_ref, bias_ref = hub.get(), dw2.get(), bias.get()
    pair_copies = (to([partner], 0, lambda p: hub_ref.at[1 - core], hubp) + to([partner], 1, lambda p: dw2_ref.at[1 - core], dw2p)
                   + to([partner], 2, lambda p: bias_ref, biasp))
    sendrow = sendrow.get()[...]
    for row in range(0, nodes, CHUNK):
        onehot[pl.ds(row, CHUNK), :] = (iota((CHUNK, halo), 0) + row == sendrow).astype(BF16)
    for c in range(TILES):
        hzr[c, me] = jnp.zeros((block, LANES), F32)
        dw1s[c] = jnp.zeros(dw1s.shape[1:], F32)
    wait(pair_copies)
    hubh[...] = hub_ref[core] + hubp[...]
    dw2h[...] = dw2_ref[core] + dw2p[...]
    biash[...] = bias_ref[...] + biasp[...]
    hubr[chip] = hubh[chip]
    dw2r[chip] = dw2h[chip]
    biasr[chip] = biash[...]
    hub_copies = to(others, 3, lambda p: hubh.at[p // 2], hubr.at[chip])
    dw2_copies = to(others, 4, lambda p: dw2h.at[p // 2], dw2r.at[chip])
    bias_copies = to(others, 5, lambda p: biash, biasr.at[chip])
    halo_copies += [to(peers, 9 + c, lambda p: hz.at[c, p], hzr.at[c, me]) for c in range(1, TILES)]

    def total_over(ref, count):
        total = ref[0]
        for q in range(1, count):
            total = total + ref[q]
        return total

    xt_ref, dz1_ref, hx_ref, w1, hubrow = xt.get(), dz1.get(), hx.get(), w1.get()[...], hubrow.get()[...]
    rs_copies, ag_copies = [None] * TILES, [None] * TILES

    def spread(c):
        wait(rs_copies[c])
        total = total_over(dw1r.at[c], groups)
        dw1t[c] = total
        ag_copies[c] = to(peers, 17 + c, lambda p: dw1t.at[c], dw1a.at[c, me])
        dw1a[c, me] = total

    for c in range(TILES):
        wait(halo_copies[c])
        cols = pl.ds(c * LANES, LANES)
        pieces = jnp.concatenate(split3(hzr[c].reshape(halo, LANES)), axis=1)

        def rows_step(i, carry):
            rows = pl.ds(pl.multiple_of(i * TALL, TALL), TALL)
            value = dot(onehot[rows, :], pieces)
            value = value[:, 2 * LANES:] + value[:, LANES:2 * LANES] + value[:, :LANES]
            dz_out[rows, cols] = (dz1_ref[rows, cols] + value).astype(BF16)
            return carry

        lax.fori_loop(0, nodes // TALL, rows_step, 0)
        if c == 0:
            wait(hub_copies)
            dz1h = total_over(hubr, chips).astype(BF16)
            dhs[...] = dz1h
            back_copies = to(peers, 6, lambda p: dhs, dha.at[own])
            dha[own] = dz1h
            hx_mine = hx_ref[pl.ds(pl.multiple_of(own * home, 8), home), :].astype(BF16)
            dw1h = dot(hx_mine[:, :feat], dz1h, CONTRACT_ROWS)
        dw1s[c, pl.ds(0, feat), :] = dot(xt_ref[...], dz_out[:, cols]) + dw1h[:, c * LANES:(c + 1) * LANES]
        rs_copies[c] = to(peers, 13 + c, lambda p: dw1s.at[c, pl.ds(pl.multiple_of(p * 8, 8), 8)], dw1r.at[c, me])
        dw1r[c, me] = dw1s[c, pl.ds(pl.multiple_of(me * 8, 8), 8), :]
        if c == 0:
            wait(dw2_copies)
            total = total_over(dw2r, chips)
            dw2s[...] = total
            dw2_back = to(others, 7, lambda p: dw2s, dw2a.at[core, chip])
            dw2a[core, chip] = total
    for c in range(TILES - 1):
        spread(c)
    wait(dw2_back)
    dw2_pair = to([partner], 8, lambda p: dw2a.at[core], dw2a.at[core])
    wait(back_copies)
    hub_rows = dha[...].reshape(hubs, HID)
    for row in range(0, nodes, 2 * CHUNK):
        rows = pl.ds(row, 2 * CHUNK)
        owned = (iota((2 * CHUNK, hubs), 0) + (base + row) == hubrow).astype(BF16)
        dz = (dz_out[rows, :].astype(F32) + dot(owned, hub_rows)).astype(BF16)
        gxt_ref[:, rows] = dot(w1, dz, CONTRACT_COLS)
    flush(gxt_ref)
    wait(bias_copies)
    bias_out[...] = total_over(biasr, chips)
    flush(bias_out)
    spread(TILES - 1)
    wait(dw2_pair)
    flush(dw2a)
    for c in range(TILES):
        wait(ag_copies[c])


def outputs_kernel(gxt, dw2, bias, dw1, gxt_ref, gw1_ref, gw2_ref, gb1_ref, gb2_ref, flush):
    feat, out = gw1_ref.shape[0], gw2_ref.shape[1]
    gxt_ref[...] = gxt.get()[...]
    flush(gxt_ref)
    gw2_ref[...] = dw2.get()[...].T[:, :out]
    flush(gw2_ref)
    bias_ref, dw1_ref = bias.get(), dw1.get()
    for c in range(TILES):
        cols = pl.ds(c * LANES, LANES)
        for q in range(dw1_ref.shape[1]):
            rows = min(8, feat - q * 8)
            if rows > 0:
                gw1_ref[pl.ds(q * 8, rows), cols] = dw1_ref[c, q, pl.ds(0, rows), :]
        gb1_ref[:, cols] = bias_ref[pl.ds(c, 1), :]
    gb2_ref[...] = bias_ref[pl.ds(TILES, 1), pl.ds(0, out)]


def shape(dims, dtype):
    return jax.ShapeDtypeStruct(dims, dtype)


def solution(mesh):
    groups = mesh.shape["graph"]
    vertex_spec = P(("data", "graph"))
    vertex_rows = P(("data", "graph"), None)
    part_spec = P("data")
    part_rows = P("data", None)
    replicated = P()
    copies1, unroll1 = 3, 32
    copies2, unroll2 = 5, 32

    def params(collective_id=None):
        if collective_id is None:
            return pltpu.CompilerParams(vmem_limit_bytes=VMEM_LIMIT)
        return pltpu.CompilerParams(vmem_limit_bytes=VMEM_LIMIT, collective_id=collective_id, has_side_effects=True)

    def device_step(x_loc, dst_loc, src_loc, w_loc, send_loc, hub_ids, w_first, b_first, w_second, dy_out):
        nodes, feat = x_loc.shape
        edges = dst_loc.shape[0]
        halo = send_loc.shape[0]
        hubs = hub_ids.shape[0]
        out = dy_out.shape[1]
        block, home = halo // groups, hubs // groups
        src_rows, dst_rows = nodes + halo + 2 * hubs, nodes + 2 * hubs
        x_t = x_loc.T
        hub_lanes = hub_ids.reshape(1, hubs)
        send_lanes = send_loc.reshape(1, halo)
        bias = b_first.reshape(1, HID)
        sems = lambda n: [pltpu.SemaphoreType.DMA((n, groups)), pltpu.SemaphoreType.DMA((n, groups))]
        table = lambda a: a.reshape(edges // LANES, LANES)
        part_list = (edges // LANES // WAYS, LANES)
        packed = (block + hubs) // 2

        xh, hx, dhh, used, db2, wide, *lists = call(
            functools.partial(gather_kernel, groups),
            [(hub_ids, "smem"), (dy_out, "vmem"), (hub_lanes, "vmem"), (x_t, "vmem"), (send_loc, "smem"),
             (table(dst_loc), "vmem"), (table(src_loc), "vmem"), (table(w_loc), "vmem")],
            (shape((halo, LANES), BF16), shape((hubs, LANES), F32), shape((hubs, LANES), F32),
             shape((8, LANES), I32), shape((8, LANES), F32), shape((edges, LANES), F32))
            + (shape(part_list, I32),) * (2 * WAYS) + (shape(part_list, F32),) * WAYS,
            [pltpu.VMEM((nodes, LANES), F32), pltpu.VMEM((halo, LANES), F32), pltpu.VMEM((hubs, LANES), F32),
             pltpu.VMEM((hubs, LANES), F32), pltpu.VMEM((hubs, LANES), F32), pltpu.VMEM((hubs, LANES), F32),
             pltpu.VMEM((groups, packed, LANES), BF16), pltpu.VMEM((groups, packed, LANES), BF16),
             pltpu.VMEM((groups // 2, hubs, LANES), F32)] + sems(2),
            "gather_rows", params(0))
        lists = [(item.reshape(edges // WAYS), "smem") for item in lists]

        h1, dz, hz, hub = call(
            functools.partial(edges_forward_kernel, copies1, unroll1),
            [(w_first, "vmem"), (x_t, "vmem"), (dy_out, "vmem"), (xh, "vmem"), (hx, "vmem"), (dhh, "vmem"),
             (used, "smem"), (hub_ids, "smem"), (bias, "vmem")] + lists,
            (shape((nodes, HID), BF16), shape((nodes, LANES), F32), shape((halo, LANES), F32), shape((hubs, HID + LANES), F32)),
            [pltpu.VMEM((src_rows * TILES, LANES), F32), pltpu.VMEM((dst_rows * TILES, LANES), F32)]
            + [pltpu.VMEM((dst_rows * TILES, LANES), F32)] * copies1 + [pltpu.VMEM((src_rows * TILES, LANES), F32)] * copies1,
            "edges_forward", params())

        dz2, dyh, h1h, dz2h = call(
            functools.partial(middle_kernel, groups),
            [(hub.reshape(groups, home, HID + LANES), "vmem"), (hz.reshape(groups, block, LANES), "vmem"), (dz, "vmem"),
             (bias, "vmem"), (w_second, "vmem"), (send_lanes, "vmem")],
            (shape((nodes, LANES), BF16), shape((hubs, HID), F32), shape((home, HID), BF16), shape((home, LANES), BF16)),
            [pltpu.VMEM((groups, block, LANES), F32), pltpu.VMEM((groups, home, HID + LANES), F32),
             pltpu.VMEM((groups, home, HID), F32), pltpu.VMEM((home, HID), F32)] + sems(3),
            "middle", params(1))

        dz1, hz1, hub1, dw2, biases = call(
            functools.partial(edges_backward_kernel, copies2, unroll2, feat, groups),
            [(w_second, "vmem"), (h1, "vmem"), (dz2, "vmem"), (dyh, "vmem"), (h1h, "vmem"), (dz2h, "vmem"),
             (used, "smem"), (hub_ids, "smem"), (xh, "vmem"), (db2, "vmem"), (wide, "vmem")] + lists[:2 * WAYS],
            (shape((nodes, HID), F32), shape((TILES, halo, LANES), F32), shape((hubs, HID), F32), shape((LANES, HID), F32), shape((8, LANES), F32)),
            [pltpu.VMEM((dst_rows * TILES, LANES), F32)] + [pltpu.VMEM((src_rows * TILES, LANES), F32)] * copies2,
            "edges_backward", params())

        chips = groups // 2
        part = LANES // groups
        grad_xt, dw1, dw2, biases = call(
            functools.partial(last_kernel, groups),
            [(hub1.reshape(2, chips, home, HID), "vmem"), (hz1.reshape(TILES, groups, block, LANES), "hbm"),
             (dw2.reshape(2, chips, part, HID), "vmem"), (biases, "vmem"), (send_lanes, "vmem"), (x_t, "vmem"), (hx, "vmem"),
             (dz1, "vmem"), (w_first, "vmem"), (hub_lanes, "vmem")],
            (shape((feat, nodes), F32), shape((TILES, groups, 8, LANES), F32), shape((2, chips, part, HID), F32), shape((8, LANES), F32)),
            [pltpu.VMEM((nodes, HID), BF16), pltpu.VMEM((nodes, halo), BF16), pltpu.VMEM((TILES, groups, block, LANES), F32)]
            + [pltpu.VMEM((chips, home, HID), F32)] * 3 + [pltpu.VMEM((8, LANES), F32)] * 2 + [pltpu.VMEM((chips, 8, LANES), F32)]
            + [pltpu.VMEM((home, HID), BF16), pltpu.VMEM((groups, home, HID), BF16)]
            + [pltpu.VMEM((chips, part, HID), F32)] * 3 + [pltpu.VMEM((part, HID), F32)]
            + [pltpu.VMEM((TILES, groups * 8, LANES), F32), pltpu.VMEM((TILES, groups, 8, LANES), F32), pltpu.VMEM((TILES, 8, LANES), F32)] + sems(21),
            "last_exchange", params(2))

        grad_xt, grad_w1, grad_w2, grad_b1, grad_b2 = call(
            outputs_kernel,
            [(grad_xt, "vmem"), (dw2.reshape(LANES, HID), "vmem"), (biases, "vmem"), (dw1, "vmem")],
            (shape((feat, nodes), F32), shape((feat, HID), F32), shape((HID, out), F32), shape((1, HID), F32), shape((1, out), F32)),
            [], "outputs", params())
        return grad_xt.T, grad_w1, grad_w2, grad_b1.reshape(HID), grad_b2.reshape(out)

    return jax.shard_map(
        device_step,
        mesh=mesh,
        in_specs=(vertex_rows, vertex_spec, vertex_spec, vertex_spec, vertex_spec, part_spec, replicated, replicated, replicated, vertex_rows),
        out_specs=(vertex_rows, part_rows, part_rows, part_spec, part_spec),
        check_vma=False,
    )
```

```python
import functools

import jax
import jax.numpy as jnp
from jax import lax
from jax.experimental import pallas as pl
from jax.experimental.pallas import tpu as pltpu
from jax.sharding import PartitionSpec as P

F32, BF16, I32 = jnp.float32, jnp.bfloat16, jnp.int32
CONTRACT_ROWS = (((0,), (0,)), ((), ()))
CONTRACT_COLS = (((1,), (1,)), ((), ()))
LANES = 128
WAYS = 4
HID = 512
TILES = HID // LANES
CHUNK = 256
TALL = 1024
VMEM_LIMIT = 67043328
HBM = pl.BlockSpec(memory_space=pltpu.HBM)


class Fetched:
    def __init__(self, src, dst, sem):
        self.copy, self.ref, self.pending = pltpu.make_async_copy(src, dst, sem), dst, True
        self.copy.start()

    def get(self):
        if self.pending:
            self.copy.wait()
            self.pending = False
        return self.ref


def call(kernel, args, out_shape, scratch_shapes, name, compiler_params):
    spaces = {"vmem": pltpu.VMEM, "smem": pltpu.SMEM}
    moved = [n for n, (_, space) in enumerate(args) if space != "hbm"]
    in_buffers = [spaces[args[n][1]](args[n][0].shape, args[n][0].dtype) for n in moved]
    out_buffers = [pltpu.VMEM(out.shape, out.dtype) for out in out_shape]
    n_in, n_out = len(args), len(out_shape)

    def body(*refs):
        inputs, outputs = refs[:n_in], refs[n_in:n_in + n_out]
        bufs = refs[n_in + n_out:n_in + 2 * n_out + len(moved)]
        scratch, sems, out_sems = refs[n_in + 2 * n_out + len(moved):-2], refs[-2], refs[-1]
        fetched = list(inputs)
        for k, n in enumerate(moved):
            fetched[n] = Fetched(inputs[n], bufs[k], sems.at[k])
        results = bufs[len(moved):]
        stores = {}

        def flush(*buffers):
            for buffer in buffers:
                n = [k for k in range(n_out) if results[k] is buffer][0]
                stores[n] = pltpu.make_async_copy(results[n], outputs[n], out_sems.at[n])
                stores[n].start()

        kernel(*fetched, *results, *scratch, flush=flush)
        for n in moved:
            fetched[n].get()
        flush(*[results[n] for n in range(n_out) if n not in stores])
        for n in range(n_out):
            stores[n].wait()

    return pl.pallas_call(
        body,
        name=name,
        out_shape=out_shape,
        in_specs=[HBM] * n_in,
        out_specs=(HBM,) * n_out,
        scratch_shapes=in_buffers + out_buffers + list(scratch_shapes) + [pltpu.SemaphoreType.DMA((n_in,)), pltpu.SemaphoreType.DMA((n_out,))],
        compiler_params=compiler_params,
    )(*[array for array, _ in args])


def dot(a, b, dims=(((1,), (0,)), ((), ()))):
    return lax.dot_general(a, b, dims, preferred_element_type=F32)


def iota(shape, dim):
    return lax.broadcasted_iota(I32, shape, dim)


def split3(value):
    high = value.astype(BF16)
    rest = value - high.astype(F32)
    mid = rest.astype(BF16)
    low = (rest - mid.astype(F32)).astype(BF16)
    return high, mid, low


def select_rows(onehot, value, dims=(((1,), (0,)), ((), ()))):
    width = value.shape[1]
    picked = dot(onehot, jnp.concatenate(split3(value), axis=1), dims)
    return picked[:, 2 * width:] + picked[:, width:2 * width] + picked[:, :width]


def pad_lanes(value):
    rows, cols = value.shape
    if cols == LANES:
        return value
    return jnp.concatenate([value, jnp.zeros((rows, LANES - cols), value.dtype)], axis=1)


def hub_block(device, groups):
    return lax.rem(device, 2) * (groups // 2) + device // 2


def greet(groups, me):
    barrier = pltpu.get_barrier_semaphore()
    for step in range(1, groups):
        pl.semaphore_signal(barrier, inc=1, device_id={"graph": lax.rem(me + step, groups)}, device_id_type=pl.DeviceIdType.MESH)
    return barrier


def send(src, dst, send_sem, recv_sem, peer):
    copy = pltpu.make_async_remote_copy(
        src_ref=src, dst_ref=dst, send_sem=send_sem, recv_sem=recv_sem,
        device_id={"graph": peer}, device_id_type=pl.DeviceIdType.MESH)
    copy.start()
    return copy


def pack_rows(value):
    half = value.shape[0] // 2
    low = iota((half, LANES), 1) < LANES // 2
    return jnp.where(low, value[:half], pltpu.roll(value[half:], LANES // 2, 1)).astype(BF16)


def unpack_rows(value):
    return jnp.concatenate([value, pltpu.roll(value, LANES // 2, 1)], axis=0)


def gather_kernel(groups, hub_ids, dh, hubrow, xt, send_idx, dst, src, w,
                  xh_ref, hx_ref, dhh_ref, used_ref, db2_ref, *rest, flush):
    lists, (x32, xg, hxg, dhg, dhp, dhs, xs, xr, dhr, ssem, rsem) = rest[:3 * WAYS], rest[3 * WAYS:]
    me = lax.axis_index("graph")
    barrier = greet(groups, me)
    feat, nodes = xt.ref.shape
    hubs = hub_ids.ref.shape[0]
    halo = send_idx.ref.shape[0]
    block = halo // groups
    base = me * nodes
    chips = groups // 2
    core, chip = lax.rem(me, 2), me // 2
    dhg[...] = jnp.zeros_like(dhg)
    hub_ref, dh_ref = hub_ids.get(), dh.get()

    def hub_position_of(k):
        row = hub_ref[k] - base
        return jnp.logical_and(row >= 0, row < nodes), jnp.clip(row, 0, nodes - 1)

    def pick_grad(i, carry):
        for u in range(8):
            k = i * 8 + u
            own, row = hub_position_of(k)
            value = dh_ref[pl.ds(row, 1), :]
            dhg[pl.ds(k, 1), pl.ds(0, value.shape[1])] = jnp.where(own, value, 0.0)
        return carry

    lax.fori_loop(0, hubs // 8, pick_grad, 0)
    pl.semaphore_wait(barrier, groups - 1)
    pair = send(dhg, dhp, ssem.at[1, 0], rsem.at[1, 0], me + 1 - 2 * core)
    eye = (iota((feat, LANES), 0) == iota((feat, LANES), 1)).astype(BF16)
    tags = jnp.where(iota((hubs, LANES), 1) == feat, iota((hubs, LANES), 0) + 1, 0).astype(F32).astype(BF16)
    hubrow = hubrow.get()[...]
    xt_ref = xt.get()
    for row in range(0, nodes, CHUNK):
        owned = (iota((CHUNK, hubs), 0) + (base + row) == hubrow).astype(BF16)
        x32[pl.ds(row, CHUNK), :] = dot(xt_ref[:, pl.ds(row, CHUNK)], eye, CONTRACT_ROWS) + dot(owned, tags)
    send_ref = send_idx.get()

    def pick(i, carry):
        for u in range(16):
            j = i * 16 + u
            xg[pl.ds(j, 1), :] = x32[pl.ds(send_ref[j], 1), :]
        return carry

    lax.fori_loop(0, halo // 16, pick, 0)

    def pick_hub(i, carry):
        for u in range(8):
            k = i * 8 + u
            own, row = hub_position_of(k)
            hxg[pl.ds(k, 1), :] = jnp.where(own, x32[pl.ds(row, 1), :], 0.0)
        return carry

    lax.fori_loop(0, hubs // 8, pick_hub, 0)
    hub_rows = pack_rows(hxg[...])
    for q in range(groups):
        xs[q, pl.ds(0, block // 2), :] = pack_rows(xg[pl.ds(q * block, block), :])
        xs[q, pl.ds(block // 2, hubs // 2), :] = hub_rows
    copies = []
    for step in range(1, groups):
        peer = lax.rem(me + step, groups)
        copies.append(send(xs.at[peer], xr.at[me], ssem.at[0, step], rsem.at[0, step], peer))
    pair.wait()
    dhs[...] = dhg[...] + dhp[...]
    dhr[chip] = dhs[...]
    half = pl.ds(pl.multiple_of(core * (hubs // 2), 8), hubs // 2)
    for step in range(1, chips):
        for other in range(2):
            n = 2 * step + other
            peer = 2 * lax.rem(chip + step, chips) + lax.rem(core + other, 2)
            copies.append(send(dhs.at[half], dhr.at[chip, half], ssem.at[1, n], rsem.at[1, n], peer))
    dst_ref, src_ref, w_ref = dst.get(), src.get(), w.get()
    blocks = w_ref.shape[0]
    for q in range(WAYS):
        part = pl.ds(q, blocks // WAYS, stride=WAYS)
        lists[q][...] = dst_ref[part, :] * TILES
        lists[WAYS + q][...] = src_ref[part, :] * TILES
        lists[2 * WAYS + q][...] = w_ref[part, :]
    flush(*lists)
    place = (iota(w_ref.shape, 0) * LANES + iota(w_ref.shape, 1) + 1).astype(F32)
    used = jnp.where(w_ref[...] > 0.0, place, 0.0).max(axis=0, keepdims=True).max(axis=1, keepdims=True)
    used_ref[...] = jnp.broadcast_to(used, used_ref.shape).astype(I32)
    total = jnp.zeros((8, dh_ref.shape[1]), F32)
    for row in range(0, nodes, CHUNK):
        total = total + dh_ref[pl.ds(row, CHUNK), :].reshape(CHUNK // 8, 8, dh_ref.shape[1]).sum(axis=0)
    db2_ref[...] = jnp.broadcast_to(pad_lanes(total.sum(axis=0, keepdims=True)), db2_ref.shape)
    flush(used_ref, db2_ref)
    xr[me] = xs[me]
    for copy in copies:
        copy.wait()
    hx = jnp.zeros((hubs // 2, LANES), F32)
    dhh = jnp.zeros((hubs, LANES), F32)
    for q in range(groups):
        xh_ref[pl.ds(q * block, block), :] = unpack_rows(xr[q, pl.ds(0, block // 2), :].astype(F32)).astype(BF16)
        hx = hx + xr[q, pl.ds(block // 2, hubs // 2), :].astype(F32)
    for q in range(chips):
        dhh = dhh + dhr[q]
    hx_ref[...] = unpack_rows(hx)
    dhh_ref[...] = dhh


def hub_position(hub_ref, k, base, nodes, spare):
    row = hub_ref[k] - base
    own = jnp.logical_and(row >= 0, row < nodes)
    return pl.multiple_of(jnp.where(own, row, spare + k) * TILES, TILES)


def trips(used_ref, unroll):
    return (used_ref[0, 0] + (WAYS * LANES - 1)) // (WAYS * LANES) * (LANES // unroll)


def strided(first, rows):
    return pl.ds(first, rows, stride=TILES)


def total_of(refs, where):
    value = refs[0][where, :]
    for ref in refs[1:]:
        value = value + ref[where, :]
    return value


def edges_forward_kernel(copies, unroll, w1, xt, dh, xh, hx, dhh, used, hub_ids, b1, *rest, flush):
    lists, (h1_ref, dz_ref, hz_ref, hub_out, zt, dt), accs = rest[:3 * WAYS], rest[3 * WAYS:3 * WAYS + 6], rest[3 * WAYS + 6:]
    ya, da = accs[:copies], accs[copies:]
    me = lax.axis_index("graph")
    feat, nodes = xt.ref.shape
    halo, hubs = xh.ref.shape[0], hx.ref.shape[0]
    base = me * nodes
    for acc in ya:
        acc[...] = jnp.zeros_like(acc)
    for acc in da:
        acc[strided(0, nodes + halo + 2 * hubs), :] = jnp.zeros((nodes + halo + 2 * hubs, LANES), F32)
    w1 = w1.get()[...]
    xt_ref, dh_ref, xh_ref, hx_ref = xt.get(), dh.get(), xh.get(), hx.get()

    def put_rows(first, z):
        z = z.astype(BF16).astype(F32)
        for c in range(TILES):
            zt[strided(first * TILES + c, z.shape[0]), :] = z[:, c * LANES:(c + 1) * LANES]

    for row in range(0, nodes, CHUNK):
        put_rows(row, dot(xt_ref[:, pl.ds(row, CHUNK)], w1, CONTRACT_ROWS))
        dt[strided(row * TILES, CHUNK), :] = pad_lanes(dh_ref[pl.ds(row, CHUNK), :])
    for row in range(0, halo, CHUNK):
        put_rows(nodes + row, dot(xh_ref[pl.ds(row, CHUNK), pl.ds(0, feat)], w1))
    put_rows(nodes + halo, dot(hx_ref[:, pl.ds(0, feat)].astype(BF16), w1))
    dt[strided(nodes * TILES, hubs), :] = dhh.get()[...]
    used_ref, hub_ref, b1_ref = used.get(), hub_ids.get(), b1.get()
    lists = [item.get() for item in lists]

    def step(i, carry):
        for n in range(unroll * WAYS):
            q, u = n % WAYS, n % copies
            j = i * unroll + n // WAYS
            d4 = pl.multiple_of(lists[q][j], TILES)
            s4 = pl.multiple_of(lists[WAYS + q][j], TILES)
            w = lists[2 * WAYS + q][j]
            y_new = ya[u][pl.ds(d4, TILES), :] + w * zt[pl.ds(s4, TILES), :]
            z_new = da[u][pl.ds(s4, 1), :] + w * dt[pl.ds(d4, 1), :]
            ya[u][pl.ds(d4, TILES), :] = y_new
            da[u][pl.ds(s4, 1), :] = z_new
        return carry

    lax.fori_loop(0, trips(used_ref, unroll), step, 0)

    def fold(i, carry):
        new = []
        for u in range(8):
            k = i * 8 + u
            y_row = hub_position(hub_ref, k, base, nodes, nodes + hubs)
            z_row = hub_position(hub_ref, k, base, nodes, nodes + halo + hubs)
            y_hub = pl.ds(pl.multiple_of((nodes + k) * TILES, TILES), TILES)
            z_hub = pl.ds(pl.multiple_of((nodes + halo + k) * TILES, TILES), 1)
            new.append((y_hub, z_hub, z_row, ya[0][y_hub, :] + total_of(ya, pl.ds(y_row, TILES)), da[0][z_hub, :] + total_of(da, pl.ds(z_row, 1))))
        for y_hub, z_hub, z_row, y_new, z_new in new:
            ya[0][y_hub, :] = y_new
            da[0][z_hub, :] = z_new
            for acc in da:
                acc[pl.ds(z_row, 1), :] = jnp.zeros((1, LANES), F32)
        return carry

    lax.fori_loop(0, hubs // 8, fold, 0)
    for row in range(0, nodes, CHUNK):
        for c in range(TILES):
            cols = pl.ds(c * LANES, LANES)
            y = total_of(ya, strided(row * TILES + c, CHUNK)) + b1_ref[:, cols]
            h1_ref[pl.ds(row, CHUNK), cols] = jnp.maximum(y, 0.0).astype(BF16)
    flush(h1_ref)
    for row in range(0, nodes, CHUNK):
        dz_ref[pl.ds(row, CHUNK), :] = total_of(da, strided(row * TILES, CHUNK))
    flush(dz_ref)
    hz = total_of(da, strided(nodes * TILES, halo))
    tag = xh_ref[...].astype(F32)[:, feat:feat + 1]
    onehot = (tag == (iota((halo, hubs), 1) + 1).astype(F32)).astype(BF16)
    hub_z = total_of(da, strided((nodes + halo) * TILES, hubs)) + select_rows(onehot, hz, CONTRACT_ROWS)
    hz_ref[...] = jnp.where(tag > 0.0, 0.0, hz)
    for c in range(TILES):
        hub_out[:, pl.ds(c * LANES, LANES)] = total_of(ya, strided(nodes * TILES + c, hubs))
    hub_out[:, pl.ds(HID, LANES)] = hub_z


def middle_kernel(groups, hub, hz, dz, b1, w2, sendrow, w,
                  dz2_ref, dyh_ref, h1h_ref, dz2h_ref, wide_ref,
                  hzr, hubr, dyr, dys, ssem, rsem, flush):
    me = lax.axis_index("graph")
    barrier = greet(groups, me)
    nodes = dz.ref.shape[0]
    out = w2.ref.shape[1]
    home = hub.ref.shape[1]
    block = hz.ref.shape[1]
    halo = groups * block
    hub_ref, hz_ref = hub.get(), hz.get()
    own = hub_block(me, groups)
    hubr[me] = hub_ref[own]
    hzr[me] = jnp.zeros(hzr.shape[1:], F32)
    pl.semaphore_wait(barrier, groups - 1)
    hub_copies, halo_copies, back = [], [], []
    for step in range(1, groups):
        peer = lax.rem(me + step, groups)
        hub_copies.append(send(hub_ref.at[hub_block(peer, groups)], hubr.at[me], ssem.at[0, step], rsem.at[0, step], peer))
    for step in range(1, groups):
        peer = lax.rem(me + step, groups)
        halo_copies.append(send(hz_ref.at[peer], hzr.at[me], ssem.at[1, step], rsem.at[1, step], peer))
    w_ref = w.get()
    blocks = w_ref.shape[0]
    diagonal = iota((LANES, LANES), 0) == iota((LANES, LANES), 1)
    ones = jnp.ones((LANES, LANES), BF16)

    def widen(i, carry):
        for q in range(WAYS):
            row = w_ref[pl.ds(i * WAYS + q, 1), :]
            spread = jnp.zeros((LANES, LANES), F32)
            for piece in reversed(split3(row)):
                column = jnp.where(diagonal, jnp.broadcast_to(piece.astype(F32), (LANES, LANES)), 0.0).astype(BF16)
                spread = spread + dot(column, ones)
            wide_ref[pl.ds(pl.multiple_of((q * (blocks // WAYS) + i) * LANES, LANES), LANES), :] = spread
        return carry

    lax.fori_loop(0, blocks // WAYS, widen, 0)
    flush(wide_ref)
    for copy in hub_copies:
        copy.wait()
    total = hubr[0]
    for q in range(1, groups):
        total = total + hubr[q]
    b1_ref, w2_ref, sendrow = b1.get(), w2.get(), sendrow.get()[...]
    pre = total[:, :HID] + b1_ref[...]
    dz2h = total[:, HID:].astype(BF16)
    h1h_ref[...] = jnp.maximum(pre, 0.0).astype(BF16)
    dz2h_ref[...] = dz2h
    dys[...] = jnp.where(pre > 0, dot(dz2h[:, :out], w2_ref[...], CONTRACT_COLS), 0.0)
    for step in range(1, groups):
        peer = lax.rem(me + step, groups)
        back.append(send(dys, dyr.at[own], ssem.at[2, step], rsem.at[2, step], peer))
    dyr[own] = dys[...]
    for copy in halo_copies:
        copy.wait()
    pieces = split3(hzr[...].reshape(halo, LANES))
    dz_ref = dz.get()
    for row in range(0, nodes, CHUNK):
        onehot = (iota((CHUNK, halo), 0) + row == sendrow).astype(BF16)
        value = dz_ref[pl.ds(row, CHUNK), :]
        for piece in reversed(pieces):
            value = value + dot(onehot, piece)
        dz2_ref[pl.ds(row, CHUNK), :] = value.astype(BF16)
    for copy in back:
        copy.wait()
    for q in range(groups):
        dyh_ref[pl.ds(q * home, home), :] = dyr[q]


def edges_backward_kernel(copies, unroll, feat, groups, w2, h1, dz2, dyh, h1h, dz2h, used, hub_ids, xh, db2, wide, *rest, flush):
    lists, rest = rest[:2 * WAYS], rest[2 * WAYS:]
    (dz1_ref, hz_ref, hub_out, dw2_ref, bias_ref, yt), za = rest[:6], rest[6:]
    me = lax.axis_index("graph")
    nodes = h1.ref.shape[0]
    out = w2.ref.shape[1]
    halo, hubs = xh.ref.shape[0], dyh.ref.shape[0]
    home = h1h.ref.shape[0]
    base = me * nodes
    for acc in za:
        acc[...] = jnp.zeros_like(acc)
    w2, h1_ref, dz2_ref, dyh_ref, h1h_ref, dz2h_ref = w2.get()[...], h1.get(), dz2.get(), dyh.get(), h1h.get(), dz2h.get()
    mine = dyh_ref[pl.ds(pl.multiple_of(hub_block(me, groups) * home, 8), home), :]
    db1 = mine
    for row in range(0, nodes, CHUNK):
        rows = pl.ds(row, CHUNK)
        grad = dot(dz2_ref[rows, pl.ds(0, out)], w2, CONTRACT_COLS)
        grad = jnp.where(h1_ref[rows, :] > 0, grad, 0.0)
        db1 = db1 + grad.reshape(CHUNK // 8, 8, HID).sum(axis=0)
        for c in range(TILES):
            yt[strided(row * TILES + c, CHUNK), :] = grad[:, c * LANES:(c + 1) * LANES]
    db1 = db1.sum(axis=0, keepdims=True)
    bias_ref[...] = db2.get()[...]
    for c in range(TILES):
        bias_ref[pl.ds(c, 1), :] = db1[:, c * LANES:(c + 1) * LANES]
        yt[strided(nodes * TILES + c, hubs), :] = dyh_ref[:, pl.ds(c * LANES, LANES)]
    dw2_ref[...] = dot(dz2_ref[...], h1_ref[...], CONTRACT_ROWS) + dot(dz2h_ref[...], h1h_ref[...], CONTRACT_ROWS)
    flush(dw2_ref, bias_ref)
    used_ref, hub_ref, xh_ref, wide_ref = used.get(), hub_ids.get(), xh.get(), wide.get()
    lists = [item.get() for item in lists]
    length = wide_ref.shape[0] // WAYS

    def place(i, carry):
        new = []
        for u in range(8):
            k = i * 8 + u
            new.append((hub_position(hub_ref, k, base, nodes, nodes + hubs), yt[pl.ds(pl.multiple_of((nodes + k) * TILES, TILES), TILES), :]))
        for row, value in new:
            yt[pl.ds(row, TILES), :] = value
        return carry

    lax.fori_loop(0, hubs // 8, place, 0)

    def step(i, carry):
        for n in range(unroll * WAYS):
            q, u = n % WAYS, n % copies
            j = pl.multiple_of(i * unroll, unroll) + n // WAYS
            d4 = pl.multiple_of(lists[q][j], TILES)
            s4 = pl.multiple_of(lists[WAYS + q][j], TILES)
            w = wide_ref[pl.ds(q * length + j, 1), :]
            za[u][pl.ds(s4, TILES), :] = za[u][pl.ds(s4, TILES), :] + w * yt[pl.ds(d4, TILES), :]
        return carry

    lax.fori_loop(0, trips(used_ref, unroll), step, 0)

    def fold(i, carry):
        new = []
        for u in range(8):
            k = i * 8 + u
            row = hub_position(hub_ref, k, base, nodes, nodes + halo + hubs)
            here = pl.ds(pl.multiple_of((nodes + halo + k) * TILES, TILES), TILES)
            new.append((row, here, za[0][here, :] + total_of(za, pl.ds(row, TILES))))
        for row, here, value in new:
            za[0][here, :] = value
            for acc in za:
                acc[pl.ds(row, TILES), :] = jnp.zeros((TILES, LANES), F32)
        return carry

    lax.fori_loop(0, hubs // 8, fold, 0)
    for row in range(0, nodes, CHUNK):
        for c in range(TILES):
            dz1_ref[pl.ds(row, CHUNK), pl.ds(c * LANES, LANES)] = total_of(za, strided(row * TILES + c, CHUNK))
    flush(dz1_ref)
    tag = xh_ref[...].astype(F32)[:, feat:feat + 1]
    onehot = (tag == (iota((halo, hubs), 1) + 1).astype(F32)).astype(BF16)
    for c in range(TILES):
        cols = pl.ds(c * LANES, LANES)
        hz = total_of(za, strided(nodes * TILES + c, halo))
        hub_out[:, cols] = total_of(za, strided((nodes + halo) * TILES + c, hubs)) + select_rows(onehot, hz, CONTRACT_ROWS)
        hz_ref[c] = jnp.where(tag > 0.0, 0.0, hz)


def last_kernel(groups, hub, hz, dw2, bias, sendrow, xt, hx, dz1, w1, hubrow,
                gxt_ref, dw1a, dw2a, bias_out,
                dz_out, onehot, hzr, hubp, hubh, hubr, biasp, biash, biasr, dhs, dha, dw2p, dw2h, dw2r, dw2s, dw1s, dw1r, dw1t, ssem, rsem, flush):
    me = lax.axis_index("graph")
    barrier = greet(groups, me)
    feat, nodes = xt.ref.shape
    chips, home = hub.ref.shape[1:3]
    hubs = groups * home
    block = hz.shape[2]
    halo = groups * block
    base = me * nodes
    core, chip = lax.rem(me, 2), me // 2
    partner = me + 1 - 2 * core
    own = hub_block(me, groups)
    peers = [lax.rem(me + step, groups) for step in range(1, groups)]
    others = [lax.rem(me + 2 * step, groups) for step in range(1, chips)]
    pl.semaphore_wait(barrier, groups - 1)

    def to(devices, slot, src, dst):
        return [send(src(peer), dst, ssem.at[slot, i], rsem.at[slot, i], peer) for i, peer in enumerate(devices)]

    def wait(pending):
        for copy in pending:
            copy.wait()

    halo_copies = [to(peers, 9, lambda p: hz.at[0, p], hzr.at[0, me])]
    hub_ref, dw2_ref, bias_ref = hub.get(), dw2.get(), bias.get()
    pair_copies = (to([partner], 0, lambda p: hub_ref.at[1 - core], hubp) + to([partner], 1, lambda p: dw2_ref.at[1 - core], dw2p)
                   + to([partner], 2, lambda p: bias_ref, biasp))
    sendrow = sendrow.get()[...]
    for row in range(0, nodes, CHUNK):
        onehot[pl.ds(row, CHUNK), :] = (iota((CHUNK, halo), 0) + row == sendrow).astype(BF16)
    for c in range(TILES):
        hzr[c, me] = jnp.zeros((block, LANES), F32)
        dw1s[c] = jnp.zeros(dw1s.shape[1:], F32)
    wait(pair_copies)
    hubh[...] = hub_ref[core] + hubp[...]
    dw2h[...] = dw2_ref[core] + dw2p[...]
    biash[...] = bias_ref[...] + biasp[...]
    hubr[chip] = hubh[chip]
    dw2r[chip] = dw2h[chip]
    biasr[chip] = biash[...]
    hub_copies = to(others, 3, lambda p: hubh.at[p // 2], hubr.at[chip])
    dw2_copies = to(others, 4, lambda p: dw2h.at[p // 2], dw2r.at[chip])
    bias_copies = to(others, 5, lambda p: biash, biasr.at[chip])
    halo_copies += [to(peers, 9 + c, lambda p: hz.at[c, p], hzr.at[c, me]) for c in range(1, TILES)]

    def total_over(ref, count):
        total = ref[0]
        for q in range(1, count):
            total = total + ref[q]
        return total

    xt_ref, dz1_ref, hx_ref, w1, hubrow = xt.get(), dz1.get(), hx.get(), w1.get()[...], hubrow.get()[...]
    rs_copies, ag_copies = [None] * TILES, [None] * TILES

    def spread(c):
        wait(rs_copies[c])
        total = total_over(dw1r.at[c], groups)
        dw1t[c] = total
        ag_copies[c] = to(peers, 17 + c, lambda p: dw1t.at[c], dw1a.at[c, me])
        dw1a[c, me] = total

    for c in range(TILES):
        wait(halo_copies[c])
        cols = pl.ds(c * LANES, LANES)
        pieces = jnp.concatenate(split3(hzr[c].reshape(halo, LANES)), axis=1)

        def rows_step(i, carry):
            rows = pl.ds(pl.multiple_of(i * TALL, TALL), TALL)
            value = dot(onehot[rows, :], pieces)
            value = value[:, 2 * LANES:] + value[:, LANES:2 * LANES] + value[:, :LANES]
            dz_out[rows, cols] = (dz1_ref[rows, cols] + value).astype(BF16)
            return carry

        lax.fori_loop(0, nodes // TALL, rows_step, 0)
        if c == 0:
            wait(hub_copies)
            dz1h = total_over(hubr, chips).astype(BF16)
            dhs[...] = dz1h
            back_copies = to(peers, 6, lambda p: dhs, dha.at[own])
            dha[own] = dz1h
            hx_mine = hx_ref[pl.ds(pl.multiple_of(own * home, 8), home), :].astype(BF16)
            dw1h = dot(hx_mine[:, :feat], dz1h, CONTRACT_ROWS)
        dw1s[c, pl.ds(0, feat), :] = dot(xt_ref[...], dz_out[:, cols]) + dw1h[:, c * LANES:(c + 1) * LANES]
        rs_copies[c] = to(peers, 13 + c, lambda p: dw1s.at[c, pl.ds(pl.multiple_of(p * 8, 8), 8)], dw1r.at[c, me])
        dw1r[c, me] = dw1s[c, pl.ds(pl.multiple_of(me * 8, 8), 8), :]
        if c == 0:
            wait(dw2_copies)
            total = total_over(dw2r, chips)
            dw2s[...] = total
            dw2_back = to(others, 7, lambda p: dw2s, dw2a.at[core, chip])
            dw2a[core, chip] = total
    for c in range(TILES - 1):
        spread(c)
    wait(dw2_back)
    dw2_pair = to([partner], 8, lambda p: dw2a.at[core], dw2a.at[core])
    wait(back_copies)
    hub_rows = dha[...].reshape(hubs, HID)
    for row in range(0, nodes, 2 * CHUNK):
        rows = pl.ds(row, 2 * CHUNK)
        owned = (iota((2 * CHUNK, hubs), 0) + (base + row) == hubrow).astype(BF16)
        dz = (dz_out[rows, :].astype(F32) + dot(owned, hub_rows)).astype(BF16)
        gxt_ref[:, rows] = dot(w1, dz, CONTRACT_COLS)
    flush(gxt_ref)
    wait(bias_copies)
    bias_out[...] = total_over(biasr, chips)
    flush(bias_out)
    spread(TILES - 1)
    wait(dw2_pair)
    flush(dw2a)
    for c in range(TILES):
        wait(ag_copies[c])


def outputs_kernel(gxt, dw2, bias, dw1, gxt_ref, gw1_ref, gw2_ref, gb1_ref, gb2_ref, flush):
    feat, out = gw1_ref.shape[0], gw2_ref.shape[1]
    gxt_ref[...] = gxt.get()[...]
    flush(gxt_ref)
    gw2_ref[...] = dw2.get()[...].T[:, :out]
    flush(gw2_ref)
    bias_ref, dw1_ref = bias.get(), dw1.get()
    for c in range(TILES):
        cols = pl.ds(c * LANES, LANES)
        for q in range(dw1_ref.shape[1]):
            rows = min(8, feat - q * 8)
            if rows > 0:
                gw1_ref[pl.ds(q * 8, rows), cols] = dw1_ref[c, q, pl.ds(0, rows), :]
        gb1_ref[:, cols] = bias_ref[pl.ds(c, 1), :]
    gb2_ref[...] = bias_ref[pl.ds(TILES, 1), pl.ds(0, out)]


def shape(dims, dtype):
    return jax.ShapeDtypeStruct(dims, dtype)


def solution(mesh):
    groups = mesh.shape["graph"]
    vertex_spec = P(("data", "graph"))
    vertex_rows = P(("data", "graph"), None)
    part_spec = P("data")
    part_rows = P("data", None)
    replicated = P()
    copies1, unroll1 = 3, 32
    copies2, unroll2 = 5, 32

    def params(collective_id=None):
        if collective_id is None:
            return pltpu.CompilerParams(vmem_limit_bytes=VMEM_LIMIT)
        return pltpu.CompilerParams(vmem_limit_bytes=VMEM_LIMIT, collective_id=collective_id, has_side_effects=True)

    def device_step(x_loc, dst_loc, src_loc, w_loc, send_loc, hub_ids, w_first, b_first, w_second, dy_out):
        nodes, feat = x_loc.shape
        edges = dst_loc.shape[0]
        halo = send_loc.shape[0]
        hubs = hub_ids.shape[0]
        out = dy_out.shape[1]
        block, home = halo // groups, hubs // groups
        src_rows, dst_rows = nodes + halo + 2 * hubs, nodes + 2 * hubs
        x_t = x_loc.T
        hub_lanes = hub_ids.reshape(1, hubs)
        send_lanes = send_loc.reshape(1, halo)
        bias = b_first.reshape(1, HID)
        sems = lambda n: [pltpu.SemaphoreType.DMA((n, groups)), pltpu.SemaphoreType.DMA((n, groups))]
        table = lambda a: a.reshape(edges // LANES, LANES)
        part_list = (edges // LANES // WAYS, LANES)
        packed = (block + hubs) // 2

        xh, hx, dhh, used, db2, *lists = call(
            functools.partial(gather_kernel, groups),
            [(hub_ids, "smem"), (dy_out, "vmem"), (hub_lanes, "vmem"), (x_t, "vmem"), (send_loc, "smem"),
             (table(dst_loc), "vmem"), (table(src_loc), "vmem"), (table(w_loc), "vmem")],
            (shape((halo, LANES), BF16), shape((hubs, LANES), F32), shape((hubs, LANES), F32),
             shape((8, LANES), I32), shape((8, LANES), F32))
            + (shape(part_list, I32),) * (2 * WAYS) + (shape(part_list, F32),) * WAYS,
            [pltpu.VMEM((nodes, LANES), F32), pltpu.VMEM((halo, LANES), F32), pltpu.VMEM((hubs, LANES), F32),
             pltpu.VMEM((hubs, LANES), F32), pltpu.VMEM((hubs, LANES), F32), pltpu.VMEM((hubs, LANES), F32),
             pltpu.VMEM((groups, packed, LANES), BF16), pltpu.VMEM((groups, packed, LANES), BF16),
             pltpu.VMEM((groups // 2, hubs, LANES), F32)] + sems(2),
            "gather_rows", params(0))
        lists = [(item.reshape(edges // WAYS), "smem") for item in lists]

        h1, dz, hz, hub = call(
            functools.partial(edges_forward_kernel, copies1, unroll1),
            [(w_first, "vmem"), (x_t, "vmem"), (dy_out, "vmem"), (xh, "vmem"), (hx, "vmem"), (dhh, "vmem"),
             (used, "smem"), (hub_ids, "smem"), (bias, "vmem")] + lists,
            (shape((nodes, HID), BF16), shape((nodes, LANES), F32), shape((halo, LANES), F32), shape((hubs, HID + LANES), F32)),
            [pltpu.VMEM((src_rows * TILES, LANES), F32), pltpu.VMEM((dst_rows * TILES, LANES), F32)]
            + [pltpu.VMEM((dst_rows * TILES, LANES), F32)] * copies1 + [pltpu.VMEM((src_rows * TILES, LANES), F32)] * copies1,
            "edges_forward", params())

        dz2, dyh, h1h, dz2h, wide = call(
            functools.partial(middle_kernel, groups),
            [(hub.reshape(groups, home, HID + LANES), "vmem"), (hz.reshape(groups, block, LANES), "vmem"), (dz, "vmem"),
             (bias, "vmem"), (w_second, "vmem"), (send_lanes, "vmem"), (table(w_loc), "vmem")],
            (shape((nodes, LANES), BF16), shape((hubs, HID), F32), shape((home, HID), BF16), shape((home, LANES), BF16), shape((edges, LANES), F32)),
            [pltpu.VMEM((groups, block, LANES), F32), pltpu.VMEM((groups, home, HID + LANES), F32),
             pltpu.VMEM((groups, home, HID), F32), pltpu.VMEM((home, HID), F32)] + sems(3),
            "middle", params(1))

        dz1, hz1, hub1, dw2, biases = call(
            functools.partial(edges_backward_kernel, copies2, unroll2, feat, groups),
            [(w_second, "vmem"), (h1, "vmem"), (dz2, "vmem"), (dyh, "vmem"), (h1h, "vmem"), (dz2h, "vmem"),
             (used, "smem"), (hub_ids, "smem"), (xh, "vmem"), (db2, "vmem"), (wide, "vmem")] + lists[:2 * WAYS],
            (shape((nodes, HID), F32), shape((TILES, halo, LANES), F32), shape((hubs, HID), F32), shape((LANES, HID), F32), shape((8, LANES), F32)),
            [pltpu.VMEM((dst_rows * TILES, LANES), F32)] + [pltpu.VMEM((src_rows * TILES, LANES), F32)] * copies2,
            "edges_backward", params())

        chips = groups // 2
        part = LANES // groups
        grad_xt, dw1, dw2, biases = call(
            functools.partial(last_kernel, groups),
            [(hub1.reshape(2, chips, home, HID), "vmem"), (hz1.reshape(TILES, groups, block, LANES), "hbm"),
             (dw2.reshape(2, chips, part, HID), "vmem"), (biases, "vmem"), (send_lanes, "vmem"), (x_t, "vmem"), (hx, "vmem"),
             (dz1, "vmem"), (w_first, "vmem"), (hub_lanes, "vmem")],
            (shape((feat, nodes), F32), shape((TILES, groups, 8, LANES), F32), shape((2, chips, part, HID), F32), shape((8, LANES), F32)),
            [pltpu.VMEM((nodes, HID), BF16), pltpu.VMEM((nodes, halo), BF16), pltpu.VMEM((TILES, groups, block, LANES), F32)]
            + [pltpu.VMEM((chips, home, HID), F32)] * 3 + [pltpu.VMEM((8, LANES), F32)] * 2 + [pltpu.VMEM((chips, 8, LANES), F32)]
            + [pltpu.VMEM((home, HID), BF16), pltpu.VMEM((groups, home, HID), BF16)]
            + [pltpu.VMEM((chips, part, HID), F32)] * 3 + [pltpu.VMEM((part, HID), F32)]
            + [pltpu.VMEM((TILES, groups * 8, LANES), F32), pltpu.VMEM((TILES, groups, 8, LANES), F32), pltpu.VMEM((TILES, 8, LANES), F32)] + sems(21),
            "last_exchange", params(2))

        grad_xt, grad_w1, grad_w2, grad_b1, grad_b2 = call(
            outputs_kernel,
            [(grad_xt, "vmem"), (dw2.reshape(LANES, HID), "vmem"), (biases, "vmem"), (dw1, "vmem")],
            (shape((feat, nodes), F32), shape((feat, HID), F32), shape((HID, out), F32), shape((1, HID), F32), shape((1, out), F32)),
            [], "outputs", params())
        return grad_xt.T, grad_w1, grad_w2, grad_b1.reshape(HID), grad_b2.reshape(out)

    return jax.shard_map(
        device_step,
        mesh=mesh,
        in_specs=(vertex_rows, vertex_spec, vertex_spec, vertex_spec, vertex_spec, part_spec, replicated, replicated, replicated, vertex_rows),
        out_specs=(vertex_rows, part_rows, part_rows, part_spec, part_spec),
        check_vma=False,
    )
```

```python
import functools

import jax
import jax.numpy as jnp
from jax import lax
from jax.experimental import pallas as pl
from jax.experimental.pallas import tpu as pltpu
from jax.sharding import PartitionSpec as P

F32, BF16, I32 = jnp.float32, jnp.bfloat16, jnp.int32
CONTRACT_ROWS = (((0,), (0,)), ((), ()))
CONTRACT_COLS = (((1,), (1,)), ((), ()))
LANES = 128
WAYS = 4
HID = 512
TILES = HID // LANES
CHUNK = 256
TALL = 2048
VMEM_LIMIT = 67043328
HBM = pl.BlockSpec(memory_space=pltpu.HBM)


class Fetched:
    def __init__(self, src, dst, sem):
        self.copy, self.ref, self.pending = pltpu.make_async_copy(src, dst, sem), dst, True
        self.copy.start()

    def get(self):
        if self.pending:
            self.copy.wait()
            self.pending = False
        return self.ref


def call(kernel, args, out_shape, scratch_shapes, name, compiler_params):
    spaces = {"vmem": pltpu.VMEM, "smem": pltpu.SMEM}
    moved = [n for n, (_, space) in enumerate(args) if space != "hbm"]
    in_buffers = [spaces[args[n][1]](args[n][0].shape, args[n][0].dtype) for n in moved]
    out_buffers = [pltpu.VMEM(out.shape, out.dtype) for out in out_shape]
    n_in, n_out = len(args), len(out_shape)

    def body(*refs):
        inputs, outputs = refs[:n_in], refs[n_in:n_in + n_out]
        bufs = refs[n_in + n_out:n_in + 2 * n_out + len(moved)]
        scratch, sems, out_sems = refs[n_in + 2 * n_out + len(moved):-2], refs[-2], refs[-1]
        fetched = list(inputs)
        for k, n in enumerate(moved):
            fetched[n] = Fetched(inputs[n], bufs[k], sems.at[k])
        results = bufs[len(moved):]
        stores = {}

        def flush(*buffers):
            for buffer in buffers:
                n = [k for k in range(n_out) if results[k] is buffer][0]
                stores[n] = pltpu.make_async_copy(results[n], outputs[n], out_sems.at[n])
                stores[n].start()

        kernel(*fetched, *results, *scratch, flush=flush)
        for n in moved:
            fetched[n].get()
        flush(*[results[n] for n in range(n_out) if n not in stores])
        for n in range(n_out):
            stores[n].wait()

    return pl.pallas_call(
        body,
        name=name,
        out_shape=out_shape,
        in_specs=[HBM] * n_in,
        out_specs=(HBM,) * n_out,
        scratch_shapes=in_buffers + out_buffers + list(scratch_shapes) + [pltpu.SemaphoreType.DMA((n_in,)), pltpu.SemaphoreType.DMA((n_out,))],
        compiler_params=compiler_params,
    )(*[array for array, _ in args])


def dot(a, b, dims=(((1,), (0,)), ((), ()))):
    return lax.dot_general(a, b, dims, preferred_element_type=F32)


def iota(shape, dim):
    return lax.broadcasted_iota(I32, shape, dim)


def split3(value):
    high = value.astype(BF16)
    rest = value - high.astype(F32)
    mid = rest.astype(BF16)
    low = (rest - mid.astype(F32)).astype(BF16)
    return high, mid, low


def select_rows(onehot, value, dims=(((1,), (0,)), ((), ()))):
    width = value.shape[1]
    picked = dot(onehot, jnp.concatenate(split3(value), axis=1), dims)
    return picked[:, 2 * width:] + picked[:, width:2 * width] + picked[:, :width]


def pad_lanes(value):
    rows, cols = value.shape
    if cols == LANES:
        return value
    return jnp.concatenate([value, jnp.zeros((rows, LANES - cols), value.dtype)], axis=1)


def hub_block(device, groups):
    return lax.rem(device, 2) * (groups // 2) + device // 2


def greet(groups, me):
    barrier = pltpu.get_barrier_semaphore()
    for step in range(1, groups):
        pl.semaphore_signal(barrier, inc=1, device_id={"graph": lax.rem(me + step, groups)}, device_id_type=pl.DeviceIdType.MESH)
    return barrier


def send(src, dst, send_sem, recv_sem, peer):
    copy = pltpu.make_async_remote_copy(
        src_ref=src, dst_ref=dst, send_sem=send_sem, recv_sem=recv_sem,
        device_id={"graph": peer}, device_id_type=pl.DeviceIdType.MESH)
    copy.start()
    return copy


def pack_rows(value):
    half = value.shape[0] // 2
    low = iota((half, LANES), 1) < LANES // 2
    return jnp.where(low, value[:half], pltpu.roll(value[half:], LANES // 2, 1)).astype(BF16)


def unpack_rows(value):
    return jnp.concatenate([value, pltpu.roll(value, LANES // 2, 1)], axis=0)


def gather_kernel(groups, hub_ids, dh, hubrow, xt, send_idx, dst, src, w,
                  xh_ref, hx_ref, dhh_ref, used_ref, db2_ref, *rest, flush):
    lists, (x32, xg, hxg, dhg, dhp, dhs, xs, xr, dhr, ssem, rsem) = rest[:3 * WAYS], rest[3 * WAYS:]
    me = lax.axis_index("graph")
    barrier = greet(groups, me)
    feat, nodes = xt.ref.shape
    hubs = hub_ids.ref.shape[0]
    halo = send_idx.ref.shape[0]
    block = halo // groups
    base = me * nodes
    chips = groups // 2
    core, chip = lax.rem(me, 2), me // 2
    dhg[...] = jnp.zeros_like(dhg)
    hub_ref, dh_ref = hub_ids.get(), dh.get()

    def hub_position_of(k):
        row = hub_ref[k] - base
        return jnp.logical_and(row >= 0, row < nodes), jnp.clip(row, 0, nodes - 1)

    def pick_grad(i, carry):
        for u in range(8):
            k = i * 8 + u
            own, row = hub_position_of(k)
            value = dh_ref[pl.ds(row, 1), :]
            dhg[pl.ds(k, 1), pl.ds(0, value.shape[1])] = jnp.where(own, value, 0.0)
        return carry

    lax.fori_loop(0, hubs // 8, pick_grad, 0)
    pl.semaphore_wait(barrier, groups - 1)
    pair = send(dhg, dhp, ssem.at[1, 0], rsem.at[1, 0], me + 1 - 2 * core)
    eye = (iota((feat, LANES), 0) == iota((feat, LANES), 1)).astype(BF16)
    tags = jnp.where(iota((hubs, LANES), 1) == feat, iota((hubs, LANES), 0) + 1, 0).astype(F32).astype(BF16)
    hubrow = hubrow.get()[...]
    xt_ref = xt.get()
    for row in range(0, nodes, CHUNK):
        owned = (iota((CHUNK, hubs), 0) + (base + row) == hubrow).astype(BF16)
        x32[pl.ds(row, CHUNK), :] = dot(xt_ref[:, pl.ds(row, CHUNK)], eye, CONTRACT_ROWS) + dot(owned, tags)
    send_ref = send_idx.get()

    def pick(i, carry):
        for u in range(16):
            j = i * 16 + u
            xg[pl.ds(j, 1), :] = x32[pl.ds(send_ref[j], 1), :]
        return carry

    lax.fori_loop(0, halo // 16, pick, 0)

    def pick_hub(i, carry):
        for u in range(8):
            k = i * 8 + u
            own, row = hub_position_of(k)
            hxg[pl.ds(k, 1), :] = jnp.where(own, x32[pl.ds(row, 1), :], 0.0)
        return carry

    lax.fori_loop(0, hubs // 8, pick_hub, 0)
    hub_rows = pack_rows(hxg[...])
    for q in range(groups):
        xs[q, pl.ds(0, block // 2), :] = pack_rows(xg[pl.ds(q * block, block), :])
        xs[q, pl.ds(block // 2, hubs // 2), :] = hub_rows
    copies = []
    for step in range(1, groups):
        peer = lax.rem(me + step, groups)
        copies.append(send(xs.at[peer], xr.at[me], ssem.at[0, step], rsem.at[0, step], peer))
    pair.wait()
    dhs[...] = dhg[...] + dhp[...]
    dhr[chip] = dhs[...]
    half = pl.ds(pl.multiple_of(core * (hubs // 2), 8), hubs // 2)
    for step in range(1, chips):
        for other in range(2):
            n = 2 * step + other
            peer = 2 * lax.rem(chip + step, chips) + lax.rem(core + other, 2)
            copies.append(send(dhs.at[half], dhr.at[chip, half], ssem.at[1, n], rsem.at[1, n], peer))
    dst_ref, src_ref, w_ref = dst.get(), src.get(), w.get()
    blocks = w_ref.shape[0]
    for q in range(WAYS):
        part = pl.ds(q, blocks // WAYS, stride=WAYS)
        lists[q][...] = dst_ref[part, :] * TILES
        lists[WAYS + q][...] = src_ref[part, :] * TILES
        lists[2 * WAYS + q][...] = w_ref[part, :]
    flush(*lists)
    place = (iota(w_ref.shape, 0) * LANES + iota(w_ref.shape, 1) + 1).astype(F32)
    used = jnp.where(w_ref[...] > 0.0, place, 0.0).max(axis=0, keepdims=True).max(axis=1, keepdims=True)
    used_ref[...] = jnp.broadcast_to(used, used_ref.shape).astype(I32)
    total = jnp.zeros((8, dh_ref.shape[1]), F32)
    for row in range(0, nodes, CHUNK):
        total = total + dh_ref[pl.ds(row, CHUNK), :].reshape(CHUNK // 8, 8, dh_ref.shape[1]).sum(axis=0)
    db2_ref[...] = jnp.broadcast_to(pad_lanes(total.sum(axis=0, keepdims=True)), db2_ref.shape)
    flush(used_ref, db2_ref)
    xr[me] = xs[me]
    for copy in copies:
        copy.wait()
    hx = jnp.zeros((hubs // 2, LANES), F32)
    dhh = jnp.zeros((hubs, LANES), F32)
    for q in range(groups):
        xh_ref[pl.ds(q * block, block), :] = unpack_rows(xr[q, pl.ds(0, block // 2), :].astype(F32)).astype(BF16)
        hx = hx + xr[q, pl.ds(block // 2, hubs // 2), :].astype(F32)
    for q in range(chips):
        dhh = dhh + dhr[q]
    hx_ref[...] = unpack_rows(hx)
    dhh_ref[...] = dhh


def hub_position(hub_ref, k, base, nodes, spare):
    row = hub_ref[k] - base
    own = jnp.logical_and(row >= 0, row < nodes)
    return pl.multiple_of(jnp.where(own, row, spare + k) * TILES, TILES)


def trips(used_ref, unroll):
    return (used_ref[0, 0] + (WAYS * LANES - 1)) // (WAYS * LANES) * (LANES // unroll)


def strided(first, rows):
    return pl.ds(first, rows, stride=TILES)


def total_of(refs, where):
    value = refs[0][where, :]
    for ref in refs[1:]:
        value = value + ref[where, :]
    return value


def edges_forward_kernel(copies, unroll, w1, xt, dh, xh, hx, dhh, used, hub_ids, b1, *rest, flush):
    lists, (h1_ref, dz_ref, hz_ref, hub_out, zt, dt), accs = rest[:3 * WAYS], rest[3 * WAYS:3 * WAYS + 6], rest[3 * WAYS + 6:]
    ya, da = accs[:copies], accs[copies:]
    me = lax.axis_index("graph")
    feat, nodes = xt.ref.shape
    halo, hubs = xh.ref.shape[0], hx.ref.shape[0]
    base = me * nodes
    for acc in ya:
        acc[...] = jnp.zeros_like(acc)
    for acc in da:
        acc[strided(0, nodes + halo + 2 * hubs), :] = jnp.zeros((nodes + halo + 2 * hubs, LANES), F32)
    w1 = w1.get()[...]
    xt_ref, dh_ref, xh_ref, hx_ref = xt.get(), dh.get(), xh.get(), hx.get()

    def put_rows(first, z):
        z = z.astype(BF16).astype(F32)
        for c in range(TILES):
            zt[strided(first * TILES + c, z.shape[0]), :] = z[:, c * LANES:(c + 1) * LANES]

    for row in range(0, nodes, CHUNK):
        put_rows(row, dot(xt_ref[:, pl.ds(row, CHUNK)], w1, CONTRACT_ROWS))
        dt[strided(row * TILES, CHUNK), :] = pad_lanes(dh_ref[pl.ds(row, CHUNK), :])
    for row in range(0, halo, CHUNK):
        put_rows(nodes + row, dot(xh_ref[pl.ds(row, CHUNK), pl.ds(0, feat)], w1))
    put_rows(nodes + halo, dot(hx_ref[:, pl.ds(0, feat)].astype(BF16), w1))
    dt[strided(nodes * TILES, hubs), :] = dhh.get()[...]
    used_ref, hub_ref, b1_ref = used.get(), hub_ids.get(), b1.get()
    lists = [item.get() for item in lists]

    def step(i, carry):
        for n in range(unroll * WAYS):
            q, u = n % WAYS, n % copies
            j = i * unroll + n // WAYS
            d4 = pl.multiple_of(lists[q][j], TILES)
            s4 = pl.multiple_of(lists[WAYS + q][j], TILES)
            w = lists[2 * WAYS + q][j]
            y_new = ya[u][pl.ds(d4, TILES), :] + w * zt[pl.ds(s4, TILES), :]
            z_new = da[u][pl.ds(s4, 1), :] + w * dt[pl.ds(d4, 1), :]
            ya[u][pl.ds(d4, TILES), :] = y_new
            da[u][pl.ds(s4, 1), :] = z_new
        return carry

    lax.fori_loop(0, trips(used_ref, unroll), step, 0)

    def fold(i, carry):
        new = []
        for u in range(8):
            k = i * 8 + u
            y_row = hub_position(hub_ref, k, base, nodes, nodes + hubs)
            z_row = hub_position(hub_ref, k, base, nodes, nodes + halo + hubs)
            y_hub = pl.ds(pl.multiple_of((nodes + k) * TILES, TILES), TILES)
            z_hub = pl.ds(pl.multiple_of((nodes + halo + k) * TILES, TILES), 1)
            new.append((y_hub, z_hub, z_row, ya[0][y_hub, :] + total_of(ya, pl.ds(y_row, TILES)), da[0][z_hub, :] + total_of(da, pl.ds(z_row, 1))))
        for y_hub, z_hub, z_row, y_new, z_new in new:
            ya[0][y_hub, :] = y_new
            da[0][z_hub, :] = z_new
            for acc in da:
                acc[pl.ds(z_row, 1), :] = jnp.zeros((1, LANES), F32)
        return carry

    lax.fori_loop(0, hubs // 8, fold, 0)
    for row in range(0, nodes, CHUNK):
        for c in range(TILES):
            cols = pl.ds(c * LANES, LANES)
            y = total_of(ya, strided(row * TILES + c, CHUNK)) + b1_ref[:, cols]
            h1_ref[pl.ds(row, CHUNK), cols] = jnp.maximum(y, 0.0).astype(BF16)
    flush(h1_ref)
    for row in range(0, nodes, CHUNK):
        dz_ref[pl.ds(row, CHUNK), :] = total_of(da, strided(row * TILES, CHUNK))
    flush(dz_ref)
    hz = total_of(da, strided(nodes * TILES, halo))
    tag = xh_ref[...].astype(F32)[:, feat:feat + 1]
    onehot = (tag == (iota((halo, hubs), 1) + 1).astype(F32)).astype(BF16)
    hub_z = total_of(da, strided((nodes + halo) * TILES, hubs)) + select_rows(onehot, hz, CONTRACT_ROWS)
    hz_ref[...] = jnp.where(tag > 0.0, 0.0, hz)
    for c in range(TILES):
        hub_out[:, pl.ds(c * LANES, LANES)] = total_of(ya, strided(nodes * TILES + c, hubs))
    hub_out[:, pl.ds(HID, LANES)] = hub_z


def middle_kernel(groups, hub, hz, dz, b1, w2, sendrow, w,
                  dz2_ref, dyh_ref, h1h_ref, dz2h_ref, wide_ref,
                  hzr, hubr, dyr, dys, ssem, rsem, flush):
    me = lax.axis_index("graph")
    barrier = greet(groups, me)
    nodes = dz.ref.shape[0]
    out = w2.ref.shape[1]
    home = hub.ref.shape[1]
    block = hz.ref.shape[1]
    halo = groups * block
    hub_ref, hz_ref = hub.get(), hz.get()
    own = hub_block(me, groups)
    hubr[me] = hub_ref[own]
    hzr[me] = jnp.zeros(hzr.shape[1:], F32)
    pl.semaphore_wait(barrier, groups - 1)
    hub_copies, halo_copies, back = [], [], []
    for step in range(1, groups):
        peer = lax.rem(me + step, groups)
        hub_copies.append(send(hub_ref.at[hub_block(peer, groups)], hubr.at[me], ssem.at[0, step], rsem.at[0, step], peer))
    for step in range(1, groups):
        peer = lax.rem(me + step, groups)
        halo_copies.append(send(hz_ref.at[peer], hzr.at[me], ssem.at[1, step], rsem.at[1, step], peer))
    w_ref = w.get()
    blocks = w_ref.shape[0]
    diagonal = iota((LANES, LANES), 0) == iota((LANES, LANES), 1)
    ones = jnp.ones((LANES, LANES), BF16)

    def widen(i, carry):
        for q in range(WAYS):
            row = w_ref[pl.ds(i * WAYS + q, 1), :]
            spread = jnp.zeros((LANES, LANES), F32)
            for piece in reversed(split3(row)):
                column = jnp.where(diagonal, jnp.broadcast_to(piece.astype(F32), (LANES, LANES)), 0.0).astype(BF16)
                spread = spread + dot(column, ones)
            wide_ref[pl.ds(pl.multiple_of((q * (blocks // WAYS) + i) * LANES, LANES), LANES), :] = spread
        return carry

    lax.fori_loop(0, blocks // WAYS, widen, 0)
    flush(wide_ref)
    for copy in hub_copies:
        copy.wait()
    total = hubr[0]
    for q in range(1, groups):
        total = total + hubr[q]
    b1_ref, w2_ref, sendrow = b1.get(), w2.get(), sendrow.get()[...]
    pre = total[:, :HID] + b1_ref[...]
    dz2h = total[:, HID:].astype(BF16)
    h1h_ref[...] = jnp.maximum(pre, 0.0).astype(BF16)
    dz2h_ref[...] = dz2h
    dys[...] = jnp.where(pre > 0, dot(dz2h[:, :out], w2_ref[...], CONTRACT_COLS), 0.0)
    for step in range(1, groups):
        peer = lax.rem(me + step, groups)
        back.append(send(dys, dyr.at[own], ssem.at[2, step], rsem.at[2, step], peer))
    dyr[own] = dys[...]
    for copy in halo_copies:
        copy.wait()
    pieces = jnp.concatenate(split3(hzr[...].reshape(halo, LANES)), axis=1)
    dz_ref = dz.get()
    for row in range(0, nodes, CHUNK):
        onehot = (iota((CHUNK, halo), 0) + row == sendrow).astype(BF16)
        value = dot(onehot, pieces)
        value = value[:, 2 * LANES:] + value[:, LANES:2 * LANES] + value[:, :LANES]
        dz2_ref[pl.ds(row, CHUNK), :] = (dz_ref[pl.ds(row, CHUNK), :] + value).astype(BF16)
    for copy in back:
        copy.wait()
    for q in range(groups):
        dyh_ref[pl.ds(q * home, home), :] = dyr[q]


def edges_backward_kernel(copies, unroll, feat, groups, w2, h1, dz2, dyh, h1h, dz2h, used, hub_ids, xh, db2, wide, *rest, flush):
    lists, rest = rest[:2 * WAYS], rest[2 * WAYS:]
    (dz1_ref, hz_ref, hub_out, dw2_ref, bias_ref, yt), za = rest[:6], rest[6:]
    me = lax.axis_index("graph")
    nodes = h1.ref.shape[0]
    out = w2.ref.shape[1]
    halo, hubs = xh.ref.shape[0], dyh.ref.shape[0]
    home = h1h.ref.shape[0]
    base = me * nodes
    for acc in za:
        acc[...] = jnp.zeros_like(acc)
    w2, h1_ref, dz2_ref, dyh_ref, h1h_ref, dz2h_ref = w2.get()[...], h1.get(), dz2.get(), dyh.get(), h1h.get(), dz2h.get()
    mine = dyh_ref[pl.ds(pl.multiple_of(hub_block(me, groups) * home, 8), home), :]
    db1 = mine
    for row in range(0, nodes, CHUNK):
        rows = pl.ds(row, CHUNK)
        grad = dot(dz2_ref[rows, pl.ds(0, out)], w2, CONTRACT_COLS)
        grad = jnp.where(h1_ref[rows, :] > 0, grad, 0.0)
        db1 = db1 + grad.reshape(CHUNK // 8, 8, HID).sum(axis=0)
        for c in range(TILES):
            yt[strided(row * TILES + c, CHUNK), :] = grad[:, c * LANES:(c + 1) * LANES]
    db1 = db1.sum(axis=0, keepdims=True)
    bias_ref[...] = db2.get()[...]
    for c in range(TILES):
        bias_ref[pl.ds(c, 1), :] = db1[:, c * LANES:(c + 1) * LANES]
        yt[strided(nodes * TILES + c, hubs), :] = dyh_ref[:, pl.ds(c * LANES, LANES)]
    dw2_ref[...] = dot(dz2_ref[...], h1_ref[...], CONTRACT_ROWS) + dot(dz2h_ref[...], h1h_ref[...], CONTRACT_ROWS)
    flush(dw2_ref, bias_ref)
    used_ref, hub_ref, xh_ref, wide_ref = used.get(), hub_ids.get(), xh.get(), wide.get()
    lists = [item.get() for item in lists]
    length = wide_ref.shape[0] // WAYS

    def place(i, carry):
        new = []
        for u in range(8):
            k = i * 8 + u
            new.append((hub_position(hub_ref, k, base, nodes, nodes + hubs), yt[pl.ds(pl.multiple_of((nodes + k) * TILES, TILES), TILES), :]))
        for row, value in new:
            yt[pl.ds(row, TILES), :] = value
        return carry

    lax.fori_loop(0, hubs // 8, place, 0)

    def step(i, carry):
        for n in range(unroll * WAYS):
            q, u = n % WAYS, n % copies
            j = pl.multiple_of(i * unroll, unroll) + n // WAYS
            d4 = pl.multiple_of(lists[q][j], TILES)
            s4 = pl.multiple_of(lists[WAYS + q][j], TILES)
            w = wide_ref[pl.ds(q * length + j, 1), :]
            za[u][pl.ds(s4, TILES), :] = za[u][pl.ds(s4, TILES), :] + w * yt[pl.ds(d4, TILES), :]
        return carry

    lax.fori_loop(0, trips(used_ref, unroll), step, 0)

    def fold(i, carry):
        new = []
        for u in range(8):
            k = i * 8 + u
            row = hub_position(hub_ref, k, base, nodes, nodes + halo + hubs)
            here = pl.ds(pl.multiple_of((nodes + halo + k) * TILES, TILES), TILES)
            new.append((row, here, za[0][here, :] + total_of(za, pl.ds(row, TILES))))
        for row, here, value in new:
            za[0][here, :] = value
            for acc in za:
                acc[pl.ds(row, TILES), :] = jnp.zeros((TILES, LANES), F32)
        return carry

    lax.fori_loop(0, hubs // 8, fold, 0)
    for row in range(0, nodes, CHUNK):
        for c in range(TILES):
            dz1_ref[pl.ds(row, CHUNK), pl.ds(c * LANES, LANES)] = total_of(za, strided(row * TILES + c, CHUNK))
    flush(dz1_ref)
    tag = xh_ref[...].astype(F32)[:, feat:feat + 1]
    onehot = (tag == (iota((halo, hubs), 1) + 1).astype(F32)).astype(BF16)
    for c in range(TILES):
        cols = pl.ds(c * LANES, LANES)
        hz = total_of(za, strided(nodes * TILES + c, halo))
        hub_out[:, cols] = total_of(za, strided((nodes + halo) * TILES + c, hubs)) + select_rows(onehot, hz, CONTRACT_ROWS)
        hz_ref[c] = jnp.where(tag > 0.0, 0.0, hz)


def last_kernel(groups, hub, hz, dw2, bias, sendrow, xt, hx, dz1, w1, hubrow,
                gxt_ref, dw1a, dw2a, bias_out,
                dz_out, onehot, hzr, hubp, hubh, hubr, biasp, biash, biasr, dhs, dha, dw2p, dw2h, dw2r, dw2s, dw1s, dw1r, dw1t, ssem, rsem, flush):
    me = lax.axis_index("graph")
    barrier = greet(groups, me)
    feat, nodes = xt.ref.shape
    chips, home = hub.ref.shape[1:3]
    hubs = groups * home
    block = hz.shape[2]
    halo = groups * block
    base = me * nodes
    core, chip = lax.rem(me, 2), me // 2
    partner = me + 1 - 2 * core
    own = hub_block(me, groups)
    peers = [lax.rem(me + step, groups) for step in range(1, groups)]
    others = [lax.rem(me + 2 * step, groups) for step in range(1, chips)]
    pl.semaphore_wait(barrier, groups - 1)

    def to(devices, slot, src, dst):
        return [send(src(peer), dst, ssem.at[slot, i], rsem.at[slot, i], peer) for i, peer in enumerate(devices)]

    def wait(pending):
        for copy in pending:
            copy.wait()

    halo_copies = [to(peers, 9, lambda p: hz.at[0, p], hzr.at[0, me])]
    hub_ref, dw2_ref, bias_ref = hub.get(), dw2.get(), bias.get()
    pair_copies = (to([partner], 0, lambda p: hub_ref.at[1 - core], hubp) + to([partner], 1, lambda p: dw2_ref.at[1 - core], dw2p)
                   + to([partner], 2, lambda p: bias_ref, biasp))
    sendrow = sendrow.get()[...]
    for row in range(0, nodes, CHUNK):
        onehot[pl.ds(row, CHUNK), :] = (iota((CHUNK, halo), 0) + row == sendrow).astype(BF16)
    for c in range(TILES):
        hzr[c, me] = jnp.zeros((block, LANES), F32)
        dw1s[c] = jnp.zeros(dw1s.shape[1:], F32)
    wait(pair_copies)
    hubh[...] = hub_ref[core] + hubp[...]
    dw2h[...] = dw2_ref[core] + dw2p[...]
    biash[...] = bias_ref[...] + biasp[...]
    hubr[chip] = hubh[chip]
    dw2r[chip] = dw2h[chip]
    biasr[chip] = biash[...]
    hub_copies = to(others, 3, lambda p: hubh.at[p // 2], hubr.at[chip])
    dw2_copies = to(others, 4, lambda p: dw2h.at[p // 2], dw2r.at[chip])
    bias_copies = to(others, 5, lambda p: biash, biasr.at[chip])
    halo_copies += [to(peers, 9 + c, lambda p: hz.at[c, p], hzr.at[c, me]) for c in range(1, TILES)]

    def total_over(ref, count):
        total = ref[0]
        for q in range(1, count):
            total = total + ref[q]
        return total

    xt_ref, dz1_ref, hx_ref, w1, hubrow = xt.get(), dz1.get(), hx.get(), w1.get()[...], hubrow.get()[...]
    rs_copies, ag_copies = [None] * TILES, [None] * TILES

    def spread(c):
        wait(rs_copies[c])
        total = total_over(dw1r.at[c], groups)
        dw1t[c] = total
        ag_copies[c] = to(peers, 17 + c, lambda p: dw1t.at[c], dw1a.at[c, me])
        dw1a[c, me] = total

    for c in range(TILES):
        wait(halo_copies[c])
        cols = pl.ds(c * LANES, LANES)
        pieces = jnp.concatenate(split3(hzr[c].reshape(halo, LANES)), axis=1)

        def rows_step(i, carry):
            rows = pl.ds(pl.multiple_of(i * TALL, TALL), TALL)
            value = dot(onehot[rows, :], pieces)
            value = value[:, 2 * LANES:] + value[:, LANES:2 * LANES] + value[:, :LANES]
            dz_out[rows, cols] = (dz1_ref[rows, cols] + value).astype(BF16)
            return carry

        lax.fori_loop(0, nodes // TALL, rows_step, 0)
        if c == 0:
            wait(hub_copies)
            dz1h = total_over(hubr, chips).astype(BF16)
            dhs[...] = dz1h
            back_copies = to(peers, 6, lambda p: dhs, dha.at[own])
            dha[own] = dz1h
            hx_mine = hx_ref[pl.ds(pl.multiple_of(own * home, 8), home), :].astype(BF16)
            dw1h = dot(hx_mine[:, :feat], dz1h, CONTRACT_ROWS)
        dw1s[c, pl.ds(0, feat), :] = dot(xt_ref[...], dz_out[:, cols]) + dw1h[:, c * LANES:(c + 1) * LANES]
        rs_copies[c] = to(peers, 13 + c, lambda p: dw1s.at[c, pl.ds(pl.multiple_of(p * 8, 8), 8)], dw1r.at[c, me])
        dw1r[c, me] = dw1s[c, pl.ds(pl.multiple_of(me * 8, 8), 8), :]
        if c == 0:
            wait(dw2_copies)
            total = total_over(dw2r, chips)
            dw2s[...] = total
            dw2_back = to(others, 7, lambda p: dw2s, dw2a.at[core, chip])
            dw2a[core, chip] = total
    for c in range(TILES - 1):
        spread(c)
    wait(dw2_back)
    dw2_pair = to([partner], 8, lambda p: dw2a.at[core], dw2a.at[core])
    wait(back_copies)
    hub_rows = dha[...].reshape(hubs, HID)
    for row in range(0, nodes, 2 * CHUNK):
        rows = pl.ds(row, 2 * CHUNK)
        owned = (iota((2 * CHUNK, hubs), 0) + (base + row) == hubrow).astype(BF16)
        dz = (dz_out[rows, :].astype(F32) + dot(owned, hub_rows)).astype(BF16)
        gxt_ref[:, rows] = dot(w1, dz, CONTRACT_COLS)
    flush(gxt_ref)
    wait(bias_copies)
    bias_out[...] = total_over(biasr, chips)
    flush(bias_out)
    spread(TILES - 1)
    wait(dw2_pair)
    flush(dw2a)
    for c in range(TILES):
        wait(ag_copies[c])


def outputs_kernel(gxt, dw2, bias, dw1, gxt_ref, gw1_ref, gw2_ref, gb1_ref, gb2_ref, flush):
    feat, out = gw1_ref.shape[0], gw2_ref.shape[1]
    gxt_ref[...] = gxt.get()[...]
    flush(gxt_ref)
    gw2_ref[...] = dw2.get()[...].T[:, :out]
    flush(gw2_ref)
    bias_ref, dw1_ref = bias.get(), dw1.get()
    for c in range(TILES):
        cols = pl.ds(c * LANES, LANES)
        for q in range(dw1_ref.shape[1]):
            rows = min(8, feat - q * 8)
            if rows > 0:
                gw1_ref[pl.ds(q * 8, rows), cols] = dw1_ref[c, q, pl.ds(0, rows), :]
        gb1_ref[:, cols] = bias_ref[pl.ds(c, 1), :]
    gb2_ref[...] = bias_ref[pl.ds(TILES, 1), pl.ds(0, out)]


def shape(dims, dtype):
    return jax.ShapeDtypeStruct(dims, dtype)


def solution(mesh):
    groups = mesh.shape["graph"]
    vertex_spec = P(("data", "graph"))
    vertex_rows = P(("data", "graph"), None)
    part_spec = P("data")
    part_rows = P("data", None)
    replicated = P()
    copies1, unroll1 = 3, 32
    copies2, unroll2 = 5, 32

    def params(collective_id=None):
        if collective_id is None:
            return pltpu.CompilerParams(vmem_limit_bytes=VMEM_LIMIT)
        return pltpu.CompilerParams(vmem_limit_bytes=VMEM_LIMIT, collective_id=collective_id, has_side_effects=True)

    def device_step(x_loc, dst_loc, src_loc, w_loc, send_loc, hub_ids, w_first, b_first, w_second, dy_out):
        nodes, feat = x_loc.shape
        edges = dst_loc.shape[0]
        halo = send_loc.shape[0]
        hubs = hub_ids.shape[0]
        out = dy_out.shape[1]
        block, home = halo // groups, hubs // groups
        src_rows, dst_rows = nodes + halo + 2 * hubs, nodes + 2 * hubs
        x_t = x_loc.T
        hub_lanes = hub_ids.reshape(1, hubs)
        send_lanes = send_loc.reshape(1, halo)
        bias = b_first.reshape(1, HID)
        sems = lambda n: [pltpu.SemaphoreType.DMA((n, groups)), pltpu.SemaphoreType.DMA((n, groups))]
        table = lambda a: a.reshape(edges // LANES, LANES)
        part_list = (edges // LANES // WAYS, LANES)
        packed = (block + hubs) // 2

        xh, hx, dhh, used, db2, *lists = call(
            functools.partial(gather_kernel, groups),
            [(hub_ids, "smem"), (dy_out, "vmem"), (hub_lanes, "vmem"), (x_t, "vmem"), (send_loc, "smem"),
             (table(dst_loc), "vmem"), (table(src_loc), "vmem"), (table(w_loc), "vmem")],
            (shape((halo, LANES), BF16), shape((hubs, LANES), F32), shape((hubs, LANES), F32),
             shape((8, LANES), I32), shape((8, LANES), F32))
            + (shape(part_list, I32),) * (2 * WAYS) + (shape(part_list, F32),) * WAYS,
            [pltpu.VMEM((nodes, LANES), F32), pltpu.VMEM((halo, LANES), F32), pltpu.VMEM((hubs, LANES), F32),
             pltpu.VMEM((hubs, LANES), F32), pltpu.VMEM((hubs, LANES), F32), pltpu.VMEM((hubs, LANES), F32),
             pltpu.VMEM((groups, packed, LANES), BF16), pltpu.VMEM((groups, packed, LANES), BF16),
             pltpu.VMEM((groups // 2, hubs, LANES), F32)] + sems(2),
            "gather_rows", params(0))
        lists = [(item.reshape(edges // WAYS), "smem") for item in lists]

        h1, dz, hz, hub = call(
            functools.partial(edges_forward_kernel, copies1, unroll1),
            [(w_first, "vmem"), (x_t, "vmem"), (dy_out, "vmem"), (xh, "vmem"), (hx, "vmem"), (dhh, "vmem"),
             (used, "smem"), (hub_ids, "smem"), (bias, "vmem")] + lists,
            (shape((nodes, HID), BF16), shape((nodes, LANES), F32), shape((halo, LANES), F32), shape((hubs, HID + LANES), F32)),
            [pltpu.VMEM((src_rows * TILES, LANES), F32), pltpu.VMEM((dst_rows * TILES, LANES), F32)]
            + [pltpu.VMEM((dst_rows * TILES, LANES), F32)] * copies1 + [pltpu.VMEM((src_rows * TILES, LANES), F32)] * copies1,
            "edges_forward", params())

        dz2, dyh, h1h, dz2h, wide = call(
            functools.partial(middle_kernel, groups),
            [(hub.reshape(groups, home, HID + LANES), "vmem"), (hz.reshape(groups, block, LANES), "vmem"), (dz, "vmem"),
             (bias, "vmem"), (w_second, "vmem"), (send_lanes, "vmem"), (table(w_loc), "vmem")],
            (shape((nodes, LANES), BF16), shape((hubs, HID), F32), shape((home, HID), BF16), shape((home, LANES), BF16), shape((edges, LANES), F32)),
            [pltpu.VMEM((groups, block, LANES), F32), pltpu.VMEM((groups, home, HID + LANES), F32),
             pltpu.VMEM((groups, home, HID), F32), pltpu.VMEM((home, HID), F32)] + sems(3),
            "middle", params(1))

        dz1, hz1, hub1, dw2, biases = call(
            functools.partial(edges_backward_kernel, copies2, unroll2, feat, groups),
            [(w_second, "vmem"), (h1, "vmem"), (dz2, "vmem"), (dyh, "vmem"), (h1h, "vmem"), (dz2h, "vmem"),
             (used, "smem"), (hub_ids, "smem"), (xh, "vmem"), (db2, "vmem"), (wide, "vmem")] + lists[:2 * WAYS],
            (shape((nodes, HID), F32), shape((TILES, halo, LANES), F32), shape((hubs, HID), F32), shape((LANES, HID), F32), shape((8, LANES), F32)),
            [pltpu.VMEM((dst_rows * TILES, LANES), F32)] + [pltpu.VMEM((src_rows * TILES, LANES), F32)] * copies2,
            "edges_backward", params())

        chips = groups // 2
        part = LANES // groups
        grad_xt, dw1, dw2, biases = call(
            functools.partial(last_kernel, groups),
            [(hub1.reshape(2, chips, home, HID), "vmem"), (hz1.reshape(TILES, groups, block, LANES), "hbm"),
             (dw2.reshape(2, chips, part, HID), "vmem"), (biases, "vmem"), (send_lanes, "vmem"), (x_t, "vmem"), (hx, "vmem"),
             (dz1, "vmem"), (w_first, "vmem"), (hub_lanes, "vmem")],
            (shape((feat, nodes), F32), shape((TILES, groups, 8, LANES), F32), shape((2, chips, part, HID), F32), shape((8, LANES), F32)),
            [pltpu.VMEM((nodes, HID), BF16), pltpu.VMEM((nodes, halo), BF16), pltpu.VMEM((TILES, groups, block, LANES), F32)]
            + [pltpu.VMEM((chips, home, HID), F32)] * 3 + [pltpu.VMEM((8, LANES), F32)] * 2 + [pltpu.VMEM((chips, 8, LANES), F32)]
            + [pltpu.VMEM((home, HID), BF16), pltpu.VMEM((groups, home, HID), BF16)]
            + [pltpu.VMEM((chips, part, HID), F32)] * 3 + [pltpu.VMEM((part, HID), F32)]
            + [pltpu.VMEM((TILES, groups * 8, LANES), F32), pltpu.VMEM((TILES, groups, 8, LANES), F32), pltpu.VMEM((TILES, 8, LANES), F32)] + sems(21),
            "last_exchange", params(2))

        grad_xt, grad_w1, grad_w2, grad_b1, grad_b2 = call(
            outputs_kernel,
            [(grad_xt, "vmem"), (dw2.reshape(LANES, HID), "vmem"), (biases, "vmem"), (dw1, "vmem")],
            (shape((feat, nodes), F32), shape((feat, HID), F32), shape((HID, out), F32), shape((1, HID), F32), shape((1, out), F32)),
            [], "outputs", params())
        return grad_xt.T, grad_w1, grad_w2, grad_b1.reshape(HID), grad_b2.reshape(out)

    return jax.shard_map(
        device_step,
        mesh=mesh,
        in_specs=(vertex_rows, vertex_spec, vertex_spec, vertex_spec, vertex_spec, part_spec, replicated, replicated, replicated, vertex_rows),
        out_specs=(vertex_rows, part_rows, part_rows, part_spec, part_spec),
        check_vma=False,
    )
```

```python
import functools

import jax
import jax.numpy as jnp
from jax import lax
from jax.experimental import pallas as pl
from jax.experimental.pallas import tpu as pltpu
from jax.sharding import PartitionSpec as P

F32, BF16, I32 = jnp.float32, jnp.bfloat16, jnp.int32
CONTRACT_ROWS = (((0,), (0,)), ((), ()))
CONTRACT_COLS = (((1,), (1,)), ((), ()))
LANES = 128
WAYS = 4
HID = 512
TILES = HID // LANES
CHUNK = 256
TALL = 2048
MIDDLE = 1024
VMEM_LIMIT = 67043328
HBM = pl.BlockSpec(memory_space=pltpu.HBM)


class Fetched:
    def __init__(self, src, dst, sem):
        self.copy, self.ref, self.pending = pltpu.make_async_copy(src, dst, sem), dst, True
        self.copy.start()

    def get(self):
        if self.pending:
            self.copy.wait()
            self.pending = False
        return self.ref


def call(kernel, args, out_shape, scratch_shapes, name, compiler_params):
    spaces = {"vmem": pltpu.VMEM, "smem": pltpu.SMEM}
    moved = [n for n, (_, space) in enumerate(args) if space != "hbm"]
    in_buffers = [spaces[args[n][1]](args[n][0].shape, args[n][0].dtype) for n in moved]
    out_buffers = [pltpu.VMEM(out.shape, out.dtype) for out in out_shape]
    n_in, n_out = len(args), len(out_shape)

    def body(*refs):
        inputs, outputs = refs[:n_in], refs[n_in:n_in + n_out]
        bufs = refs[n_in + n_out:n_in + 2 * n_out + len(moved)]
        scratch, sems, out_sems = refs[n_in + 2 * n_out + len(moved):-2], refs[-2], refs[-1]
        fetched = list(inputs)
        for k, n in enumerate(moved):
            fetched[n] = Fetched(inputs[n], bufs[k], sems.at[k])
        results = bufs[len(moved):]
        stores = {}

        def flush(*buffers):
            for buffer in buffers:
                n = [k for k in range(n_out) if results[k] is buffer][0]
                stores[n] = pltpu.make_async_copy(results[n], outputs[n], out_sems.at[n])
                stores[n].start()

        kernel(*fetched, *results, *scratch, flush=flush)
        for n in moved:
            fetched[n].get()
        flush(*[results[n] for n in range(n_out) if n not in stores])
        for n in range(n_out):
            stores[n].wait()

    return pl.pallas_call(
        body,
        name=name,
        out_shape=out_shape,
        in_specs=[HBM] * n_in,
        out_specs=(HBM,) * n_out,
        scratch_shapes=in_buffers + out_buffers + list(scratch_shapes) + [pltpu.SemaphoreType.DMA((n_in,)), pltpu.SemaphoreType.DMA((n_out,))],
        compiler_params=compiler_params,
    )(*[array for array, _ in args])


def dot(a, b, dims=(((1,), (0,)), ((), ()))):
    return lax.dot_general(a, b, dims, preferred_element_type=F32)


def iota(shape, dim):
    return lax.broadcasted_iota(I32, shape, dim)


def split3(value):
    high = value.astype(BF16)
    rest = value - high.astype(F32)
    mid = rest.astype(BF16)
    low = (rest - mid.astype(F32)).astype(BF16)
    return high, mid, low


def select_rows(onehot, value, dims=(((1,), (0,)), ((), ()))):
    width = value.shape[1]
    picked = dot(onehot, jnp.concatenate(split3(value), axis=1), dims)
    return picked[:, 2 * width:] + picked[:, width:2 * width] + picked[:, :width]


def pad_lanes(value):
    rows, cols = value.shape
    if cols == LANES:
        return value
    return jnp.concatenate([value, jnp.zeros((rows, LANES - cols), value.dtype)], axis=1)


def hub_block(device, groups):
    return lax.rem(device, 2) * (groups // 2) + device // 2


def greet(groups, me):
    barrier = pltpu.get_barrier_semaphore()
    for step in range(1, groups):
        pl.semaphore_signal(barrier, inc=1, device_id={"graph": lax.rem(me + step, groups)}, device_id_type=pl.DeviceIdType.MESH)
    return barrier


def send(src, dst, send_sem, recv_sem, peer):
    copy = pltpu.make_async_remote_copy(
        src_ref=src, dst_ref=dst, send_sem=send_sem, recv_sem=recv_sem,
        device_id={"graph": peer}, device_id_type=pl.DeviceIdType.MESH)
    copy.start()
    return copy


def pack_rows(value):
    half = value.shape[0] // 2
    low = iota((half, LANES), 1) < LANES // 2
    return jnp.where(low, value[:half], pltpu.roll(value[half:], LANES // 2, 1)).astype(BF16)


def unpack_rows(value):
    return jnp.concatenate([value, pltpu.roll(value, LANES // 2, 1)], axis=0)


def gather_kernel(groups, hub_ids, dh, hubrow, xt, send_idx, dst, src, w,
                  xh_ref, hx_ref, dhh_ref, used_ref, db2_ref, *rest, flush):
    lists, (x32, xg, hxg, dhg, dhp, dhs, xs, xr, dhr, ssem, rsem) = rest[:3 * WAYS], rest[3 * WAYS:]
    me = lax.axis_index("graph")
    barrier = greet(groups, me)
    feat, nodes = xt.ref.shape
    hubs = hub_ids.ref.shape[0]
    halo = send_idx.ref.shape[0]
    block = halo // groups
    base = me * nodes
    chips = groups // 2
    core, chip = lax.rem(me, 2), me // 2
    dhg[...] = jnp.zeros_like(dhg)
    hub_ref, dh_ref = hub_ids.get(), dh.get()

    def hub_position_of(k):
        row = hub_ref[k] - base
        return jnp.logical_and(row >= 0, row < nodes), jnp.clip(row, 0, nodes - 1)

    def pick_grad(i, carry):
        for u in range(8):
            k = i * 8 + u
            own, row = hub_position_of(k)
            value = dh_ref[pl.ds(row, 1), :]
            dhg[pl.ds(k, 1), pl.ds(0, value.shape[1])] = jnp.where(own, value, 0.0)
        return carry

    lax.fori_loop(0, hubs // 8, pick_grad, 0)
    pl.semaphore_wait(barrier, groups - 1)
    pair = send(dhg, dhp, ssem.at[1, 0], rsem.at[1, 0], me + 1 - 2 * core)
    eye = (iota((feat, LANES), 0) == iota((feat, LANES), 1)).astype(BF16)
    tags = jnp.where(iota((hubs, LANES), 1) == feat, iota((hubs, LANES), 0) + 1, 0).astype(F32).astype(BF16)
    hubrow = hubrow.get()[...]
    xt_ref = xt.get()
    for row in range(0, nodes, CHUNK):
        owned = (iota((CHUNK, hubs), 0) + (base + row) == hubrow).astype(BF16)
        x32[pl.ds(row, CHUNK), :] = dot(xt_ref[:, pl.ds(row, CHUNK)], eye, CONTRACT_ROWS) + dot(owned, tags)
    send_ref = send_idx.get()

    def pick(i, carry):
        for u in range(16):
            j = i * 16 + u
            xg[pl.ds(j, 1), :] = x32[pl.ds(send_ref[j], 1), :]
        return carry

    lax.fori_loop(0, halo // 16, pick, 0)

    def pick_hub(i, carry):
        for u in range(8):
            k = i * 8 + u
            own, row = hub_position_of(k)
            hxg[pl.ds(k, 1), :] = jnp.where(own, x32[pl.ds(row, 1), :], 0.0)
        return carry

    lax.fori_loop(0, hubs // 8, pick_hub, 0)
    hub_rows = pack_rows(hxg[...])
    for q in range(groups):
        xs[q, pl.ds(0, block // 2), :] = pack_rows(xg[pl.ds(q * block, block), :])
        xs[q, pl.ds(block // 2, hubs // 2), :] = hub_rows
    copies = []
    for step in range(1, groups):
        peer = lax.rem(me + step, groups)
        copies.append(send(xs.at[peer], xr.at[me], ssem.at[0, step], rsem.at[0, step], peer))
    pair.wait()
    dhs[...] = dhg[...] + dhp[...]
    dhr[chip] = dhs[...]
    half = pl.ds(pl.multiple_of(core * (hubs // 2), 8), hubs // 2)
    for step in range(1, chips):
        for other in range(2):
            n = 2 * step + other
            peer = 2 * lax.rem(chip + step, chips) + lax.rem(core + other, 2)
            copies.append(send(dhs.at[half], dhr.at[chip, half], ssem.at[1, n], rsem.at[1, n], peer))
    dst_ref, src_ref, w_ref = dst.get(), src.get(), w.get()
    blocks = w_ref.shape[0]
    for q in range(WAYS):
        part = pl.ds(q, blocks // WAYS, stride=WAYS)
        lists[q][...] = dst_ref[part, :] * TILES
        lists[WAYS + q][...] = src_ref[part, :] * TILES
        lists[2 * WAYS + q][...] = w_ref[part, :]
    flush(*lists)
    place = (iota(w_ref.shape, 0) * LANES + iota(w_ref.shape, 1) + 1).astype(F32)
    used = jnp.where(w_ref[...] > 0.0, place, 0.0).max(axis=0, keepdims=True).max(axis=1, keepdims=True)
    used_ref[...] = jnp.broadcast_to(used, used_ref.shape).astype(I32)
    total = jnp.zeros((8, dh_ref.shape[1]), F32)
    for row in range(0, nodes, CHUNK):
        total = total + dh_ref[pl.ds(row, CHUNK), :].reshape(CHUNK // 8, 8, dh_ref.shape[1]).sum(axis=0)
    db2_ref[...] = jnp.broadcast_to(pad_lanes(total.sum(axis=0, keepdims=True)), db2_ref.shape)
    flush(used_ref, db2_ref)
    xr[me] = xs[me]
    for copy in copies:
        copy.wait()
    hx = jnp.zeros((hubs // 2, LANES), F32)
    dhh = jnp.zeros((hubs, LANES), F32)
    for q in range(groups):
        xh_ref[pl.ds(q * block, block), :] = unpack_rows(xr[q, pl.ds(0, block // 2), :].astype(F32)).astype(BF16)
        hx = hx + xr[q, pl.ds(block // 2, hubs // 2), :].astype(F32)
    for q in range(chips):
        dhh = dhh + dhr[q]
    hx_ref[...] = unpack_rows(hx)
    dhh_ref[...] = dhh


def hub_position(hub_ref, k, base, nodes, spare):
    row = hub_ref[k] - base
    own = jnp.logical_and(row >= 0, row < nodes)
    return pl.multiple_of(jnp.where(own, row, spare + k) * TILES, TILES)


def trips(used_ref, unroll):
    return (used_ref[0, 0] + (WAYS * LANES - 1)) // (WAYS * LANES) * (LANES // unroll)


def strided(first, rows):
    return pl.ds(first, rows, stride=TILES)


def total_of(refs, where):
    value = refs[0][where, :]
    for ref in refs[1:]:
        value = value + ref[where, :]
    return value


def edges_forward_kernel(copies, unroll, w1, xt, dh, xh, hx, dhh, used, hub_ids, b1, *rest, flush):
    lists, (h1_ref, dz_ref, hz_ref, hub_out, zt, dt), accs = rest[:3 * WAYS], rest[3 * WAYS:3 * WAYS + 6], rest[3 * WAYS + 6:]
    ya, da = accs[:copies], accs[copies:]
    me = lax.axis_index("graph")
    feat, nodes = xt.ref.shape
    halo, hubs = xh.ref.shape[0], hx.ref.shape[0]
    base = me * nodes
    for acc in ya:
        acc[...] = jnp.zeros_like(acc)
    for acc in da:
        acc[strided(0, nodes + halo + 2 * hubs), :] = jnp.zeros((nodes + halo + 2 * hubs, LANES), F32)
    w1 = w1.get()[...]
    xt_ref, dh_ref, xh_ref, hx_ref = xt.get(), dh.get(), xh.get(), hx.get()

    def put_rows(first, z):
        z = z.astype(BF16).astype(F32)
        for c in range(TILES):
            zt[strided(first * TILES + c, z.shape[0]), :] = z[:, c * LANES:(c + 1) * LANES]

    for row in range(0, nodes, CHUNK):
        put_rows(row, dot(xt_ref[:, pl.ds(row, CHUNK)], w1, CONTRACT_ROWS))
        dt[strided(row * TILES, CHUNK), :] = pad_lanes(dh_ref[pl.ds(row, CHUNK), :])
    for row in range(0, halo, CHUNK):
        put_rows(nodes + row, dot(xh_ref[pl.ds(row, CHUNK), pl.ds(0, feat)], w1))
    put_rows(nodes + halo, dot(hx_ref[:, pl.ds(0, feat)].astype(BF16), w1))
    dt[strided(nodes * TILES, hubs), :] = dhh.get()[...]
    used_ref, hub_ref, b1_ref = used.get(), hub_ids.get(), b1.get()
    lists = [item.get() for item in lists]

    def step(i, carry):
        for n in range(unroll * WAYS):
            q, u = n % WAYS, n % copies
            j = i * unroll + n // WAYS
            d4 = pl.multiple_of(lists[q][j], TILES)
            s4 = pl.multiple_of(lists[WAYS + q][j], TILES)
            w = lists[2 * WAYS + q][j]
            y_new = ya[u][pl.ds(d4, TILES), :] + w * zt[pl.ds(s4, TILES), :]
            z_new = da[u][pl.ds(s4, 1), :] + w * dt[pl.ds(d4, 1), :]
            ya[u][pl.ds(d4, TILES), :] = y_new
            da[u][pl.ds(s4, 1), :] = z_new
        return carry

    lax.fori_loop(0, trips(used_ref, unroll), step, 0)

    def fold(i, carry):
        new = []
        for u in range(8):
            k = i * 8 + u
            y_row = hub_position(hub_ref, k, base, nodes, nodes + hubs)
            z_row = hub_position(hub_ref, k, base, nodes, nodes + halo + hubs)
            y_hub = pl.ds(pl.multiple_of((nodes + k) * TILES, TILES), TILES)
            z_hub = pl.ds(pl.multiple_of((nodes + halo + k) * TILES, TILES), 1)
            new.append((y_hub, z_hub, z_row, ya[0][y_hub, :] + total_of(ya, pl.ds(y_row, TILES)), da[0][z_hub, :] + total_of(da, pl.ds(z_row, 1))))
        for y_hub, z_hub, z_row, y_new, z_new in new:
            ya[0][y_hub, :] = y_new
            da[0][z_hub, :] = z_new
            for acc in da:
                acc[pl.ds(z_row, 1), :] = jnp.zeros((1, LANES), F32)
        return carry

    lax.fori_loop(0, hubs // 8, fold, 0)
    for row in range(0, nodes, CHUNK):
        for c in range(TILES):
            cols = pl.ds(c * LANES, LANES)
            y = total_of(ya, strided(row * TILES + c, CHUNK)) + b1_ref[:, cols]
            h1_ref[pl.ds(row, CHUNK), cols] = jnp.maximum(y, 0.0).astype(BF16)
    flush(h1_ref)
    for row in range(0, nodes, CHUNK):
        dz_ref[pl.ds(row, CHUNK), :] = total_of(da, strided(row * TILES, CHUNK))
    flush(dz_ref)
    hz = total_of(da, strided(nodes * TILES, halo))
    tag = xh_ref[...].astype(F32)[:, feat:feat + 1]
    onehot = (tag == (iota((halo, hubs), 1) + 1).astype(F32)).astype(BF16)
    hub_z = total_of(da, strided((nodes + halo) * TILES, hubs)) + select_rows(onehot, hz, CONTRACT_ROWS)
    hz_ref[...] = jnp.where(tag > 0.0, 0.0, hz)
    for c in range(TILES):
        hub_out[:, pl.ds(c * LANES, LANES)] = total_of(ya, strided(nodes * TILES + c, hubs))
    hub_out[:, pl.ds(HID, LANES)] = hub_z


def middle_kernel(groups, hub, hz, dz, b1, w2, sendrow, w,
                  dz2_ref, dyh_ref, h1h_ref, dz2h_ref, wide_ref,
                  hzr, hubr, dyr, dys, ssem, rsem, flush):
    me = lax.axis_index("graph")
    barrier = greet(groups, me)
    nodes = dz.ref.shape[0]
    out = w2.ref.shape[1]
    home = hub.ref.shape[1]
    block = hz.ref.shape[1]
    halo = groups * block
    hub_ref, hz_ref = hub.get(), hz.get()
    own = hub_block(me, groups)
    hubr[me] = hub_ref[own]
    hzr[me] = jnp.zeros(hzr.shape[1:], F32)
    pl.semaphore_wait(barrier, groups - 1)
    hub_copies, halo_copies, back = [], [], []
    for step in range(1, groups):
        peer = lax.rem(me + step, groups)
        hub_copies.append(send(hub_ref.at[hub_block(peer, groups)], hubr.at[me], ssem.at[0, step], rsem.at[0, step], peer))
    for step in range(1, groups):
        peer = lax.rem(me + step, groups)
        halo_copies.append(send(hz_ref.at[peer], hzr.at[me], ssem.at[1, step], rsem.at[1, step], peer))
    w_ref = w.get()
    blocks = w_ref.shape[0]
    diagonal = iota((LANES, LANES), 0) == iota((LANES, LANES), 1)
    ones = jnp.ones((LANES, LANES), BF16)

    def widen(i, carry):
        for q in range(WAYS):
            row = w_ref[pl.ds(i * WAYS + q, 1), :]
            spread = jnp.zeros((LANES, LANES), F32)
            for piece in reversed(split3(row)):
                column = jnp.where(diagonal, jnp.broadcast_to(piece.astype(F32), (LANES, LANES)), 0.0).astype(BF16)
                spread = spread + dot(column, ones)
            wide_ref[pl.ds(pl.multiple_of((q * (blocks // WAYS) + i) * LANES, LANES), LANES), :] = spread
        return carry

    lax.fori_loop(0, blocks // WAYS, widen, 0)
    flush(wide_ref)
    for copy in hub_copies:
        copy.wait()
    total = hubr[0]
    for q in range(1, groups):
        total = total + hubr[q]
    b1_ref, w2_ref, sendrow = b1.get(), w2.get(), sendrow.get()[...]
    pre = total[:, :HID] + b1_ref[...]
    dz2h = total[:, HID:].astype(BF16)
    h1h_ref[...] = jnp.maximum(pre, 0.0).astype(BF16)
    dz2h_ref[...] = dz2h
    dys[...] = jnp.where(pre > 0, dot(dz2h[:, :out], w2_ref[...], CONTRACT_COLS), 0.0)
    for step in range(1, groups):
        peer = lax.rem(me + step, groups)
        back.append(send(dys, dyr.at[own], ssem.at[2, step], rsem.at[2, step], peer))
    dyr[own] = dys[...]
    for copy in halo_copies:
        copy.wait()
    pieces = jnp.concatenate(split3(hzr[...].reshape(halo, LANES)), axis=1)
    dz_ref = dz.get()
    for row in range(0, nodes, MIDDLE):
        onehot = (iota((MIDDLE, halo), 0) + row == sendrow).astype(BF16)
        value = dot(onehot, pieces)
        value = value[:, 2 * LANES:] + value[:, LANES:2 * LANES] + value[:, :LANES]
        dz2_ref[pl.ds(row, MIDDLE), :] = (dz_ref[pl.ds(row, MIDDLE), :] + value).astype(BF16)
    for copy in back:
        copy.wait()
    for q in range(groups):
        dyh_ref[pl.ds(q * home, home), :] = dyr[q]


def edges_backward_kernel(copies, unroll, feat, groups, w2, h1, dz2, dyh, h1h, dz2h, used, hub_ids, xh, db2, wide, *rest, flush):
    lists, rest = rest[:2 * WAYS], rest[2 * WAYS:]
    (dz1_ref, hz_ref, hub_out, dw2_ref, bias_ref, yt), za = rest[:6], rest[6:]
    me = lax.axis_index("graph")
    nodes = h1.ref.shape[0]
    out = w2.ref.shape[1]
    halo, hubs = xh.ref.shape[0], dyh.ref.shape[0]
    home = h1h.ref.shape[0]
    base = me * nodes
    for acc in za:
        acc[...] = jnp.zeros_like(acc)
    w2, h1_ref, dz2_ref, dyh_ref, h1h_ref, dz2h_ref = w2.get()[...], h1.get(), dz2.get(), dyh.get(), h1h.get(), dz2h.get()
    mine = dyh_ref[pl.ds(pl.multiple_of(hub_block(me, groups) * home, 8), home), :]
    db1 = mine
    for row in range(0, nodes, CHUNK):
        rows = pl.ds(row, CHUNK)
        grad = dot(dz2_ref[rows, pl.ds(0, out)], w2, CONTRACT_COLS)
        grad = jnp.where(h1_ref[rows, :] > 0, grad, 0.0)
        db1 = db1 + grad.reshape(CHUNK // 8, 8, HID).sum(axis=0)
        for c in range(TILES):
            yt[strided(row * TILES + c, CHUNK), :] = grad[:, c * LANES:(c + 1) * LANES]
    db1 = db1.sum(axis=0, keepdims=True)
    bias_ref[...] = db2.get()[...]
    for c in range(TILES):
        bias_ref[pl.ds(c, 1), :] = db1[:, c * LANES:(c + 1) * LANES]
        yt[strided(nodes * TILES + c, hubs), :] = dyh_ref[:, pl.ds(c * LANES, LANES)]
    dw2_ref[...] = dot(dz2_ref[...], h1_ref[...], CONTRACT_ROWS) + dot(dz2h_ref[...], h1h_ref[...], CONTRACT_ROWS)
    flush(dw2_ref, bias_ref)
    used_ref, hub_ref, xh_ref, wide_ref = used.get(), hub_ids.get(), xh.get(), wide.get()
    lists = [item.get() for item in lists]
    length = wide_ref.shape[0] // WAYS

    def place(i, carry):
        new = []
        for u in range(8):
            k = i * 8 + u
            new.append((hub_position(hub_ref, k, base, nodes, nodes + hubs), yt[pl.ds(pl.multiple_of((nodes + k) * TILES, TILES), TILES), :]))
        for row, value in new:
            yt[pl.ds(row, TILES), :] = value
        return carry

    lax.fori_loop(0, hubs // 8, place, 0)

    def step(i, carry):
        for n in range(unroll * WAYS):
            q, u = n % WAYS, n % copies
            j = pl.multiple_of(i * unroll, unroll) + n // WAYS
            d4 = pl.multiple_of(lists[q][j], TILES)
            s4 = pl.multiple_of(lists[WAYS + q][j], TILES)
            w = wide_ref[pl.ds(q * length + j, 1), :]
            za[u][pl.ds(s4, TILES), :] = za[u][pl.ds(s4, TILES), :] + w * yt[pl.ds(d4, TILES), :]
        return carry

    lax.fori_loop(0, trips(used_ref, unroll), step, 0)

    def fold(i, carry):
        new = []
        for u in range(8):
            k = i * 8 + u
            row = hub_position(hub_ref, k, base, nodes, nodes + halo + hubs)
            here = pl.ds(pl.multiple_of((nodes + halo + k) * TILES, TILES), TILES)
            new.append((row, here, za[0][here, :] + total_of(za, pl.ds(row, TILES))))
        for row, here, value in new:
            za[0][here, :] = value
            for acc in za:
                acc[pl.ds(row, TILES), :] = jnp.zeros((TILES, LANES), F32)
        return carry

    lax.fori_loop(0, hubs // 8, fold, 0)
    for row in range(0, nodes, CHUNK):
        for c in range(TILES):
            dz1_ref[pl.ds(row, CHUNK), pl.ds(c * LANES, LANES)] = total_of(za, strided(row * TILES + c, CHUNK))
    flush(dz1_ref)
    tag = xh_ref[...].astype(F32)[:, feat:feat + 1]
    onehot = (tag == (iota((halo, hubs), 1) + 1).astype(F32)).astype(BF16)
    for c in range(TILES):
        cols = pl.ds(c * LANES, LANES)
        hz = total_of(za, strided(nodes * TILES + c, halo))
        hub_out[:, cols] = total_of(za, strided((nodes + halo) * TILES + c, hubs)) + select_rows(onehot, hz, CONTRACT_ROWS)
        hz_ref[c] = jnp.where(tag > 0.0, 0.0, hz)


def last_kernel(groups, hub, hz, dw2, bias, sendrow, xt, hx, dz1, w1, hubrow,
                gxt_ref, dw1a, dw2a, bias_out,
                dz_out, onehot, hzr, hubp, hubh, hubr, biasp, biash, biasr, dhs, dha, dw2p, dw2h, dw2r, dw2s, dw1s, dw1r, dw1t, ssem, rsem, flush):
    me = lax.axis_index("graph")
    barrier = greet(groups, me)
    feat, nodes = xt.ref.shape
    chips, home = hub.ref.shape[1:3]
    hubs = groups * home
    block = hz.shape[2]
    halo = groups * block
    base = me * nodes
    core, chip = lax.rem(me, 2), me // 2
    partner = me + 1 - 2 * core
    own = hub_block(me, groups)
    peers = [lax.rem(me + step, groups) for step in range(1, groups)]
    others = [lax.rem(me + 2 * step, groups) for step in range(1, chips)]
    pl.semaphore_wait(barrier, groups - 1)

    def to(devices, slot, src, dst):
        return [send(src(peer), dst, ssem.at[slot, i], rsem.at[slot, i], peer) for i, peer in enumerate(devices)]

    def wait(pending):
        for copy in pending:
            copy.wait()

    halo_copies = [to(peers, 9, lambda p: hz.at[0, p], hzr.at[0, me])]
    hub_ref, dw2_ref, bias_ref = hub.get(), dw2.get(), bias.get()
    pair_copies = (to([partner], 0, lambda p: hub_ref.at[1 - core], hubp) + to([partner], 1, lambda p: dw2_ref.at[1 - core], dw2p)
                   + to([partner], 2, lambda p: bias_ref, biasp))
    sendrow = sendrow.get()[...]
    for row in range(0, nodes, CHUNK):
        onehot[pl.ds(row, CHUNK), :] = (iota((CHUNK, halo), 0) + row == sendrow).astype(BF16)
    for c in range(TILES):
        hzr[c, me] = jnp.zeros((block, LANES), F32)
        dw1s[c] = jnp.zeros(dw1s.shape[1:], F32)
    wait(pair_copies)
    hubh[...] = hub_ref[core] + hubp[...]
    dw2h[...] = dw2_ref[core] + dw2p[...]
    biash[...] = bias_ref[...] + biasp[...]
    hubr[chip] = hubh[chip]
    dw2r[chip] = dw2h[chip]
    biasr[chip] = biash[...]
    hub_copies = to(others, 3, lambda p: hubh.at[p // 2], hubr.at[chip])
    dw2_copies = to(others, 4, lambda p: dw2h.at[p // 2], dw2r.at[chip])
    bias_copies = to(others, 5, lambda p: biash, biasr.at[chip])
    halo_copies += [to(peers, 9 + c, lambda p: hz.at[c, p], hzr.at[c, me]) for c in range(1, TILES)]

    def total_over(ref, count):
        total = ref[0]
        for q in range(1, count):
            total = total + ref[q]
        return total

    xt_ref, dz1_ref, hx_ref, w1, hubrow = xt.get(), dz1.get(), hx.get(), w1.get()[...], hubrow.get()[...]
    rs_copies, ag_copies = [None] * TILES, [None] * TILES

    def spread(c):
        wait(rs_copies[c])
        total = total_over(dw1r.at[c], groups)
        dw1t[c] = total
        ag_copies[c] = to(peers, 17 + c, lambda p: dw1t.at[c], dw1a.at[c, me])
        dw1a[c, me] = total

    for c in range(TILES):
        wait(halo_copies[c])
        cols = pl.ds(c * LANES, LANES)
        pieces = jnp.concatenate(split3(hzr[c].reshape(halo, LANES)), axis=1)

        def rows_step(i, carry):
            rows = pl.ds(pl.multiple_of(i * TALL, TALL), TALL)
            value = dot(onehot[rows, :], pieces)
            value = value[:, 2 * LANES:] + value[:, LANES:2 * LANES] + value[:, :LANES]
            dz_out[rows, cols] = (dz1_ref[rows, cols] + value).astype(BF16)
            return carry

        lax.fori_loop(0, nodes // TALL, rows_step, 0)
        if c == 0:
            wait(hub_copies)
            dz1h = total_over(hubr, chips).astype(BF16)
            dhs[...] = dz1h
            back_copies = to(peers, 6, lambda p: dhs, dha.at[own])
            dha[own] = dz1h
            hx_mine = hx_ref[pl.ds(pl.multiple_of(own * home, 8), home), :].astype(BF16)
            dw1h = dot(hx_mine[:, :feat], dz1h, CONTRACT_ROWS)
        dw1s[c, pl.ds(0, feat), :] = dot(xt_ref[...], dz_out[:, cols]) + dw1h[:, c * LANES:(c + 1) * LANES]
        rs_copies[c] = to(peers, 13 + c, lambda p: dw1s.at[c, pl.ds(pl.multiple_of(p * 8, 8), 8)], dw1r.at[c, me])
        dw1r[c, me] = dw1s[c, pl.ds(pl.multiple_of(me * 8, 8), 8), :]
        if c == 0:
            wait(dw2_copies)
            total = total_over(dw2r, chips)
            dw2s[...] = total
            dw2_back = to(others, 7, lambda p: dw2s, dw2a.at[core, chip])
            dw2a[core, chip] = total
    for c in range(TILES - 1):
        spread(c)
    wait(dw2_back)
    dw2_pair = to([partner], 8, lambda p: dw2a.at[core], dw2a.at[core])
    wait(back_copies)
    hub_rows = dha[...].reshape(hubs, HID)
    for row in range(0, nodes, 2 * CHUNK):
        rows = pl.ds(row, 2 * CHUNK)
        owned = (iota((2 * CHUNK, hubs), 0) + (base + row) == hubrow).astype(BF16)
        dz = (dz_out[rows, :].astype(F32) + dot(owned, hub_rows)).astype(BF16)
        gxt_ref[:, rows] = dot(w1, dz, CONTRACT_COLS)
    flush(gxt_ref)
    wait(bias_copies)
    bias_out[...] = total_over(biasr, chips)
    flush(bias_out)
    spread(TILES - 1)
    wait(dw2_pair)
    flush(dw2a)
    for c in range(TILES):
        wait(ag_copies[c])


def outputs_kernel(gxt, dw2, bias, dw1, gxt_ref, gw1_ref, gw2_ref, gb1_ref, gb2_ref, flush):
    feat, out = gw1_ref.shape[0], gw2_ref.shape[1]
    gxt_ref[...] = gxt.get()[...]
    flush(gxt_ref)
    gw2_ref[...] = dw2.get()[...].T[:, :out]
    flush(gw2_ref)
    bias_ref, dw1_ref = bias.get(), dw1.get()
    for c in range(TILES):
        cols = pl.ds(c * LANES, LANES)
        for q in range(dw1_ref.shape[1]):
            rows = min(8, feat - q * 8)
            if rows > 0:
                gw1_ref[pl.ds(q * 8, rows), cols] = dw1_ref[c, q, pl.ds(0, rows), :]
        gb1_ref[:, cols] = bias_ref[pl.ds(c, 1), :]
    gb2_ref[...] = bias_ref[pl.ds(TILES, 1), pl.ds(0, out)]


def shape(dims, dtype):
    return jax.ShapeDtypeStruct(dims, dtype)


def solution(mesh):
    groups = mesh.shape["graph"]
    vertex_spec = P(("data", "graph"))
    vertex_rows = P(("data", "graph"), None)
    part_spec = P("data")
    part_rows = P("data", None)
    replicated = P()
    copies1, unroll1 = 3, 32
    copies2, unroll2 = 5, 32

    def params(collective_id=None):
        if collective_id is None:
            return pltpu.CompilerParams(vmem_limit_bytes=VMEM_LIMIT)
        return pltpu.CompilerParams(vmem_limit_bytes=VMEM_LIMIT, collective_id=collective_id, has_side_effects=True)

    def device_step(x_loc, dst_loc, src_loc, w_loc, send_loc, hub_ids, w_first, b_first, w_second, dy_out):
        nodes, feat = x_loc.shape
        edges = dst_loc.shape[0]
        halo = send_loc.shape[0]
        hubs = hub_ids.shape[0]
        out = dy_out.shape[1]
        block, home = halo // groups, hubs // groups
        src_rows, dst_rows = nodes + halo + 2 * hubs, nodes + 2 * hubs
        x_t = x_loc.T
        hub_lanes = hub_ids.reshape(1, hubs)
        send_lanes = send_loc.reshape(1, halo)
        bias = b_first.reshape(1, HID)
        sems = lambda n: [pltpu.SemaphoreType.DMA((n, groups)), pltpu.SemaphoreType.DMA((n, groups))]
        table = lambda a: a.reshape(edges // LANES, LANES)
        part_list = (edges // LANES // WAYS, LANES)
        packed = (block + hubs) // 2

        xh, hx, dhh, used, db2, *lists = call(
            functools.partial(gather_kernel, groups),
            [(hub_ids, "smem"), (dy_out, "vmem"), (hub_lanes, "vmem"), (x_t, "vmem"), (send_loc, "smem"),
             (table(dst_loc), "vmem"), (table(src_loc), "vmem"), (table(w_loc), "vmem")],
            (shape((halo, LANES), BF16), shape((hubs, LANES), F32), shape((hubs, LANES), F32),
             shape((8, LANES), I32), shape((8, LANES), F32))
            + (shape(part_list, I32),) * (2 * WAYS) + (shape(part_list, F32),) * WAYS,
            [pltpu.VMEM((nodes, LANES), F32), pltpu.VMEM((halo, LANES), F32), pltpu.VMEM((hubs, LANES), F32),
             pltpu.VMEM((hubs, LANES), F32), pltpu.VMEM((hubs, LANES), F32), pltpu.VMEM((hubs, LANES), F32),
             pltpu.VMEM((groups, packed, LANES), BF16), pltpu.VMEM((groups, packed, LANES), BF16),
             pltpu.VMEM((groups // 2, hubs, LANES), F32)] + sems(2),
            "gather_rows", params(0))
        lists = [(item.reshape(edges // WAYS), "smem") for item in lists]

        h1, dz, hz, hub = call(
            functools.partial(edges_forward_kernel, copies1, unroll1),
            [(w_first, "vmem"), (x_t, "vmem"), (dy_out, "vmem"), (xh, "vmem"), (hx, "vmem"), (dhh, "vmem"),
             (used, "smem"), (hub_ids, "smem"), (bias, "vmem")] + lists,
            (shape((nodes, HID), BF16), shape((nodes, LANES), F32), shape((halo, LANES), F32), shape((hubs, HID + LANES), F32)),
            [pltpu.VMEM((src_rows * TILES, LANES), F32), pltpu.VMEM((dst_rows * TILES, LANES), F32)]
            + [pltpu.VMEM((dst_rows * TILES, LANES), F32)] * copies1 + [pltpu.VMEM((src_rows * TILES, LANES), F32)] * copies1,
            "edges_forward", params())

        dz2, dyh, h1h, dz2h, wide = call(
            functools.partial(middle_kernel, groups),
            [(hub.reshape(groups, home, HID + LANES), "vmem"), (hz.reshape(groups, block, LANES), "vmem"), (dz, "vmem"),
             (bias, "vmem"), (w_second, "vmem"), (send_lanes, "vmem"), (table(w_loc), "vmem")],
            (shape((nodes, LANES), BF16), shape((hubs, HID), F32), shape((home, HID), BF16), shape((home, LANES), BF16), shape((edges, LANES), F32)),
            [pltpu.VMEM((groups, block, LANES), F32), pltpu.VMEM((groups, home, HID + LANES), F32),
             pltpu.VMEM((groups, home, HID), F32), pltpu.VMEM((home, HID), F32)] + sems(3),
            "middle", params(1))

        dz1, hz1, hub1, dw2, biases = call(
            functools.partial(edges_backward_kernel, copies2, unroll2, feat, groups),
            [(w_second, "vmem"), (h1, "vmem"), (dz2, "vmem"), (dyh, "vmem"), (h1h, "vmem"), (dz2h, "vmem"),
             (used, "smem"), (hub_ids, "smem"), (xh, "vmem"), (db2, "vmem"), (wide, "vmem")] + lists[:2 * WAYS],
            (shape((nodes, HID), F32), shape((TILES, halo, LANES), F32), shape((hubs, HID), F32), shape((LANES, HID), F32), shape((8, LANES), F32)),
            [pltpu.VMEM((dst_rows * TILES, LANES), F32)] + [pltpu.VMEM((src_rows * TILES, LANES), F32)] * copies2,
            "edges_backward", params())

        chips = groups // 2
        part = LANES // groups
        grad_xt, dw1, dw2, biases = call(
            functools.partial(last_kernel, groups),
            [(hub1.reshape(2, chips, home, HID), "vmem"), (hz1.reshape(TILES, groups, block, LANES), "hbm"),
             (dw2.reshape(2, chips, part, HID), "vmem"), (biases, "vmem"), (send_lanes, "vmem"), (x_t, "vmem"), (hx, "vmem"),
             (dz1, "vmem"), (w_first, "vmem"), (hub_lanes, "vmem")],
            (shape((feat, nodes), F32), shape((TILES, groups, 8, LANES), F32), shape((2, chips, part, HID), F32), shape((8, LANES), F32)),
            [pltpu.VMEM((nodes, HID), BF16), pltpu.VMEM((nodes, halo), BF16), pltpu.VMEM((TILES, groups, block, LANES), F32)]
            + [pltpu.VMEM((chips, home, HID), F32)] * 3 + [pltpu.VMEM((8, LANES), F32)] * 2 + [pltpu.VMEM((chips, 8, LANES), F32)]
            + [pltpu.VMEM((home, HID), BF16), pltpu.VMEM((groups, home, HID), BF16)]
            + [pltpu.VMEM((chips, part, HID), F32)] * 3 + [pltpu.VMEM((part, HID), F32)]
            + [pltpu.VMEM((TILES, groups * 8, LANES), F32), pltpu.VMEM((TILES, groups, 8, LANES), F32), pltpu.VMEM((TILES, 8, LANES), F32)] + sems(21),
            "last_exchange", params(2))

        grad_xt, grad_w1, grad_w2, grad_b1, grad_b2 = call(
            outputs_kernel,
            [(grad_xt, "vmem"), (dw2.reshape(LANES, HID), "vmem"), (biases, "vmem"), (dw1, "vmem")],
            (shape((feat, nodes), F32), shape((feat, HID), F32), shape((HID, out), F32), shape((1, HID), F32), shape((1, out), F32)),
            [], "outputs", params())
        return grad_xt.T, grad_w1, grad_w2, grad_b1.reshape(HID), grad_b2.reshape(out)

    return jax.shard_map(
        device_step,
        mesh=mesh,
        in_specs=(vertex_rows, vertex_spec, vertex_spec, vertex_spec, vertex_spec, part_spec, replicated, replicated, replicated, vertex_rows),
        out_specs=(vertex_rows, part_rows, part_rows, part_spec, part_spec),
        check_vma=False,
    )
```
